32 devices in a mesh: fsdp: 16 (over z, y, x), sub: 2 (over core).
Axes of the slice: x: 2, y: 2, z: 4, core: 2. Of those that a mesh axis runs over, the one named last changes fastest.
Arguments:
- inputs: bfloat16 [64, 512, 768], P(('fsdp', 'sub')), may hold values from -6 to 6
- lengths: int32 [64], P(('fsdp', 'sub')), may hold values from 257 to 512, as said below
- positions: int32 [64, 128], P(('fsdp', 'sub')), may hold values from 0 to 512, as said below
- masked_output_gradient: bfloat16 [64, 128, 768], P(('fsdp', 'sub')), may hold values from -6 to 6
- w_query: bfloat16 [768, 768], P(('fsdp', 'sub')), may hold values from -0.21875 to 0.21875
- b_query: bfloat16 [768], P(('fsdp', 'sub')), may hold values from -3 to 3
- w_key: bfloat16 [768, 768], P(('fsdp', 'sub')), may hold values from -0.21875 to 0.21875
- w_value: bfloat16 [768, 768], P(('fsdp', 'sub')), may hold values from -0.21875 to 0.21875
- b_value: bfloat16 [768], P(('fsdp', 'sub')), may hold values from -3 to 3
- w_out: bfloat16 [768, 768], P(('fsdp', 'sub')), may hold values from -1.75 to 1.75
- b_out: bfloat16 [768], P(('fsdp', 'sub')), may hold values from -3 to 3
- gain_attn: bfloat16 [768], P(('fsdp', 'sub')), may hold values from 0.5 to 1.5
- shift_attn: bfloat16 [768], P(('fsdp', 'sub')), may hold values from -3 to 3
- w_up: bfloat16 [768, 3072], P(('fsdp', 'sub')), may hold values from -0.21875 to 0.21875
- b_up: bfloat16 [3072], P(('fsdp', 'sub')), may hold values from -3 to 3
- w_down: bfloat16 [3072, 768], P(('fsdp', 'sub')), may hold values from -0.109375 to 0.109375
- b_down: bfloat16 [768], P(('fsdp', 'sub')), may hold values from -3 to 3
- gain_ffn: bfloat16 [768], P(('fsdp', 'sub')), may hold values from 0.5 to 1.5
- shift_ffn: bfloat16 [768], P(('fsdp', 'sub')), may hold values from -3 to 3
Outputs:
- output: bfloat16 [64, 512, 768], P(('fsdp', 'sub'))
- grad_inputs: bfloat16 [64, 512, 768], P(('fsdp', 'sub'))
- grad_w_query: float32 [768, 768], P(('fsdp', 'sub'))
- grad_b_query: float32 [768], P(('fsdp', 'sub'))
- grad_w_key: float32 [768, 768], P(('fsdp', 'sub'))
- grad_w_value: float32 [768, 768], P(('fsdp', 'sub'))
- grad_b_value: float32 [768], P(('fsdp', 'sub'))
- grad_w_out: float32 [768, 768], P(('fsdp', 'sub'))
- grad_b_out: float32 [768], P(('fsdp', 'sub'))
- grad_gain_attn: float32 [768], P(('fsdp', 'sub'))
- grad_shift_attn: float32 [768], P(('fsdp', 'sub'))
- grad_w_up: float32 [768, 3072], P(('fsdp', 'sub'))
- grad_b_up: float32 [3072], P(('fsdp', 'sub'))
- grad_w_down: float32 [3072, 768], P(('fsdp', 'sub'))
- grad_b_down: float32 [768], P(('fsdp', 'sub'))
- grad_gain_ffn: float32 [768], P(('fsdp', 'sub'))
- feedforward_shift_gradient: float32 [768], P(('fsdp', 'sub'))
The draws below stay inside these ranges and needn't reach their ends.
Inputs may be any that keep to these rules, and one draw needn't show every extreme that they name: `lengths`: the valid tokens of a sequence come first; the first sequence is full. In each sequence the used slots come first, from 16 to 128 of them, holding distinct positions below the sequence's length; the other slots hold 512. Some sequence uses all 128 slots.
All inputs are finite; a program needn't handle non-finite values.
Results may differ from the reference program's by a relative error of at most 0.014.
The reference program's roundings to bfloat16 on the way count: a program that leaves them out, or rounds other values in their place, can miss the bound.
Values may be sent and summed in bfloat16 or wider, within the bound.
A program may use at most 192 MiB of HBM per device.

```python
import math
import jax
import jax.numpy as jnp
from jax import lax

D = 768
HEADS = 12
HD = 64
FF = 3072
SEQ_LEN = 512
MAX_MASK = 128
SEQS = 64


def mask_plan(key):
    key = jax.random.fold_in(key, 7)
    key_len, key_extra, key_factor, key_order = jax.random.split(key, 4)
    shortage = jax.random.randint(key_len, (SEQS,), 0, SEQ_LEN // 2)
    seq_lengths = (SEQ_LEN - shortage).at[0].set(SEQ_LEN)
    extras = jax.random.randint(key_extra, (SEQS,), 0, MAX_MASK // 2)
    factor_table = jnp.array([1, 2, 4], jnp.int32)
    factor = factor_table[jax.random.randint(key_factor, (SEQS,), 0, 3)]
    counts = jnp.minimum(MAX_MASK, MAX_MASK // 8 + extras * factor)
    counts = counts.at[0].set(MAX_MASK).at[1].set(MAX_MASK // 8)
    order_keys = jax.random.split(key_order, SEQS)
    orders = jax.vmap(lambda one_key: jax.random.permutation(one_key, SEQ_LEN))(order_keys)
    outside = (orders >= seq_lengths[:, None]).astype(jnp.int32)
    ranked = jnp.argsort(outside, axis=1, stable=True)
    picked = jnp.take_along_axis(orders, ranked, axis=1)[:, :MAX_MASK]
    slot_ids = jnp.arange(MAX_MASK, dtype=jnp.int32)[None, :]
    chosen = jnp.where(slot_ids < counts[:, None], picked, SEQ_LEN)
    return (seq_lengths.astype(jnp.int32), chosen.astype(jnp.int32))


def draw_lengths(key, part):
    return mask_plan(key)[0]


def draw_positions(key, part):
    return mask_plan(key)[1]


def spiked(values, stream_key, source, target, shards_of, factor):
    owner, partner = [(jnp.arange(values.shape[dim]) // (values.shape[dim] // shards_of)).reshape([-1 if axis == dim else 1 for axis in range(values.ndim)]) for dim in (source, target)]
    chosen = jax.random.permutation(stream_key, shards_of)[partner]
    strong = (owner == chosen) | (owner == (partner + shards_of // 2) % shards_of)
    return jnp.where(strong, factor * values, values)


def block_scale(own_key, dims, cuts, smallest, largest):
    level, own = 1.0, jax.random.fold_in(own_key, 6)
    for dim, blocks in cuts:
        steps = jnp.exp(jax.random.uniform(jax.random.fold_in(own, dim), (blocks,), jnp.float32, smallest / len(cuts), largest / len(cuts)))
        level = level * jnp.repeat(steps, dims[dim] // blocks).reshape([-1 if axis == dim else 1 for axis in range(len(dims))])
    return level


def gaussian(rng, dims, spread, reach, cuts=(), held_as=jnp.bfloat16):
    loudness = block_scale(rng, dims, cuts, -0.22, 0.18) if cuts else 1.0
    values = jax.random.normal(rng, dims, jnp.float32) * spread * loudness
    return jnp.minimum(jnp.maximum(values, -reach), reach).astype(held_as)


def noise_with(stream_key, shape, deviation, limit, shards, heavy, kind=jnp.bfloat16):
    drawn = deviation * jax.random.normal(stream_key, shape, jnp.float32)
    if shards:
        drawn = drawn * block_scale(stream_key, shape, shards, -0.22, 0.18)
    return jnp.clip(spiked(drawn, jax.random.fold_in(stream_key, 3), *heavy), -limit, limit).astype(kind)


def setup_inputs(seed: int = 0) -> dict:
    streams_of = jax.random.split(jax.random.key(seed), 20)
    inputs = noise_with(streams_of[0], (SEQS, SEQ_LEN, D), 1.0, 6.0, ((0, 32),), (0, 2, 32, 2.75))
    lengths = draw_lengths(jax.random.fold_in(streams_of[19], 71), 0)
    positions = draw_positions(jax.random.fold_in(streams_of[19], 71), 0)
    masked_output_gradient = gaussian(streams_of[3], (SEQS, MAX_MASK, D), 1.0, 6.0, ((0, 32),))
    w_query = gaussian(streams_of[4], (D, D), D ** -0.5, 0.21875, ((0, 32),))
    b_query = gaussian(streams_of[5], (D,), 0.5, 3.0, ((0, 32),))
    w_key = gaussian(streams_of[6], (D, D), D ** -0.5, 0.21875, ((0, 32),))
    w_value = gaussian(streams_of[7], (D, D), D ** -0.5, 0.21875, ((0, 32),))
    b_value = gaussian(streams_of[8], (D,), 0.5, 3.0, ((0, 32),))
    w_out = gaussian(streams_of[9], (D, D), (D // 64) ** -0.5, 1.75, ((0, 32),))
    b_out = gaussian(streams_of[10], (D,), 0.5, 3.0, ((0, 32),))
    gain_attn = jnp.clip(1.0 + 0.1 * jax.random.normal(streams_of[11], (D,), jnp.float32), 0.5, 1.5).astype(jnp.bfloat16)
    shift_attn = gaussian(streams_of[12], (D,), 0.5, 3.0, ((0, 32),))
    w_up = gaussian(streams_of[13], (D, FF), D ** -0.5, 0.21875, ((0, 32),))
    b_up = gaussian(streams_of[14], (FF,), 0.5, 3.0, ((0, 32),))
    w_down = gaussian(streams_of[15], (FF, D), FF ** -0.5, 0.109375, ((0, 32),))
    b_down = gaussian(streams_of[16], (D,), 0.5, 3.0, ((0, 32),))
    gain_ffn = jnp.clip(1.0 + 0.1 * jax.random.normal(streams_of[17], (D,), jnp.float32), 0.5, 1.5).astype(jnp.bfloat16)
    shift_ffn = gaussian(streams_of[18], (D,), 0.5, 3.0, ((0, 32),))
    return {"inputs": inputs, "lengths": lengths, "positions": positions, "masked_output_gradient": masked_output_gradient, "w_query": w_query, "b_query": b_query, "w_key": w_key, "w_value": w_value, "b_value": b_value, "w_out": w_out, "b_out": b_out, "gain_attn": gain_attn, "shift_attn": shift_attn, "w_up": w_up, "b_up": b_up, "w_down": w_down, "b_down": b_down, "gain_ffn": gain_ffn, "shift_ffn": shift_ffn}


@jax.custom_vjp
def low(v):
    return lax.optimization_barrier(v.astype(jnp.bfloat16)).astype(jnp.float32)

@jax.custom_vjp
def low_back(v):
    return v

def low_keep(v):
    return (low(v), None)

def low_pass(kept, grad):
    return (grad,)

def back_keep(v):
    return (v, None)

def back_low(kept, grad):
    return (low(grad),)
low.defvjp(low_keep, low_pass)
low_back.defvjp(back_keep, back_low)
EPSILON = 1e-06
HIGHEST = lax.Precision.HIGHEST

def layer_norm(values, gain, shift):
    average = lax.optimization_barrier(jnp.mean(values, axis=-1, keepdims=True))
    centered = values - average
    variance = lax.optimization_barrier(jnp.mean(centered * centered, axis=-1, keepdims=True))
    return centered * lax.rsqrt(variance + EPSILON) * gain + shift

def matmul_high(left, right):
    return jnp.matmul(left, right, precision=HIGHEST)

def forward(params, rows_in, valid_keys):
    w_query, b_query, w_key, w_value, b_value, w_out, b_out, gain_attn, shift_attn, w_up, b_up, w_down, b_down, gain_ffn, shift_ffn = params
    groups, seq_slots, width = rows_in.shape
    head_shape = (groups, seq_slots, HEADS, HD)
    query = low(low_back(matmul_high(rows_in, w_query) + b_query)).reshape(head_shape)
    keys = low(low_back(matmul_high(rows_in, w_key))).reshape(head_shape)
    values = low(low_back(matmul_high(rows_in, w_value) + b_value)).reshape(head_shape)
    scores = jnp.einsum('gqhd,gkhd->ghqk', query, keys, precision=HIGHEST) * HD ** (-0.5)
    scores = low_back(jnp.where(valid_keys[:, None, None, :], scores, -1e+30))
    row_top = lax.optimization_barrier(jnp.max(scores, axis=-1, keepdims=True))
    expon = jnp.exp(scores - row_top)
    probs_low = low(expon / lax.optimization_barrier(jnp.sum(expon, axis=-1, keepdims=True)))
    attention_mixed = jnp.einsum('ghqk,gkhd->gqhd', probs_low, values, precision=HIGHEST)
    attended_low = low(low_back(attention_mixed.reshape(groups, seq_slots, width)))
    branch = low_back(matmul_high(attended_low, w_out) + b_out)
    middle = layer_norm(rows_in + branch, gain_attn, shift_attn)
    middle_low = low(middle)
    hidden = low_back(matmul_high(middle_low, w_up) + b_up)
    active_low = low(jax.nn.gelu(hidden, approximate=False))
    second_branch = low_back(matmul_high(active_low, w_down) + b_down)
    return layer_norm(middle + second_branch, gain_ffn, shift_ffn)

def reference(inputs, lengths, positions, masked_output_gradient, w_query, b_query, w_key, w_value, b_value, w_out, b_out, gain_attn, shift_attn, w_up, b_up, w_down, b_down, gain_ffn, shift_ffn):
    params = tuple((item.astype(jnp.float32) for item in (w_query, b_query, w_key, w_value, b_value, w_out, b_out, gain_attn, shift_attn, w_up, b_up, w_down, b_down, gain_ffn, shift_ffn)))
    total_seqs = inputs.shape[0]
    group_size = math.gcd(total_seqs, max(1, 4096 // SEQ_LEN))
    block_count = total_seqs // group_size
    token_ids = jnp.arange(SEQ_LEN, dtype=jnp.int32)
    group_ids = jnp.arange(group_size, dtype=jnp.int32)

    def one_group(carry, pieces):
        rows_in, group_lengths, group_positions, group_cot = pieces
        valid_keys = token_ids[None, :] < group_lengths[:, None]
        cotangent = jnp.zeros((group_size, SEQ_LEN, D), jnp.float32).at[group_ids[:, None], group_positions.astype(jnp.int32)].add(group_cot.astype(jnp.float32), mode='drop')
        result, pull_back = jax.vjp(lambda weights, rows: forward(weights, rows, valid_keys), params, rows_in.astype(jnp.float32))
        grad_params, grad_rows = pull_back(cotangent)
        carry = jax.tree.map(jnp.add, carry, grad_params)
        return (carry, (result.astype(jnp.bfloat16), grad_rows.astype(jnp.bfloat16)))
    zero_grads = tuple((jnp.zeros_like(item) for item in params))
    grads, (outputs, grad_rows) = lax.scan(one_group, zero_grads, (inputs.reshape(block_count, group_size, SEQ_LEN, D), lengths.reshape(block_count, group_size), positions.reshape(block_count, group_size, MAX_MASK), masked_output_gradient.reshape(block_count, group_size, MAX_MASK, D)))
    output = outputs.reshape(total_seqs, SEQ_LEN, D)
    grad_inputs = grad_rows.reshape(total_seqs, SEQ_LEN, D)
    return (output, grad_inputs, grads[0], grads[1], grads[2], grads[3], grads[4], grads[5], grads[6], grads[7], grads[8], grads[9], grads[10], grads[11], grads[12], grads[13], grads[14])
```

```python
import jax
import jax.numpy as jnp
from jax import lax
from jax.sharding import PartitionSpec as P

HD = 64
EPSILON = 1e-06
AXES = ("fsdp", "sub")
GRAD_WIRE = jnp.float32
VEC_COLS = 256


def layer_norm(values, gain, shift):
    average = jnp.mean(values, axis=-1, keepdims=True)
    centered = values - average
    variance = jnp.mean(centered * centered, axis=-1, keepdims=True)
    return centered * lax.rsqrt(variance + EPSILON) * gain + shift


def gelu_exact(values):
    return jax.nn.gelu(values, approximate=False)


def project(rows_low, weight):
    return jnp.dot(rows_low, weight, preferred_element_type=jnp.float32)


def reverse_projection(grad_low, weight):
    return lax.dot_general(
        grad_low, weight, (((1,), (1,)), ((), ())), preferred_element_type=jnp.float32
    )


def weight_grad(rows_low, grad_low):
    return lax.dot_general(
        rows_low, grad_low, (((0,), (0,)), ((), ())), preferred_element_type=jnp.float32
    )


def column_sum(grad_low):
    return jnp.sum(grad_low.astype(jnp.float32), axis=0)


def attention_scores(query_heads, key_heads, valid_keys, scale):
    scores = (
        jnp.einsum("sqhd,skhd->shqk", query_heads, key_heads, preferred_element_type=jnp.float32)
        * scale
    )
    return jnp.where(valid_keys[:, None, None, :], scores, -1e30)


def pack_vectors(rows, vectors, dtype):
    cols = [v.reshape(rows, -1).astype(dtype) for v in vectors]
    block = jnp.concatenate(cols, axis=1)
    return jnp.pad(block, ((0, 0), (0, VEC_COLS - block.shape[1])))


def unpack_vectors(block, widths):
    out, at = [], 0
    for width in widths:
        out.append(block[:, at : at + width].reshape(-1))
        at += width
    return out


def gather_rows(pack):
    return lax.all_gather(pack, AXES, axis=0, tiled=True)


def scatter_rows(pack):
    return lax.psum_scatter(pack.astype(GRAD_WIRE), AXES, scatter_dimension=0, tiled=True).astype(
        jnp.float32
    )


def body(
    inputs,
    lengths,
    positions,
    masked_output_gradient,
    w_query,
    b_query,
    w_key,
    w_value,
    b_value,
    w_out,
    b_out,
    gain_attn,
    shift_attn,
    w_up,
    b_up,
    w_down,
    b_down,
    gain_ffn,
    shift_ffn,
):
    seq_count, seq_slots, width = inputs.shape
    head_count = width // HD
    scale = HD ** (-0.5)
    row_count = seq_count * seq_slots
    head_shape = (seq_count, seq_slots, head_count, HD)
    shard_rows = w_query.shape[0]
    ff_ratio = w_down.shape[0] // shard_rows
    ff_width = w_up.shape[1]
    token_ids = jnp.arange(seq_slots, dtype=jnp.int32)
    valid_keys = token_ids[None, :] < lengths[:, None]

    with jax.named_scope("gather_attn"):
        attn_pack = jnp.concatenate(
            [
                w_query,
                w_key,
                w_value,
                w_out,
                pack_vectors(
                    shard_rows, (b_query, b_value, b_out, gain_attn, shift_attn), jnp.bfloat16
                ),
            ],
            axis=1,
        )
        attn_full = gather_rows(attn_pack)
    query_weight = attn_full[:, 0:width]
    key_weight = attn_full[:, width : 2 * width]
    value_weight = attn_full[:, 2 * width : 3 * width]
    out_weight = attn_full[:, 3 * width : 4 * width]
    query_bias, value_bias, out_bias, norm1_gain, norm1_shift = unpack_vectors(
        attn_full[:, 4 * width :], (1, 1, 1, 1, 1)
    )

    with jax.named_scope("gather_ffn"):
        ffn_pack = jnp.concatenate(
            [
                w_up,
                w_down.reshape(shard_rows, ff_ratio * width),
                pack_vectors(
                    shard_rows, (b_up, b_down, gain_ffn, shift_ffn), jnp.bfloat16
                ),
            ],
            axis=1,
        )
        ffn_full = gather_rows(ffn_pack)
    up_weight = ffn_full[:, 0:ff_width]
    down_weight = ffn_full[:, ff_width : 2 * ff_width].reshape(ff_width, width)
    up_bias, downward_bias, norm2_gain, norm2_shift = unpack_vectors(
        ffn_full[:, 2 * ff_width :], (ff_ratio, 1, 1, 1)
    )

    flat_in = inputs.reshape(row_count, width)
    input_rows = flat_in.astype(jnp.float32)
    query_low = (project(flat_in, query_weight) + query_bias.astype(jnp.float32)).astype(
        jnp.bfloat16
    )
    keys_low = project(flat_in, key_weight).astype(jnp.bfloat16)
    values_low = (project(flat_in, value_weight) + value_bias.astype(jnp.float32)).astype(
        jnp.bfloat16
    )
    query_heads = query_low.reshape(head_shape)
    key_heads = keys_low.reshape(head_shape)
    value_heads = values_low.reshape(head_shape)
    scores = attention_scores(query_heads, key_heads, valid_keys, scale)
    row_top = jnp.max(scores, axis=-1, keepdims=True)
    expon = jnp.exp(scores - row_top)
    row_total = jnp.sum(expon, axis=-1, keepdims=True)
    log_total = row_top + jnp.log(row_total)
    probs_low = (expon / row_total).astype(jnp.bfloat16)
    attention_mixed = jnp.einsum(
        "shqk,skhd->sqhd", probs_low, value_heads, preferred_element_type=jnp.float32
    )
    attended_low = attention_mixed.reshape(row_count, width).astype(jnp.bfloat16)
    branch = project(attended_low, out_weight) + out_bias.astype(jnp.float32)
    middle, norm1_pull = jax.vjp(
        layer_norm,
        input_rows + branch,
        norm1_gain.astype(jnp.float32),
        norm1_shift.astype(jnp.float32),
    )
    middle_low = middle.astype(jnp.bfloat16)
    hidden = project(middle_low, up_weight) + up_bias.astype(jnp.float32)
    active, gelu_pull = jax.vjp(gelu_exact, hidden)
    active_low = active.astype(jnp.bfloat16)
    second_branch = project(active_low, down_weight) + downward_bias.astype(jnp.float32)
    output, norm2_pull = jax.vjp(
        layer_norm,
        middle + second_branch,
        norm2_gain.astype(jnp.float32),
        norm2_shift.astype(jnp.float32),
    )
    position_matches = (positions[:, :, None] == token_ids[None, None, :]).astype(jnp.bfloat16)
    cotangent = jnp.einsum(
        "efw,efv->ewv", position_matches, masked_output_gradient, preferred_element_type=jnp.float32
    ).reshape(row_count, width)
    grad_sum2, grad_gain2, grad_shift2 = norm2_pull(cotangent)
    second_grad = grad_sum2.astype(jnp.bfloat16)
    grad_down = weight_grad(active_low, second_grad)
    grad_down_bias = column_sum(second_grad)
    (grad_hidden,) = gelu_pull(reverse_projection(second_grad, down_weight))
    hidden_grad = grad_hidden.astype(jnp.bfloat16)
    grad_up = weight_grad(middle_low, hidden_grad)
    grad_up_bias = column_sum(hidden_grad)
    grad_middle = grad_sum2 + reverse_projection(hidden_grad, up_weight)
    grad_residual, grad_gain1, grad_shift1 = norm1_pull(grad_middle)
    branch_grad = grad_residual.astype(jnp.bfloat16)
    grad_out = weight_grad(attended_low, branch_grad)
    grad_out_bias = column_sum(branch_grad)

    with jax.named_scope("scatter_late"):
        late_pack = jnp.concatenate(
            [
                grad_up,
                grad_down.reshape(width, ff_ratio * width),
                grad_out,
                pack_vectors(
                    width,
                    (
                        grad_up_bias,
                        grad_down_bias,
                        grad_gain2,
                        grad_shift2,
                        grad_out_bias,
                        grad_gain1,
                        grad_shift1,
                    ),
                    jnp.float32,
                ),
            ],
            axis=1,
        )
        late_own = scatter_rows(late_pack)
    grad_up_own = late_own[:, 0:ff_width]
    grad_down_own = late_own[:, ff_width : 2 * ff_width].reshape(shard_rows * ff_ratio, width)
    grad_out_own = late_own[:, 2 * ff_width : 2 * ff_width + width]
    (
        grad_up_bias_own,
        grad_down_bias_own,
        grad_gain2_own,
        grad_shift2_own,
        grad_out_bias_own,
        grad_gain1_own,
        grad_shift1_own,
    ) = unpack_vectors(late_own[:, 2 * ff_width + width :], (ff_ratio, 1, 1, 1, 1, 1, 1))

    attended_grad = (
        reverse_projection(branch_grad, out_weight).astype(jnp.bfloat16).reshape(head_shape)
    )
    scores_again = attention_scores(query_heads, key_heads, valid_keys, scale)
    probs = jnp.exp(scores_again - log_total)
    probs_again = probs.astype(jnp.bfloat16)
    probs_grad = jnp.einsum(
        "sqhd,skhd->shqk", attended_grad, value_heads, preferred_element_type=jnp.float32
    )
    values_grad = jnp.einsum(
        "shqk,sqhd->skhd", probs_again, attended_grad, preferred_element_type=jnp.float32
    )
    values_grad = values_grad.astype(jnp.bfloat16).reshape(row_count, width)
    inner_sum = jnp.sum(probs * probs_grad, axis=-1, keepdims=True)
    scores_grad = (probs * (probs_grad - inner_sum)).astype(jnp.bfloat16)
    query_grad = jnp.einsum(
        "shqk,skhd->sqhd", scores_grad, key_heads, preferred_element_type=jnp.float32
    )
    query_grad = (query_grad * scale).astype(jnp.bfloat16).reshape(row_count, width)
    keys_grad = jnp.einsum(
        "shqk,sqhd->skhd", scores_grad, query_heads, preferred_element_type=jnp.float32
    )
    keys_grad = (keys_grad * scale).astype(jnp.bfloat16).reshape(row_count, width)
    grad_query = weight_grad(flat_in, query_grad)
    grad_query_bias = column_sum(query_grad)
    grad_key = weight_grad(flat_in, keys_grad)
    grad_value = weight_grad(flat_in, values_grad)
    value_bias_gradient = column_sum(values_grad)
    grad_input = (
        grad_residual
        + reverse_projection(query_grad, query_weight)
        + reverse_projection(keys_grad, key_weight)
        + reverse_projection(values_grad, value_weight)
    )
    with jax.named_scope("scatter_qkv"):
        qkv_pack = jnp.concatenate(
            [
                grad_query,
                grad_key,
                grad_value,
                pack_vectors(width, (grad_query_bias, value_bias_gradient), jnp.float32),
            ],
            axis=1,
        )
        qkv_own = scatter_rows(qkv_pack)
    grad_query_own = qkv_own[:, 0:width]
    grad_key_own = qkv_own[:, width : 2 * width]
    grad_value_own = qkv_own[:, 2 * width : 3 * width]
    grad_query_bias_own, value_bias_gradient_own = unpack_vectors(
        qkv_own[:, 3 * width :], (1, 1)
    )
    return (
        output.astype(jnp.bfloat16).reshape(inputs.shape),
        grad_input.astype(jnp.bfloat16).reshape(inputs.shape),
        grad_query_own,
        grad_query_bias_own,
        grad_key_own,
        grad_value_own,
        value_bias_gradient_own,
        grad_out_own,
        grad_out_bias_own,
        grad_gain1_own,
        grad_shift1_own,
        grad_up_own,
        grad_up_bias_own,
        grad_down_own,
        grad_down_bias_own,
        grad_gain2_own,
        grad_shift2_own,
    )


def solution(mesh):
    rows3 = P(AXES, None, None)
    rows2 = P(AXES, None)
    rows1 = P(AXES)
    return jax.shard_map(
        body,
        mesh=mesh,
        in_specs=(
            rows3,
            rows1,
            rows2,
            rows3,
            rows2,
            rows1,
            rows2,
            rows2,
            rows1,
            rows2,
            rows1,
            rows1,
            rows1,
            rows2,
            rows1,
            rows2,
            rows1,
            rows1,
            rows1,
        ),
        out_specs=(
            rows3,
            rows3,
            rows2,
            rows1,
            rows2,
            rows2,
            rows1,
            rows2,
            rows1,
            rows1,
            rows1,
            rows2,
            rows1,
            rows2,
            rows1,
            rows1,
            rows1,
        ),
        check_vma=False,
    )
```

```python
import jax
import jax.numpy as jnp
from jax import lax
from jax.sharding import PartitionSpec as P

HD = 64
EPSILON = 1e-06
AXES = ("fsdp", "sub")
GRAD_WIRE = jnp.float32
VEC_COLS = 256


def layer_norm(values, gain, shift):
    average = jnp.mean(values, axis=-1, keepdims=True)
    centered = values - average
    variance = jnp.mean(centered * centered, axis=-1, keepdims=True)
    return centered * lax.rsqrt(variance + EPSILON) * gain + shift


def gelu_exact(values):
    return jax.nn.gelu(values, approximate=False)


def project(rows_low, weight):
    return jnp.dot(rows_low, weight, preferred_element_type=jnp.float32)


def reverse_projection(grad_low, weight):
    return lax.dot_general(
        grad_low, weight, (((1,), (1,)), ((), ())), preferred_element_type=jnp.float32
    )


def weight_grad(rows_low, grad_low):
    return lax.dot_general(
        rows_low, grad_low, (((0,), (0,)), ((), ())), preferred_element_type=jnp.float32
    )


def column_sum(grad_low):
    return jnp.sum(grad_low.astype(jnp.float32), axis=0)


def attention_scores(query_heads, key_heads, valid_keys, scale):
    scores = (
        jnp.einsum("sqhd,skhd->shqk", query_heads, key_heads, preferred_element_type=jnp.float32)
        * scale
    )
    return jnp.where(valid_keys[:, None, None, :], scores, -1e30)


def pack_vectors(rows, vectors, dtype):
    cols = [v.reshape(rows, -1).astype(dtype) for v in vectors]
    block = jnp.concatenate(cols, axis=1)
    return jnp.pad(block, ((0, 0), (0, VEC_COLS - block.shape[1])))


def unpack_vectors(block, widths):
    out, at = [], 0
    for width in widths:
        out.append(block[:, at : at + width].reshape(-1))
        at += width
    return out


def gather_rows(pack):
    return lax.all_gather(pack, AXES, axis=0, tiled=True)


def scatter_rows(pack):
    return lax.psum_scatter(pack.astype(GRAD_WIRE), AXES, scatter_dimension=0, tiled=True).astype(
        jnp.float32
    )


def body(
    inputs,
    lengths,
    positions,
    masked_output_gradient,
    w_query,
    b_query,
    w_key,
    w_value,
    b_value,
    w_out,
    b_out,
    gain_attn,
    shift_attn,
    w_up,
    b_up,
    w_down,
    b_down,
    gain_ffn,
    shift_ffn,
):
    seq_count, seq_slots, width = inputs.shape
    head_count = width // HD
    scale = HD ** (-0.5)
    row_count = seq_count * seq_slots
    head_shape = (seq_count, seq_slots, head_count, HD)
    shard_rows = w_query.shape[0]
    ff_ratio = w_down.shape[0] // shard_rows
    ff_width = w_up.shape[1]
    token_ids = jnp.arange(seq_slots, dtype=jnp.int32)
    valid_keys = token_ids[None, :] < lengths[:, None]

    with jax.named_scope("gather_attn"):
        attn_pack = jnp.concatenate(
            [
                w_query,
                w_key,
                w_value,
                w_out,
                pack_vectors(
                    shard_rows, (b_query, b_value, b_out, gain_attn, shift_attn), jnp.bfloat16
                ),
            ],
            axis=1,
        )
        attn_full = gather_rows(attn_pack)
    query_weight = attn_full[:, 0:width]
    key_weight = attn_full[:, width : 2 * width]
    value_weight = attn_full[:, 2 * width : 3 * width]
    out_weight = attn_full[:, 3 * width : 4 * width]
    query_bias, value_bias, out_bias, norm1_gain, norm1_shift = unpack_vectors(
        attn_full[:, 4 * width :], (1, 1, 1, 1, 1)
    )

    with jax.named_scope("gather_ffn"):
        ffn_pack = jnp.concatenate(
            [
                w_up,
                w_down.reshape(shard_rows, ff_ratio * width),
                pack_vectors(
                    shard_rows, (b_up, b_down, gain_ffn, shift_ffn), jnp.bfloat16
                ),
            ],
            axis=1,
        )
        ffn_full = gather_rows(ffn_pack)
    up_weight = ffn_full[:, 0:ff_width]
    down_weight = ffn_full[:, ff_width : 2 * ff_width].reshape(ff_width, width)
    up_bias, downward_bias, norm2_gain, norm2_shift = unpack_vectors(
        ffn_full[:, 2 * ff_width :], (ff_ratio, 1, 1, 1)
    )

    flat_in = inputs.reshape(row_count, width)
    input_rows = flat_in.astype(jnp.float32)
    query_low = (project(flat_in, query_weight) + query_bias.astype(jnp.float32)).astype(
        jnp.bfloat16
    )
    keys_low = project(flat_in, key_weight).astype(jnp.bfloat16)
    values_low = (project(flat_in, value_weight) + value_bias.astype(jnp.float32)).astype(
        jnp.bfloat16
    )
    query_heads = query_low.reshape(head_shape)
    key_heads = keys_low.reshape(head_shape)
    value_heads = values_low.reshape(head_shape)
    scores = attention_scores(query_heads, key_heads, valid_keys, scale)
    row_top = jnp.max(scores, axis=-1, keepdims=True)
    expon = jnp.exp(scores - row_top)
    row_total = jnp.sum(expon, axis=-1, keepdims=True)
    log_total = row_top + jnp.log(row_total)
    probs_low = (expon / row_total).astype(jnp.bfloat16)
    attention_mixed = jnp.einsum(
        "shqk,skhd->sqhd", probs_low, value_heads, preferred_element_type=jnp.float32
    )
    attended_low = attention_mixed.reshape(row_count, width).astype(jnp.bfloat16)
    branch = project(attended_low, out_weight) + out_bias.astype(jnp.float32)
    middle, norm1_pull = jax.vjp(
        layer_norm,
        input_rows + branch,
        norm1_gain.astype(jnp.float32),
        norm1_shift.astype(jnp.float32),
    )
    middle_low = middle.astype(jnp.bfloat16)
    hidden = project(middle_low, up_weight) + up_bias.astype(jnp.float32)
    active, gelu_pull = jax.vjp(gelu_exact, hidden)
    active_low = active.astype(jnp.bfloat16)
    second_branch = project(active_low, down_weight) + downward_bias.astype(jnp.float32)
    output, norm2_pull = jax.vjp(
        layer_norm,
        middle + second_branch,
        norm2_gain.astype(jnp.float32),
        norm2_shift.astype(jnp.float32),
    )
    position_matches = (positions[:, :, None] == token_ids[None, None, :]).astype(jnp.bfloat16)
    cotangent = jnp.einsum(
        "efw,efv->ewv", position_matches, masked_output_gradient, preferred_element_type=jnp.float32
    ).reshape(row_count, width)
    grad_sum2, grad_gain2, grad_shift2 = norm2_pull(cotangent)
    second_grad = grad_sum2.astype(jnp.bfloat16)
    grad_down = weight_grad(active_low, second_grad)
    grad_down_bias = column_sum(second_grad)
    (grad_hidden,) = gelu_pull(reverse_projection(second_grad, down_weight))
    hidden_grad = grad_hidden.astype(jnp.bfloat16)
    grad_up = weight_grad(middle_low, hidden_grad)
    grad_up_bias = column_sum(hidden_grad)
    grad_middle = grad_sum2 + reverse_projection(hidden_grad, up_weight)
    grad_residual, grad_gain1, grad_shift1 = norm1_pull(grad_middle)
    branch_grad = grad_residual.astype(jnp.bfloat16)
    grad_out = weight_grad(attended_low, branch_grad)
    grad_out_bias = column_sum(branch_grad)

    with jax.named_scope("scatter_late"):
        late_pack = jnp.concatenate(
            [
                grad_up,
                grad_down.reshape(width, ff_ratio * width),
                grad_out,
                pack_vectors(
                    width,
                    (
                        grad_up_bias,
                        grad_down_bias,
                        grad_gain2,
                        grad_shift2,
                        grad_out_bias,
                        grad_gain1,
                        grad_shift1,
                    ),
                    jnp.float32,
                ),
            ],
            axis=1,
        )
        late_pack, branch_grad = lax.optimization_barrier((late_pack, branch_grad))
        late_own = scatter_rows(late_pack)
    grad_up_own = late_own[:, 0:ff_width]
    grad_down_own = late_own[:, ff_width : 2 * ff_width].reshape(shard_rows * ff_ratio, width)
    grad_out_own = late_own[:, 2 * ff_width : 2 * ff_width + width]
    (
        grad_up_bias_own,
        grad_down_bias_own,
        grad_gain2_own,
        grad_shift2_own,
        grad_out_bias_own,
        grad_gain1_own,
        grad_shift1_own,
    ) = unpack_vectors(late_own[:, 2 * ff_width + width :], (ff_ratio, 1, 1, 1, 1, 1, 1))

    attended_grad = (
        reverse_projection(branch_grad, out_weight).astype(jnp.bfloat16).reshape(head_shape)
    )
    scores_again = attention_scores(query_heads, key_heads, valid_keys, scale)
    probs = jnp.exp(scores_again - log_total)
    probs_again = probs.astype(jnp.bfloat16)
    probs_grad = jnp.einsum(
        "sqhd,skhd->shqk", attended_grad, value_heads, preferred_element_type=jnp.float32
    )
    values_grad = jnp.einsum(
        "shqk,sqhd->skhd", probs_again, attended_grad, preferred_element_type=jnp.float32
    )
    values_grad = values_grad.astype(jnp.bfloat16).reshape(row_count, width)
    inner_sum = jnp.sum(probs * probs_grad, axis=-1, keepdims=True)
    scores_grad = (probs * (probs_grad - inner_sum)).astype(jnp.bfloat16)
    query_grad = jnp.einsum(
        "shqk,skhd->sqhd", scores_grad, key_heads, preferred_element_type=jnp.float32
    )
    query_grad = (query_grad * scale).astype(jnp.bfloat16).reshape(row_count, width)
    keys_grad = jnp.einsum(
        "shqk,sqhd->skhd", scores_grad, query_heads, preferred_element_type=jnp.float32
    )
    keys_grad = (keys_grad * scale).astype(jnp.bfloat16).reshape(row_count, width)
    grad_query = weight_grad(flat_in, query_grad)
    grad_query_bias = column_sum(query_grad)
    grad_key = weight_grad(flat_in, keys_grad)
    grad_value = weight_grad(flat_in, values_grad)
    value_bias_gradient = column_sum(values_grad)
    grad_input = (
        grad_residual
        + reverse_projection(query_grad, query_weight)
        + reverse_projection(keys_grad, key_weight)
        + reverse_projection(values_grad, value_weight)
    )
    with jax.named_scope("scatter_qkv"):
        qkv_pack = jnp.concatenate(
            [
                grad_query,
                grad_key,
                grad_value,
                pack_vectors(width, (grad_query_bias, value_bias_gradient), jnp.float32),
            ],
            axis=1,
        )
        qkv_pack, late_own = lax.optimization_barrier((qkv_pack, late_own))
        qkv_own = scatter_rows(qkv_pack)
    grad_query_own = qkv_own[:, 0:width]
    grad_key_own = qkv_own[:, width : 2 * width]
    grad_value_own = qkv_own[:, 2 * width : 3 * width]
    grad_query_bias_own, value_bias_gradient_own = unpack_vectors(
        qkv_own[:, 3 * width :], (1, 1)
    )
    return (
        output.astype(jnp.bfloat16).reshape(inputs.shape),
        grad_input.astype(jnp.bfloat16).reshape(inputs.shape),
        grad_query_own,
        grad_query_bias_own,
        grad_key_own,
        grad_value_own,
        value_bias_gradient_own,
        grad_out_own,
        grad_out_bias_own,
        grad_gain1_own,
        grad_shift1_own,
        grad_up_own,
        grad_up_bias_own,
        grad_down_own,
        grad_down_bias_own,
        grad_gain2_own,
        grad_shift2_own,
    )


def solution(mesh):
    rows3 = P(AXES, None, None)
    rows2 = P(AXES, None)
    rows1 = P(AXES)
    return jax.shard_map(
        body,
        mesh=mesh,
        in_specs=(
            rows3,
            rows1,
            rows2,
            rows3,
            rows2,
            rows1,
            rows2,
            rows2,
            rows1,
            rows2,
            rows1,
            rows1,
            rows1,
            rows2,
            rows1,
            rows2,
            rows1,
            rows1,
            rows1,
        ),
        out_specs=(
            rows3,
            rows3,
            rows2,
            rows1,
            rows2,
            rows2,
            rows1,
            rows2,
            rows1,
            rows1,
            rows1,
            rows2,
            rows1,
            rows2,
            rows1,
            rows1,
            rows1,
        ),
        check_vma=False,
    )
```

```python
import jax
import jax.numpy as jnp
from jax import lax
from jax.sharding import PartitionSpec as P

HD = 64
EPSILON = 1e-06
AXES = ("fsdp", "sub")
GRAD_WIRE = jnp.bfloat16
VEC_COLS = 256


def layer_norm(values, gain, shift):
    average = jnp.mean(values, axis=-1, keepdims=True)
    centered = values - average
    variance = jnp.mean(centered * centered, axis=-1, keepdims=True)
    return centered * lax.rsqrt(variance + EPSILON) * gain + shift


def gelu_exact(values):
    return jax.nn.gelu(values, approximate=False)


def project(rows_low, weight):
    return jnp.dot(rows_low, weight, preferred_element_type=jnp.float32)


def reverse_projection(grad_low, weight):
    return lax.dot_general(
        grad_low, weight, (((1,), (1,)), ((), ())), preferred_element_type=jnp.float32
    )


def weight_grad(rows_low, grad_low):
    return lax.dot_general(
        rows_low, grad_low, (((0,), (0,)), ((), ())), preferred_element_type=jnp.float32
    )


def column_sum(grad_low):
    return jnp.sum(grad_low.astype(jnp.float32), axis=0)


def attention_scores(query_heads, key_heads, valid_keys, scale):
    scores = (
        jnp.einsum("sqhd,skhd->shqk", query_heads, key_heads, preferred_element_type=jnp.float32)
        * scale
    )
    return jnp.where(valid_keys[:, None, None, :], scores, -1e30)


def pack_vectors(rows, vectors, dtype):
    cols = [v.reshape(rows, -1).astype(dtype) for v in vectors]
    block = jnp.concatenate(cols, axis=1)
    return jnp.pad(block, ((0, 0), (0, VEC_COLS - block.shape[1])))


def unpack_vectors(block, widths):
    out, at = [], 0
    for width in widths:
        out.append(block[:, at : at + width].reshape(-1))
        at += width
    return out


def gather_rows(pack):
    return lax.all_gather(pack, AXES, axis=0, tiled=True)


def scatter_rows(pack):
    return lax.psum_scatter(pack.astype(GRAD_WIRE), AXES, scatter_dimension=0, tiled=True).astype(
        jnp.float32
    )


def body(
    inputs,
    lengths,
    positions,
    masked_output_gradient,
    w_query,
    b_query,
    w_key,
    w_value,
    b_value,
    w_out,
    b_out,
    gain_attn,
    shift_attn,
    w_up,
    b_up,
    w_down,
    b_down,
    gain_ffn,
    shift_ffn,
):
    seq_count, seq_slots, width = inputs.shape
    head_count = width // HD
    scale = HD ** (-0.5)
    row_count = seq_count * seq_slots
    head_shape = (seq_count, seq_slots, head_count, HD)
    shard_rows = w_query.shape[0]
    ff_ratio = w_down.shape[0] // shard_rows
    ff_width = w_up.shape[1]
    token_ids = jnp.arange(seq_slots, dtype=jnp.int32)
    valid_keys = token_ids[None, :] < lengths[:, None]

    with jax.named_scope("gather_attn"):
        attn_pack = jnp.concatenate(
            [
                w_query,
                w_key,
                w_value,
                w_out,
                pack_vectors(
                    shard_rows, (b_query, b_value, b_out, gain_attn, shift_attn), jnp.bfloat16
                ),
            ],
            axis=1,
        )
        attn_full = gather_rows(attn_pack)
    query_weight = attn_full[:, 0:width]
    key_weight = attn_full[:, width : 2 * width]
    value_weight = attn_full[:, 2 * width : 3 * width]
    out_weight = attn_full[:, 3 * width : 4 * width]
    query_bias, value_bias, out_bias, norm1_gain, norm1_shift = unpack_vectors(
        attn_full[:, 4 * width :], (1, 1, 1, 1, 1)
    )

    with jax.named_scope("gather_ffn"):
        ffn_pack = jnp.concatenate(
            [
                w_up,
                w_down.reshape(shard_rows, ff_ratio * width),
                pack_vectors(
                    shard_rows, (b_up, b_down, gain_ffn, shift_ffn), jnp.bfloat16
                ),
            ],
            axis=1,
        )
        ffn_full = gather_rows(ffn_pack)
    up_weight = ffn_full[:, 0:ff_width]
    down_weight = ffn_full[:, ff_width : 2 * ff_width].reshape(ff_width, width)
    up_bias, downward_bias, norm2_gain, norm2_shift = unpack_vectors(
        ffn_full[:, 2 * ff_width :], (ff_ratio, 1, 1, 1)
    )

    flat_in = inputs.reshape(row_count, width)
    input_rows = flat_in.astype(jnp.float32)
    query_low = (project(flat_in, query_weight) + query_bias.astype(jnp.float32)).astype(
        jnp.bfloat16
    )
    keys_low = project(flat_in, key_weight).astype(jnp.bfloat16)
    values_low = (project(flat_in, value_weight) + value_bias.astype(jnp.float32)).astype(
        jnp.bfloat16
    )
    query_heads = query_low.reshape(head_shape)
    key_heads = keys_low.reshape(head_shape)
    value_heads = values_low.reshape(head_shape)
    scores = attention_scores(query_heads, key_heads, valid_keys, scale)
    row_top = jnp.max(scores, axis=-1, keepdims=True)
    expon = jnp.exp(scores - row_top)
    row_total = jnp.sum(expon, axis=-1, keepdims=True)
    log_total = row_top + jnp.log(row_total)
    probs_low = (expon / row_total).astype(jnp.bfloat16)
    attention_mixed = jnp.einsum(
        "shqk,skhd->sqhd", probs_low, value_heads, preferred_element_type=jnp.float32
    )
    attended_low = attention_mixed.reshape(row_count, width).astype(jnp.bfloat16)
    branch = project(attended_low, out_weight) + out_bias.astype(jnp.float32)
    middle, norm1_pull = jax.vjp(
        layer_norm,
        input_rows + branch,
        norm1_gain.astype(jnp.float32),
        norm1_shift.astype(jnp.float32),
    )
    middle_low = middle.astype(jnp.bfloat16)
    hidden = project(middle_low, up_weight) + up_bias.astype(jnp.float32)
    active, gelu_pull = jax.vjp(gelu_exact, hidden)
    active_low = active.astype(jnp.bfloat16)
    second_branch = project(active_low, down_weight) + downward_bias.astype(jnp.float32)
    output, norm2_pull = jax.vjp(
        layer_norm,
        middle + second_branch,
        norm2_gain.astype(jnp.float32),
        norm2_shift.astype(jnp.float32),
    )
    position_matches = (positions[:, :, None] == token_ids[None, None, :]).astype(jnp.bfloat16)
    cotangent = jnp.einsum(
        "efw,efv->ewv", position_matches, masked_output_gradient, preferred_element_type=jnp.float32
    ).reshape(row_count, width)
    grad_sum2, grad_gain2, grad_shift2 = norm2_pull(cotangent)
    second_grad = grad_sum2.astype(jnp.bfloat16)
    grad_down = weight_grad(active_low, second_grad)
    grad_down_bias = column_sum(second_grad)
    (grad_hidden,) = gelu_pull(reverse_projection(second_grad, down_weight))
    hidden_grad = grad_hidden.astype(jnp.bfloat16)
    grad_up = weight_grad(middle_low, hidden_grad)
    grad_up_bias = column_sum(hidden_grad)
    grad_middle = grad_sum2 + reverse_projection(hidden_grad, up_weight)
    grad_residual, grad_gain1, grad_shift1 = norm1_pull(grad_middle)
    branch_grad = grad_residual.astype(jnp.bfloat16)
    grad_out = weight_grad(attended_low, branch_grad)
    grad_out_bias = column_sum(branch_grad)

    with jax.named_scope("scatter_late"):
        late_pack = jnp.concatenate(
            [
                grad_up,
                grad_down.reshape(width, ff_ratio * width),
                grad_out,
                pack_vectors(
                    width,
                    (
                        grad_up_bias,
                        grad_down_bias,
                        grad_gain2,
                        grad_shift2,
                        grad_out_bias,
                        grad_gain1,
                        grad_shift1,
                    ),
                    jnp.float32,
                ),
            ],
            axis=1,
        )
        late_pack, branch_grad = lax.optimization_barrier((late_pack, branch_grad))
        late_own = scatter_rows(late_pack)
    grad_up_own = late_own[:, 0:ff_width]
    grad_down_own = late_own[:, ff_width : 2 * ff_width].reshape(shard_rows * ff_ratio, width)
    grad_out_own = late_own[:, 2 * ff_width : 2 * ff_width + width]
    (
        grad_up_bias_own,
        grad_down_bias_own,
        grad_gain2_own,
        grad_shift2_own,
        grad_out_bias_own,
        grad_gain1_own,
        grad_shift1_own,
    ) = unpack_vectors(late_own[:, 2 * ff_width + width :], (ff_ratio, 1, 1, 1, 1, 1, 1))

    attended_grad = (
        reverse_projection(branch_grad, out_weight).astype(jnp.bfloat16).reshape(head_shape)
    )
    scores_again = attention_scores(query_heads, key_heads, valid_keys, scale)
    probs = jnp.exp(scores_again - log_total)
    probs_again = probs.astype(jnp.bfloat16)
    probs_grad = jnp.einsum(
        "sqhd,skhd->shqk", attended_grad, value_heads, preferred_element_type=jnp.float32
    )
    values_grad = jnp.einsum(
        "shqk,sqhd->skhd", probs_again, attended_grad, preferred_element_type=jnp.float32
    )
    values_grad = values_grad.astype(jnp.bfloat16).reshape(row_count, width)
    inner_sum = jnp.sum(probs * probs_grad, axis=-1, keepdims=True)
    scores_grad = (probs * (probs_grad - inner_sum)).astype(jnp.bfloat16)
    query_grad = jnp.einsum(
        "shqk,skhd->sqhd", scores_grad, key_heads, preferred_element_type=jnp.float32
    )
    query_grad = (query_grad * scale).astype(jnp.bfloat16).reshape(row_count, width)
    keys_grad = jnp.einsum(
        "shqk,sqhd->skhd", scores_grad, query_heads, preferred_element_type=jnp.float32
    )
    keys_grad = (keys_grad * scale).astype(jnp.bfloat16).reshape(row_count, width)
    grad_query = weight_grad(flat_in, query_grad)
    grad_query_bias = column_sum(query_grad)
    grad_key = weight_grad(flat_in, keys_grad)
    grad_value = weight_grad(flat_in, values_grad)
    value_bias_gradient = column_sum(values_grad)
    grad_input = (
        grad_residual
        + reverse_projection(query_grad, query_weight)
        + reverse_projection(keys_grad, key_weight)
        + reverse_projection(values_grad, value_weight)
    )
    with jax.named_scope("scatter_qkv"):
        qkv_pack = jnp.concatenate(
            [
                grad_query,
                grad_key,
                grad_value,
                pack_vectors(width, (grad_query_bias, value_bias_gradient), jnp.float32),
            ],
            axis=1,
        )
        qkv_pack, late_own = lax.optimization_barrier((qkv_pack, late_own))
        qkv_own = scatter_rows(qkv_pack)
    grad_query_own = qkv_own[:, 0:width]
    grad_key_own = qkv_own[:, width : 2 * width]
    grad_value_own = qkv_own[:, 2 * width : 3 * width]
    grad_query_bias_own, value_bias_gradient_own = unpack_vectors(
        qkv_own[:, 3 * width :], (1, 1)
    )
    return (
        output.astype(jnp.bfloat16).reshape(inputs.shape),
        grad_input.astype(jnp.bfloat16).reshape(inputs.shape),
        grad_query_own,
        grad_query_bias_own,
        grad_key_own,
        grad_value_own,
        value_bias_gradient_own,
        grad_out_own,
        grad_out_bias_own,
        grad_gain1_own,
        grad_shift1_own,
        grad_up_own,
        grad_up_bias_own,
        grad_down_own,
        grad_down_bias_own,
        grad_gain2_own,
        grad_shift2_own,
    )


def solution(mesh):
    rows3 = P(AXES, None, None)
    rows2 = P(AXES, None)
    rows1 = P(AXES)
    return jax.shard_map(
        body,
        mesh=mesh,
        in_specs=(
            rows3,
            rows1,
            rows2,
            rows3,
            rows2,
            rows1,
            rows2,
            rows2,
            rows1,
            rows2,
            rows1,
            rows1,
            rows1,
            rows2,
            rows1,
            rows2,
            rows1,
            rows1,
            rows1,
        ),
        out_specs=(
            rows3,
            rows3,
            rows2,
            rows1,
            rows2,
            rows2,
            rows1,
            rows2,
            rows1,
            rows1,
            rows1,
            rows2,
            rows1,
            rows2,
            rows1,
            rows1,
            rows1,
        ),
        check_vma=False,
    )
```

```python
import jax
import jax.numpy as jnp
from jax import lax
from jax.sharding import PartitionSpec as P

HD = 64
EPSILON = 1e-06
AXES = ("fsdp", "sub")
GRAD_WIRE = jnp.bfloat16
VEC_COLS = 256


def layer_norm(values, gain, shift):
    average = jnp.mean(values, axis=-1, keepdims=True)
    centered = values - average
    variance = jnp.mean(centered * centered, axis=-1, keepdims=True)
    return centered * lax.rsqrt(variance + EPSILON) * gain + shift


def gelu_exact(values):
    return jax.nn.gelu(values, approximate=False)


def project(rows_low, weight):
    return jnp.dot(rows_low, weight, preferred_element_type=jnp.float32)


def reverse_projection(grad_low, weight):
    return lax.dot_general(
        grad_low, weight, (((1,), (1,)), ((), ())), preferred_element_type=jnp.float32
    )


def weight_grad(rows_low, grad_low):
    return lax.dot_general(
        rows_low, grad_low, (((0,), (0,)), ((), ())), preferred_element_type=jnp.float32
    )


def column_sum(grad_low):
    return jnp.sum(grad_low.astype(jnp.float32), axis=0)


def attention_scores(query_heads, key_heads, valid_keys, scale):
    scores = (
        jnp.einsum("sqhd,skhd->shqk", query_heads, key_heads, preferred_element_type=jnp.float32)
        * scale
    )
    return jnp.where(valid_keys[:, None, None, :], scores, -1e30)


def pack_vectors(rows, vectors, dtype):
    cols = [v.reshape(rows, -1).astype(dtype) for v in vectors]
    block = jnp.concatenate(cols, axis=1)
    return jnp.pad(block, ((0, 0), (0, VEC_COLS - block.shape[1])))


def unpack_vectors(block, widths):
    out, at = [], 0
    for width in widths:
        out.append(block[:, at : at + width].reshape(-1))
        at += width
    return out


def gather_rows(pack):
    return lax.all_gather(pack, AXES, axis=0, tiled=True)


def scatter_rows(pack):
    return lax.psum_scatter(pack.astype(GRAD_WIRE), AXES, scatter_dimension=0, tiled=True).astype(
        jnp.float32
    )


def tree_scatter(full):
    n_sub = lax.axis_size("sub")
    n_f = lax.axis_size("fsdp")
    rows = full.shape[0] // (n_sub * n_f)
    acc = full.reshape(n_f, n_sub, rows, -1)
    core = lax.axis_index("sub")
    keep = lax.dynamic_index_in_dim(acc, core, 1, keepdims=False)
    send = lax.dynamic_index_in_dim(acc, 1 - core, 1, keepdims=False)
    acc = keep + lax.ppermute(send, "sub", [(0, 1), (1, 0)])
    chip = lax.axis_index("fsdp")
    bits = n_f.bit_length() - 1
    acc = acc.reshape((2,) * bits + (rows, -1))
    for j in range(bits):
        axis = bits - 1 - j
        bit = (chip >> j) & 1
        keep = lax.dynamic_index_in_dim(acc, bit, axis, keepdims=False)
        send = lax.dynamic_index_in_dim(acc, 1 - bit, axis, keepdims=False)
        pairs = [(g, g ^ (1 << j)) for g in range(n_f)]
        recv = lax.ppermute(send.astype(GRAD_WIRE), "fsdp", pairs)
        acc = keep + recv.astype(jnp.float32)
    return acc.reshape(rows, -1)


def body(
    inputs,
    lengths,
    positions,
    masked_output_gradient,
    w_query,
    b_query,
    w_key,
    w_value,
    b_value,
    w_out,
    b_out,
    gain_attn,
    shift_attn,
    w_up,
    b_up,
    w_down,
    b_down,
    gain_ffn,
    shift_ffn,
):
    seq_count, seq_slots, width = inputs.shape
    head_count = width // HD
    scale = HD ** (-0.5)
    row_count = seq_count * seq_slots
    head_shape = (seq_count, seq_slots, head_count, HD)
    shard_rows = w_query.shape[0]
    ff_ratio = w_down.shape[0] // shard_rows
    ff_width = w_up.shape[1]
    token_ids = jnp.arange(seq_slots, dtype=jnp.int32)
    valid_keys = token_ids[None, :] < lengths[:, None]

    with jax.named_scope("gather_attn"):
        attn_pack = jnp.concatenate(
            [
                w_query,
                w_key,
                w_value,
                w_out,
                pack_vectors(
                    shard_rows, (b_query, b_value, b_out, gain_attn, shift_attn), jnp.bfloat16
                ),
            ],
            axis=1,
        )
        attn_full = gather_rows(attn_pack)
    query_weight = attn_full[:, 0:width]
    key_weight = attn_full[:, width : 2 * width]
    value_weight = attn_full[:, 2 * width : 3 * width]
    out_weight = attn_full[:, 3 * width : 4 * width]
    query_bias, value_bias, out_bias, norm1_gain, norm1_shift = unpack_vectors(
        attn_full[:, 4 * width :], (1, 1, 1, 1, 1)
    )

    with jax.named_scope("gather_ffn"):
        ffn_pack = jnp.concatenate(
            [
                w_up,
                w_down.reshape(shard_rows, ff_ratio * width),
                pack_vectors(
                    shard_rows, (b_up, b_down, gain_ffn, shift_ffn), jnp.bfloat16
                ),
            ],
            axis=1,
        )
        ffn_full = gather_rows(ffn_pack)
    up_weight = ffn_full[:, 0:ff_width]
    down_weight = ffn_full[:, ff_width : 2 * ff_width].reshape(ff_width, width)
    up_bias, downward_bias, norm2_gain, norm2_shift = unpack_vectors(
        ffn_full[:, 2 * ff_width :], (ff_ratio, 1, 1, 1)
    )

    flat_in = inputs.reshape(row_count, width)
    input_rows = flat_in.astype(jnp.float32)
    query_low = (project(flat_in, query_weight) + query_bias.astype(jnp.float32)).astype(
        jnp.bfloat16
    )
    keys_low = project(flat_in, key_weight).astype(jnp.bfloat16)
    values_low = (project(flat_in, value_weight) + value_bias.astype(jnp.float32)).astype(
        jnp.bfloat16
    )
    query_heads = query_low.reshape(head_shape)
    key_heads = keys_low.reshape(head_shape)
    value_heads = values_low.reshape(head_shape)
    scores = attention_scores(query_heads, key_heads, valid_keys, scale)
    row_top = jnp.max(scores, axis=-1, keepdims=True)
    expon = jnp.exp(scores - row_top)
    row_total = jnp.sum(expon, axis=-1, keepdims=True)
    log_total = row_top + jnp.log(row_total)
    probs_low = (expon / row_total).astype(jnp.bfloat16)
    attention_mixed = jnp.einsum(
        "shqk,skhd->sqhd", probs_low, value_heads, preferred_element_type=jnp.float32
    )
    attended_low = attention_mixed.reshape(row_count, width).astype(jnp.bfloat16)
    branch = project(attended_low, out_weight) + out_bias.astype(jnp.float32)
    middle, norm1_pull = jax.vjp(
        layer_norm,
        input_rows + branch,
        norm1_gain.astype(jnp.float32),
        norm1_shift.astype(jnp.float32),
    )
    middle_low = middle.astype(jnp.bfloat16)
    hidden = project(middle_low, up_weight) + up_bias.astype(jnp.float32)
    active, gelu_pull = jax.vjp(gelu_exact, hidden)
    active_low = active.astype(jnp.bfloat16)
    second_branch = project(active_low, down_weight) + downward_bias.astype(jnp.float32)
    output, norm2_pull = jax.vjp(
        layer_norm,
        middle + second_branch,
        norm2_gain.astype(jnp.float32),
        norm2_shift.astype(jnp.float32),
    )
    position_matches = (positions[:, :, None] == token_ids[None, None, :]).astype(jnp.bfloat16)
    cotangent = jnp.einsum(
        "efw,efv->ewv", position_matches, masked_output_gradient, preferred_element_type=jnp.float32
    ).reshape(row_count, width)
    grad_sum2, grad_gain2, grad_shift2 = norm2_pull(cotangent)
    second_grad = grad_sum2.astype(jnp.bfloat16)
    grad_down = weight_grad(active_low, second_grad)
    grad_down_bias = column_sum(second_grad)
    (grad_hidden,) = gelu_pull(reverse_projection(second_grad, down_weight))
    hidden_grad = grad_hidden.astype(jnp.bfloat16)
    grad_up = weight_grad(middle_low, hidden_grad)
    grad_up_bias = column_sum(hidden_grad)
    grad_middle = grad_sum2 + reverse_projection(hidden_grad, up_weight)
    grad_residual, grad_gain1, grad_shift1 = norm1_pull(grad_middle)
    branch_grad = grad_residual.astype(jnp.bfloat16)
    grad_out = weight_grad(attended_low, branch_grad)
    grad_out_bias = column_sum(branch_grad)

    with jax.named_scope("scatter_late"):
        late_pack = jnp.concatenate(
            [
                grad_up,
                grad_down.reshape(width, ff_ratio * width),
                grad_out,
                pack_vectors(
                    width,
                    (
                        grad_up_bias,
                        grad_down_bias,
                        grad_gain2,
                        grad_shift2,
                        grad_out_bias,
                        grad_gain1,
                        grad_shift1,
                    ),
                    jnp.float32,
                ),
            ],
            axis=1,
        )
        late_pack, branch_grad = lax.optimization_barrier((late_pack, branch_grad))
        late_own = scatter_rows(late_pack)
    grad_up_own = late_own[:, 0:ff_width]
    grad_down_own = late_own[:, ff_width : 2 * ff_width].reshape(shard_rows * ff_ratio, width)
    grad_out_own = late_own[:, 2 * ff_width : 2 * ff_width + width]
    (
        grad_up_bias_own,
        grad_down_bias_own,
        grad_gain2_own,
        grad_shift2_own,
        grad_out_bias_own,
        grad_gain1_own,
        grad_shift1_own,
    ) = unpack_vectors(late_own[:, 2 * ff_width + width :], (ff_ratio, 1, 1, 1, 1, 1, 1))

    attended_grad = (
        reverse_projection(branch_grad, out_weight).astype(jnp.bfloat16).reshape(head_shape)
    )
    scores_again = attention_scores(query_heads, key_heads, valid_keys, scale)
    probs = jnp.exp(scores_again - log_total)
    probs_again = probs.astype(jnp.bfloat16)
    probs_grad = jnp.einsum(
        "sqhd,skhd->shqk", attended_grad, value_heads, preferred_element_type=jnp.float32
    )
    values_grad = jnp.einsum(
        "shqk,sqhd->skhd", probs_again, attended_grad, preferred_element_type=jnp.float32
    )
    values_grad = values_grad.astype(jnp.bfloat16).reshape(row_count, width)
    inner_sum = jnp.sum(probs * probs_grad, axis=-1, keepdims=True)
    scores_grad = (probs * (probs_grad - inner_sum)).astype(jnp.bfloat16)
    query_grad = jnp.einsum(
        "shqk,skhd->sqhd", scores_grad, key_heads, preferred_element_type=jnp.float32
    )
    query_grad = (query_grad * scale).astype(jnp.bfloat16).reshape(row_count, width)
    keys_grad = jnp.einsum(
        "shqk,sqhd->skhd", scores_grad, query_heads, preferred_element_type=jnp.float32
    )
    keys_grad = (keys_grad * scale).astype(jnp.bfloat16).reshape(row_count, width)
    grad_query = weight_grad(flat_in, query_grad)
    grad_query_bias = column_sum(query_grad)
    grad_key = weight_grad(flat_in, keys_grad)
    grad_value = weight_grad(flat_in, values_grad)
    value_bias_gradient = column_sum(values_grad)
    grad_input = (
        grad_residual
        + reverse_projection(query_grad, query_weight)
        + reverse_projection(keys_grad, key_weight)
        + reverse_projection(values_grad, value_weight)
    )
    with jax.named_scope("scatter_qkv"):
        qkv_pack = jnp.concatenate(
            [
                grad_query,
                grad_key,
                grad_value,
                pack_vectors(width, (grad_query_bias, value_bias_gradient), jnp.float32),
            ],
            axis=1,
        )
        qkv_own = tree_scatter(qkv_pack)
    grad_query_own = qkv_own[:, 0:width]
    grad_key_own = qkv_own[:, width : 2 * width]
    grad_value_own = qkv_own[:, 2 * width : 3 * width]
    grad_query_bias_own, value_bias_gradient_own = unpack_vectors(
        qkv_own[:, 3 * width :], (1, 1)
    )
    return (
        output.astype(jnp.bfloat16).reshape(inputs.shape),
        grad_input.astype(jnp.bfloat16).reshape(inputs.shape),
        grad_query_own,
        grad_query_bias_own,
        grad_key_own,
        grad_value_own,
        value_bias_gradient_own,
        grad_out_own,
        grad_out_bias_own,
        grad_gain1_own,
        grad_shift1_own,
        grad_up_own,
        grad_up_bias_own,
        grad_down_own,
        grad_down_bias_own,
        grad_gain2_own,
        grad_shift2_own,
    )


def solution(mesh):
    rows3 = P(AXES, None, None)
    rows2 = P(AXES, None)
    rows1 = P(AXES)
    return jax.shard_map(
        body,
        mesh=mesh,
        in_specs=(
            rows3,
            rows1,
            rows2,
            rows3,
            rows2,
            rows1,
            rows2,
            rows2,
            rows1,
            rows2,
            rows1,
            rows1,
            rows1,
            rows2,
            rows1,
            rows2,
            rows1,
            rows1,
            rows1,
        ),
        out_specs=(
            rows3,
            rows3,
            rows2,
            rows1,
            rows2,
            rows2,
            rows1,
            rows2,
            rows1,
            rows1,
            rows1,
            rows2,
            rows1,
            rows2,
            rows1,
            rows1,
            rows1,
        ),
        check_vma=False,
    )
```

```python
import jax
import jax.numpy as jnp
from jax import lax
from jax.sharding import PartitionSpec as P

HD = 64
EPSILON = 1e-06
AXES = ("fsdp", "sub")
GRAD_WIRE = jnp.bfloat16
VEC_COLS = 256


def layer_norm(values, gain, shift):
    average = jnp.mean(values, axis=-1, keepdims=True)
    centered = values - average
    variance = jnp.mean(centered * centered, axis=-1, keepdims=True)
    return centered * lax.rsqrt(variance + EPSILON) * gain + shift


def gelu_exact(values):
    return jax.nn.gelu(values, approximate=False)


def project(rows_low, weight):
    return jnp.dot(rows_low, weight, preferred_element_type=jnp.float32)


def reverse_projection(grad_low, weight):
    return lax.dot_general(
        grad_low, weight, (((1,), (1,)), ((), ())), preferred_element_type=jnp.float32
    )


def weight_grad(rows_low, grad_low):
    return lax.dot_general(
        rows_low, grad_low, (((0,), (0,)), ((), ())), preferred_element_type=jnp.float32
    )


def column_sum(grad_low):
    return jnp.sum(grad_low.astype(jnp.float32), axis=0)


def attention_scores(query_heads, key_heads, valid_keys, scale):
    scores = (
        jnp.einsum("sqhd,skhd->shqk", query_heads, key_heads, preferred_element_type=jnp.float32)
        * scale
    )
    return jnp.where(valid_keys[:, None, None, :], scores, -1e30)


def pack_vectors(rows, vectors, dtype):
    cols = [v.reshape(rows, -1).astype(dtype) for v in vectors]
    block = jnp.concatenate(cols, axis=1)
    return jnp.pad(block, ((0, 0), (0, VEC_COLS - block.shape[1])))


def unpack_vectors(block, widths):
    out, at = [], 0
    for width in widths:
        out.append(block[:, at : at + width].reshape(-1))
        at += width
    return out


def gather_rows(pack):
    return lax.all_gather(pack, AXES, axis=0, tiled=True)


def scatter_rows(pack):
    return lax.psum_scatter(pack.astype(GRAD_WIRE), AXES, scatter_dimension=0, tiled=True).astype(
        jnp.float32
    )


def _pick(bit, first, second):
    return jnp.where(bit == 0, first, second), jnp.where(bit == 0, second, first)


def tree_gather(block, last_bit):
    n_sub = lax.axis_size("sub")
    n_f = lax.axis_size("fsdp")
    bits = n_f.bit_length() - 1
    chip = lax.axis_index("fsdp")
    order = [b for b in range(bits - 1, -1, -1) if b != last_bit] + [last_bit]
    acc = block
    done = []
    for j in order:
        pairs = [(g, g ^ (1 << j)) for g in range(n_f)]
        recv = lax.ppermute(acc, "fsdp", pairs)
        bit = (chip >> j) & 1
        lo, hi = _pick(bit, acc, recv)
        axis = sum(1 for b in done if b > j)
        acc = jnp.stack([lo, hi], axis=axis)
        done.append(j)
    acc = acc.reshape((n_f,) + block.shape)
    core = lax.axis_index("sub")
    recv = lax.ppermute(acc, "sub", [(0, 1), (1, 0)])
    lo, hi = _pick(core, acc, recv)
    full = jnp.stack([lo, hi], axis=1)
    return full.reshape((n_f * n_sub * block.shape[0],) + block.shape[1:])


def tree_scatter(full, first_bit):
    n_sub = lax.axis_size("sub")
    n_f = lax.axis_size("fsdp")
    rows = full.shape[0] // (n_sub * n_f)
    acc = full.reshape(n_f, n_sub, rows, -1)
    core = lax.axis_index("sub")
    keep = lax.dynamic_index_in_dim(acc, core, 1, keepdims=False)
    send = lax.dynamic_index_in_dim(acc, 1 - core, 1, keepdims=False)
    acc = keep + lax.ppermute(send, "sub", [(0, 1), (1, 0)])
    chip = lax.axis_index("fsdp")
    bits = n_f.bit_length() - 1
    acc = acc.reshape((2,) * bits + (rows, -1))
    left = list(range(bits - 1, -1, -1))
    order = [first_bit] + [b for b in range(bits) if b != first_bit]
    for j in order:
        axis = left.index(j)
        left.remove(j)
        bit = (chip >> j) & 1
        keep = lax.dynamic_index_in_dim(acc, bit, axis, keepdims=False)
        send = lax.dynamic_index_in_dim(acc, 1 - bit, axis, keepdims=False)
        pairs = [(g, g ^ (1 << j)) for g in range(n_f)]
        recv = lax.ppermute(send.astype(GRAD_WIRE), "fsdp", pairs)
        acc = keep + recv.astype(jnp.float32)
    return acc.reshape(rows, -1)


def body(
    inputs,
    lengths,
    positions,
    masked_output_gradient,
    w_query,
    b_query,
    w_key,
    w_value,
    b_value,
    w_out,
    b_out,
    gain_attn,
    shift_attn,
    w_up,
    b_up,
    w_down,
    b_down,
    gain_ffn,
    shift_ffn,
):
    seq_count, seq_slots, width = inputs.shape
    head_count = width // HD
    scale = HD ** (-0.5)
    row_count = seq_count * seq_slots
    head_shape = (seq_count, seq_slots, head_count, HD)
    shard_rows = w_query.shape[0]
    ff_ratio = w_down.shape[0] // shard_rows
    ff_width = w_up.shape[1]
    token_ids = jnp.arange(seq_slots, dtype=jnp.int32)
    valid_keys = token_ids[None, :] < lengths[:, None]

    with jax.named_scope("gather_attn"):
        vec_pack = pack_vectors(
            shard_rows, (b_query, b_value, b_out, gain_attn, shift_attn), jnp.bfloat16
        )
        query_part = tree_gather(jnp.concatenate([w_query, vec_pack], axis=1), 0)
        kv_part = tree_gather(jnp.concatenate([w_key, w_value], axis=1), 1)
        out_weight = tree_gather(w_out, 2)
    query_weight = query_part[:, 0:width]
    key_weight = kv_part[:, 0:width]
    value_weight = kv_part[:, width : 2 * width]
    query_bias, value_bias, out_bias, norm1_gain, norm1_shift = unpack_vectors(
        query_part[:, width:], (1, 1, 1, 1, 1)
    )

    with jax.named_scope("gather_ffn"):
        ffn_pack = jnp.concatenate(
            [
                w_up,
                w_down.reshape(shard_rows, ff_ratio * width),
                pack_vectors(
                    shard_rows, (b_up, b_down, gain_ffn, shift_ffn), jnp.bfloat16
                ),
            ],
            axis=1,
        )
        ffn_full = gather_rows(ffn_pack)
    up_weight = ffn_full[:, 0:ff_width]
    down_weight = ffn_full[:, ff_width : 2 * ff_width].reshape(ff_width, width)
    up_bias, downward_bias, norm2_gain, norm2_shift = unpack_vectors(
        ffn_full[:, 2 * ff_width :], (ff_ratio, 1, 1, 1)
    )

    flat_in = inputs.reshape(row_count, width)
    input_rows = flat_in.astype(jnp.float32)
    query_low = (project(flat_in, query_weight) + query_bias.astype(jnp.float32)).astype(
        jnp.bfloat16
    )
    keys_low = project(flat_in, key_weight).astype(jnp.bfloat16)
    values_low = (project(flat_in, value_weight) + value_bias.astype(jnp.float32)).astype(
        jnp.bfloat16
    )
    query_heads = query_low.reshape(head_shape)
    key_heads = keys_low.reshape(head_shape)
    value_heads = values_low.reshape(head_shape)
    scores = attention_scores(query_heads, key_heads, valid_keys, scale)
    row_top = jnp.max(scores, axis=-1, keepdims=True)
    expon = jnp.exp(scores - row_top)
    row_total = jnp.sum(expon, axis=-1, keepdims=True)
    log_total = row_top + jnp.log(row_total)
    probs_low = (expon / row_total).astype(jnp.bfloat16)
    attention_mixed = jnp.einsum(
        "shqk,skhd->sqhd", probs_low, value_heads, preferred_element_type=jnp.float32
    )
    attended_low = attention_mixed.reshape(row_count, width).astype(jnp.bfloat16)
    branch = project(attended_low, out_weight) + out_bias.astype(jnp.float32)
    middle, norm1_pull = jax.vjp(
        layer_norm,
        input_rows + branch,
        norm1_gain.astype(jnp.float32),
        norm1_shift.astype(jnp.float32),
    )
    middle_low = middle.astype(jnp.bfloat16)
    hidden = project(middle_low, up_weight) + up_bias.astype(jnp.float32)
    active, gelu_pull = jax.vjp(gelu_exact, hidden)
    active_low = active.astype(jnp.bfloat16)
    second_branch = project(active_low, down_weight) + downward_bias.astype(jnp.float32)
    output, norm2_pull = jax.vjp(
        layer_norm,
        middle + second_branch,
        norm2_gain.astype(jnp.float32),
        norm2_shift.astype(jnp.float32),
    )
    position_matches = (positions[:, :, None] == token_ids[None, None, :]).astype(jnp.bfloat16)
    cotangent = jnp.einsum(
        "efw,efv->ewv", position_matches, masked_output_gradient, preferred_element_type=jnp.float32
    ).reshape(row_count, width)
    grad_sum2, grad_gain2, grad_shift2 = norm2_pull(cotangent)
    second_grad = grad_sum2.astype(jnp.bfloat16)
    grad_down = weight_grad(active_low, second_grad)
    grad_down_bias = column_sum(second_grad)
    (grad_hidden,) = gelu_pull(reverse_projection(second_grad, down_weight))
    hidden_grad = grad_hidden.astype(jnp.bfloat16)
    grad_up = weight_grad(middle_low, hidden_grad)
    grad_up_bias = column_sum(hidden_grad)
    grad_middle = grad_sum2 + reverse_projection(hidden_grad, up_weight)
    grad_residual, grad_gain1, grad_shift1 = norm1_pull(grad_middle)
    branch_grad = grad_residual.astype(jnp.bfloat16)
    grad_out = weight_grad(attended_low, branch_grad)
    grad_out_bias = column_sum(branch_grad)

    with jax.named_scope("scatter_late"):
        late_pack = jnp.concatenate(
            [
                grad_up,
                grad_down.reshape(width, ff_ratio * width),
                grad_out,
                pack_vectors(
                    width,
                    (
                        grad_up_bias,
                        grad_down_bias,
                        grad_gain2,
                        grad_shift2,
                        grad_out_bias,
                        grad_gain1,
                        grad_shift1,
                    ),
                    jnp.float32,
                ),
            ],
            axis=1,
        )
        late_pack, branch_grad = lax.optimization_barrier((late_pack, branch_grad))
        late_own = scatter_rows(late_pack)
    grad_up_own = late_own[:, 0:ff_width]
    grad_down_own = late_own[:, ff_width : 2 * ff_width].reshape(shard_rows * ff_ratio, width)
    grad_out_own = late_own[:, 2 * ff_width : 2 * ff_width + width]
    (
        grad_up_bias_own,
        grad_down_bias_own,
        grad_gain2_own,
        grad_shift2_own,
        grad_out_bias_own,
        grad_gain1_own,
        grad_shift1_own,
    ) = unpack_vectors(late_own[:, 2 * ff_width + width :], (ff_ratio, 1, 1, 1, 1, 1, 1))

    attended_grad = (
        reverse_projection(branch_grad, out_weight).astype(jnp.bfloat16).reshape(head_shape)
    )
    scores_again = attention_scores(query_heads, key_heads, valid_keys, scale)
    probs = jnp.exp(scores_again - log_total)
    probs_again = probs.astype(jnp.bfloat16)
    probs_grad = jnp.einsum(
        "sqhd,skhd->shqk", attended_grad, value_heads, preferred_element_type=jnp.float32
    )
    values_grad = jnp.einsum(
        "shqk,sqhd->skhd", probs_again, attended_grad, preferred_element_type=jnp.float32
    )
    values_grad = values_grad.astype(jnp.bfloat16).reshape(row_count, width)
    inner_sum = jnp.sum(probs * probs_grad, axis=-1, keepdims=True)
    scores_grad = (probs * (probs_grad - inner_sum)).astype(jnp.bfloat16)
    query_grad = jnp.einsum(
        "shqk,skhd->sqhd", scores_grad, key_heads, preferred_element_type=jnp.float32
    )
    query_grad = (query_grad * scale).astype(jnp.bfloat16).reshape(row_count, width)
    keys_grad = jnp.einsum(
        "shqk,sqhd->skhd", scores_grad, query_heads, preferred_element_type=jnp.float32
    )
    keys_grad = (keys_grad * scale).astype(jnp.bfloat16).reshape(row_count, width)
    grad_query = weight_grad(flat_in, query_grad)
    grad_query_bias = column_sum(query_grad)
    grad_key = weight_grad(flat_in, keys_grad)
    grad_value = weight_grad(flat_in, values_grad)
    value_bias_gradient = column_sum(values_grad)
    grad_input = (
        grad_residual
        + reverse_projection(query_grad, query_weight)
        + reverse_projection(keys_grad, key_weight)
        + reverse_projection(values_grad, value_weight)
    )
    with jax.named_scope("scatter_qkv"):
        query_own_pack = tree_scatter(
            jnp.concatenate(
                [
                    grad_query,
                    pack_vectors(width, (grad_query_bias, value_bias_gradient), jnp.float32),
                ],
                axis=1,
            ),
            0,
        )
        grad_key_own = tree_scatter(grad_key, 1)
        grad_value_own = tree_scatter(grad_value, 2)
    grad_query_own = query_own_pack[:, 0:width]
    grad_query_bias_own, value_bias_gradient_own = unpack_vectors(
        query_own_pack[:, width:], (1, 1)
    )
    return (
        output.astype(jnp.bfloat16).reshape(inputs.shape),
        grad_input.astype(jnp.bfloat16).reshape(inputs.shape),
        grad_query_own,
        grad_query_bias_own,
        grad_key_own,
        grad_value_own,
        value_bias_gradient_own,
        grad_out_own,
        grad_out_bias_own,
        grad_gain1_own,
        grad_shift1_own,
        grad_up_own,
        grad_up_bias_own,
        grad_down_own,
        grad_down_bias_own,
        grad_gain2_own,
        grad_shift2_own,
    )


def solution(mesh):
    rows3 = P(AXES, None, None)
    rows2 = P(AXES, None)
    rows1 = P(AXES)
    return jax.shard_map(
        body,
        mesh=mesh,
        in_specs=(
            rows3,
            rows1,
            rows2,
            rows3,
            rows2,
            rows1,
            rows2,
            rows2,
            rows1,
            rows2,
            rows1,
            rows1,
            rows1,
            rows2,
            rows1,
            rows2,
            rows1,
            rows1,
            rows1,
        ),
        out_specs=(
            rows3,
            rows3,
            rows2,
            rows1,
            rows2,
            rows2,
            rows1,
            rows2,
            rows1,
            rows1,
            rows1,
            rows2,
            rows1,
            rows2,
            rows1,
            rows1,
            rows1,
        ),
        check_vma=False,
    )
```

```python
import jax
import jax.numpy as jnp
from jax import lax
from jax.sharding import PartitionSpec as P

HD = 64
EPSILON = 1e-06
AXES = ("fsdp", "sub")
GRAD_WIRE = jnp.bfloat16
VEC_COLS = 256


def layer_norm(values, gain, shift):
    average = jnp.mean(values, axis=-1, keepdims=True)
    centered = values - average
    variance = jnp.mean(centered * centered, axis=-1, keepdims=True)
    return centered * lax.rsqrt(variance + EPSILON) * gain + shift


def gelu_exact(values):
    return values * (0.5 * (1.0 + lax.erf(values * (2.0 ** -0.5))))


def project(rows_low, weight):
    return jnp.dot(rows_low, weight, preferred_element_type=jnp.float32)


def reverse_projection(grad_low, weight):
    return lax.dot_general(
        grad_low, weight, (((1,), (1,)), ((), ())), preferred_element_type=jnp.float32
    )


def weight_grad(rows_low, grad_low):
    return lax.dot_general(
        rows_low, grad_low, (((0,), (0,)), ((), ())), preferred_element_type=jnp.float32
    )


def column_sum(grad_low):
    return jnp.sum(grad_low.astype(jnp.float32), axis=0)


def attention_scores(query_heads, key_heads, valid_keys, scale):
    scores = (
        jnp.einsum("sqhd,skhd->shqk", query_heads, key_heads, preferred_element_type=jnp.float32)
        * scale
    )
    return jnp.where(valid_keys[:, None, None, :], scores, -1e30)


def pack_vectors(rows, vectors, dtype):
    cols = [v.reshape(rows, -1).astype(dtype) for v in vectors]
    block = jnp.concatenate(cols, axis=1)
    return jnp.pad(block, ((0, 0), (0, VEC_COLS - block.shape[1])))


def unpack_vectors(block, widths):
    out, at = [], 0
    for width in widths:
        out.append(block[:, at : at + width].reshape(-1))
        at += width
    return out


def gather_rows(pack):
    return lax.all_gather(pack, AXES, axis=0, tiled=True)


def scatter_rows(pack):
    return lax.psum_scatter(pack.astype(GRAD_WIRE), AXES, scatter_dimension=0, tiled=True).astype(
        jnp.float32
    )


def _pick(bit, first, second):
    return jnp.where(bit == 0, first, second), jnp.where(bit == 0, second, first)


def tree_gather(block, last_bit):
    n_sub = lax.axis_size("sub")
    n_f = lax.axis_size("fsdp")
    bits = n_f.bit_length() - 1
    chip = lax.axis_index("fsdp")
    order = [b for b in range(bits - 1, -1, -1) if b != last_bit] + [last_bit]
    acc = block
    done = []
    for j in order:
        pairs = [(g, g ^ (1 << j)) for g in range(n_f)]
        recv = lax.ppermute(acc, "fsdp", pairs)
        bit = (chip >> j) & 1
        lo, hi = _pick(bit, acc, recv)
        axis = sum(1 for b in done if b > j)
        acc = jnp.stack([lo, hi], axis=axis)
        done.append(j)
    acc = acc.reshape((n_f,) + block.shape)
    core = lax.axis_index("sub")
    recv = lax.ppermute(acc, "sub", [(0, 1), (1, 0)])
    lo, hi = _pick(core, acc, recv)
    full = jnp.stack([lo, hi], axis=1)
    return full.reshape((n_f * n_sub * block.shape[0],) + block.shape[1:])


def tree_scatter(full, first_bit):
    n_sub = lax.axis_size("sub")
    n_f = lax.axis_size("fsdp")
    rows = full.shape[0] // (n_sub * n_f)
    acc = full.reshape(n_f, n_sub, rows, -1)
    core = lax.axis_index("sub")
    keep = lax.dynamic_index_in_dim(acc, core, 1, keepdims=False)
    send = lax.dynamic_index_in_dim(acc, 1 - core, 1, keepdims=False)
    acc = keep + lax.ppermute(send, "sub", [(0, 1), (1, 0)])
    chip = lax.axis_index("fsdp")
    bits = n_f.bit_length() - 1
    acc = acc.reshape((2,) * bits + (rows, -1))
    left = list(range(bits - 1, -1, -1))
    order = [first_bit] + [b for b in range(bits) if b != first_bit]
    for j in order:
        axis = left.index(j)
        left.remove(j)
        bit = (chip >> j) & 1
        keep = lax.dynamic_index_in_dim(acc, bit, axis, keepdims=False)
        send = lax.dynamic_index_in_dim(acc, 1 - bit, axis, keepdims=False)
        pairs = [(g, g ^ (1 << j)) for g in range(n_f)]
        recv = lax.ppermute(send.astype(GRAD_WIRE), "fsdp", pairs)
        acc = keep + recv.astype(jnp.float32)
    return acc.reshape(rows, -1)


def body(
    inputs,
    lengths,
    positions,
    masked_output_gradient,
    w_query,
    b_query,
    w_key,
    w_value,
    b_value,
    w_out,
    b_out,
    gain_attn,
    shift_attn,
    w_up,
    b_up,
    w_down,
    b_down,
    gain_ffn,
    shift_ffn,
):
    seq_count, seq_slots, width = inputs.shape
    head_count = width // HD
    scale = HD ** (-0.5)
    row_count = seq_count * seq_slots
    head_shape = (seq_count, seq_slots, head_count, HD)
    shard_rows = w_query.shape[0]
    ff_ratio = w_down.shape[0] // shard_rows
    ff_width = w_up.shape[1]
    token_ids = jnp.arange(seq_slots, dtype=jnp.int32)
    valid_keys = token_ids[None, :] < lengths[:, None]

    with jax.named_scope("gather_attn"):
        vec_pack = pack_vectors(
            shard_rows, (b_query, b_value, b_out, gain_attn, shift_attn), jnp.bfloat16
        )
        query_part = tree_gather(jnp.concatenate([w_query, vec_pack], axis=1), 0)
        kv_part = tree_gather(jnp.concatenate([w_key, w_value], axis=1), 1)
        out_weight = tree_gather(w_out, 2)
    query_weight = query_part[:, 0:width]
    key_weight = kv_part[:, 0:width]
    value_weight = kv_part[:, width : 2 * width]
    query_bias, value_bias, out_bias, norm1_gain, norm1_shift = unpack_vectors(
        query_part[:, width:], (1, 1, 1, 1, 1)
    )

    with jax.named_scope("gather_ffn"):
        ffn_pack = jnp.concatenate(
            [
                w_up,
                w_down.reshape(shard_rows, ff_ratio * width),
                pack_vectors(
                    shard_rows, (b_up, b_down, gain_ffn, shift_ffn), jnp.bfloat16
                ),
            ],
            axis=1,
        )
        ffn_full = gather_rows(ffn_pack)
    up_weight = ffn_full[:, 0:ff_width]
    down_weight = ffn_full[:, ff_width : 2 * ff_width].reshape(ff_width, width)
    up_bias, downward_bias, norm2_gain, norm2_shift = unpack_vectors(
        ffn_full[:, 2 * ff_width :], (ff_ratio, 1, 1, 1)
    )

    flat_in = inputs.reshape(row_count, width)
    input_rows = flat_in.astype(jnp.float32)
    query_low = (project(flat_in, query_weight) + query_bias.astype(jnp.float32)).astype(
        jnp.bfloat16
    )
    keys_low = project(flat_in, key_weight).astype(jnp.bfloat16)
    values_low = (project(flat_in, value_weight) + value_bias.astype(jnp.float32)).astype(
        jnp.bfloat16
    )
    query_heads = query_low.reshape(head_shape)
    key_heads = keys_low.reshape(head_shape)
    value_heads = values_low.reshape(head_shape)
    scores = attention_scores(query_heads, key_heads, valid_keys, scale)
    row_top = jnp.max(scores, axis=-1, keepdims=True)
    expon = jnp.exp(scores - row_top)
    row_total = jnp.sum(expon, axis=-1, keepdims=True)
    log_total = row_top + jnp.log(row_total)
    probs_low = (expon / row_total).astype(jnp.bfloat16)
    attention_mixed = jnp.einsum(
        "shqk,skhd->sqhd", probs_low, value_heads, preferred_element_type=jnp.float32
    )
    attended_low = attention_mixed.reshape(row_count, width).astype(jnp.bfloat16)
    branch = project(attended_low, out_weight) + out_bias.astype(jnp.float32)
    middle, norm1_pull = jax.vjp(
        layer_norm,
        input_rows + branch,
        norm1_gain.astype(jnp.float32),
        norm1_shift.astype(jnp.float32),
    )
    middle_low = middle.astype(jnp.bfloat16)
    hidden = project(middle_low, up_weight) + up_bias.astype(jnp.float32)
    active, gelu_pull = jax.vjp(gelu_exact, hidden)
    active_low = active.astype(jnp.bfloat16)
    second_branch = project(active_low, down_weight) + downward_bias.astype(jnp.float32)
    output, norm2_pull = jax.vjp(
        layer_norm,
        middle + second_branch,
        norm2_gain.astype(jnp.float32),
        norm2_shift.astype(jnp.float32),
    )
    position_matches = (positions[:, :, None] == token_ids[None, None, :]).astype(jnp.bfloat16)
    cotangent = jnp.einsum(
        "efw,efv->ewv", position_matches, masked_output_gradient, preferred_element_type=jnp.float32
    ).reshape(row_count, width)
    grad_sum2, grad_gain2, grad_shift2 = norm2_pull(cotangent)
    second_grad = grad_sum2.astype(jnp.bfloat16)
    grad_down = weight_grad(active_low, second_grad)
    grad_down_bias = column_sum(second_grad)
    (grad_hidden,) = gelu_pull(reverse_projection(second_grad, down_weight))
    hidden_grad = grad_hidden.astype(jnp.bfloat16)
    grad_up = weight_grad(middle_low, hidden_grad)
    grad_up_bias = column_sum(hidden_grad)
    grad_middle = grad_sum2 + reverse_projection(hidden_grad, up_weight)
    grad_residual, grad_gain1, grad_shift1 = norm1_pull(grad_middle)
    branch_grad = grad_residual.astype(jnp.bfloat16)
    grad_out = weight_grad(attended_low, branch_grad)
    grad_out_bias = column_sum(branch_grad)

    with jax.named_scope("scatter_late"):
        late_pack = jnp.concatenate(
            [
                grad_up,
                grad_down.reshape(width, ff_ratio * width),
                grad_out,
                pack_vectors(
                    width,
                    (
                        grad_up_bias,
                        grad_down_bias,
                        grad_gain2,
                        grad_shift2,
                        grad_out_bias,
                        grad_gain1,
                        grad_shift1,
                    ),
                    jnp.float32,
                ),
            ],
            axis=1,
        )
        late_pack, branch_grad = lax.optimization_barrier((late_pack, branch_grad))
        late_own = scatter_rows(late_pack)
    grad_up_own = late_own[:, 0:ff_width]
    grad_down_own = late_own[:, ff_width : 2 * ff_width].reshape(shard_rows * ff_ratio, width)
    grad_out_own = late_own[:, 2 * ff_width : 2 * ff_width + width]
    (
        grad_up_bias_own,
        grad_down_bias_own,
        grad_gain2_own,
        grad_shift2_own,
        grad_out_bias_own,
        grad_gain1_own,
        grad_shift1_own,
    ) = unpack_vectors(late_own[:, 2 * ff_width + width :], (ff_ratio, 1, 1, 1, 1, 1, 1))

    attended_grad = (
        reverse_projection(branch_grad, out_weight).astype(jnp.bfloat16).reshape(head_shape)
    )
    scores_again = attention_scores(query_heads, key_heads, valid_keys, scale)
    probs = jnp.exp(scores_again - log_total)
    probs_again = probs.astype(jnp.bfloat16)
    probs_grad = jnp.einsum(
        "sqhd,skhd->shqk", attended_grad, value_heads, preferred_element_type=jnp.float32
    )
    values_grad = jnp.einsum(
        "shqk,sqhd->skhd", probs_again, attended_grad, preferred_element_type=jnp.float32
    )
    values_grad = values_grad.astype(jnp.bfloat16).reshape(row_count, width)
    inner_sum = jnp.sum(probs * probs_grad, axis=-1, keepdims=True)
    scores_grad = (probs * (probs_grad - inner_sum)).astype(jnp.bfloat16)
    query_grad = jnp.einsum(
        "shqk,skhd->sqhd", scores_grad, key_heads, preferred_element_type=jnp.float32
    )
    query_grad = (query_grad * scale).astype(jnp.bfloat16).reshape(row_count, width)
    keys_grad = jnp.einsum(
        "shqk,sqhd->skhd", scores_grad, query_heads, preferred_element_type=jnp.float32
    )
    keys_grad = (keys_grad * scale).astype(jnp.bfloat16).reshape(row_count, width)
    grad_query = weight_grad(flat_in, query_grad)
    grad_query_bias = column_sum(query_grad)
    grad_key = weight_grad(flat_in, keys_grad)
    grad_value = weight_grad(flat_in, values_grad)
    value_bias_gradient = column_sum(values_grad)
    grad_input = (
        grad_residual
        + reverse_projection(query_grad, query_weight)
        + reverse_projection(keys_grad, key_weight)
        + reverse_projection(values_grad, value_weight)
    )
    with jax.named_scope("scatter_qkv"):
        query_own_pack = tree_scatter(
            jnp.concatenate(
                [
                    grad_query,
                    pack_vectors(width, (grad_query_bias, value_bias_gradient), jnp.float32),
                ],
                axis=1,
            ),
            0,
        )
        grad_key_own = tree_scatter(grad_key, 1)
        grad_value_own = tree_scatter(grad_value, 2)
    grad_query_own = query_own_pack[:, 0:width]
    grad_query_bias_own, value_bias_gradient_own = unpack_vectors(
        query_own_pack[:, width:], (1, 1)
    )
    return (
        output.astype(jnp.bfloat16).reshape(inputs.shape),
        grad_input.astype(jnp.bfloat16).reshape(inputs.shape),
        grad_query_own,
        grad_query_bias_own,
        grad_key_own,
        grad_value_own,
        value_bias_gradient_own,
        grad_out_own,
        grad_out_bias_own,
        grad_gain1_own,
        grad_shift1_own,
        grad_up_own,
        grad_up_bias_own,
        grad_down_own,
        grad_down_bias_own,
        grad_gain2_own,
        grad_shift2_own,
    )


def solution(mesh):
    rows3 = P(AXES, None, None)
    rows2 = P(AXES, None)
    rows1 = P(AXES)
    return jax.shard_map(
        body,
        mesh=mesh,
        in_specs=(
            rows3,
            rows1,
            rows2,
            rows3,
            rows2,
            rows1,
            rows2,
            rows2,
            rows1,
            rows2,
            rows1,
            rows1,
            rows1,
            rows2,
            rows1,
            rows2,
            rows1,
            rows1,
            rows1,
        ),
        out_specs=(
            rows3,
            rows3,
            rows2,
            rows1,
            rows2,
            rows2,
            rows1,
            rows2,
            rows1,
            rows1,
            rows1,
            rows2,
            rows1,
            rows2,
            rows1,
            rows1,
            rows1,
        ),
        check_vma=False,
    )
```

```python
import jax
import jax.numpy as jnp
from jax import lax
from jax.sharding import PartitionSpec as P

HD = 64
EPSILON = 1e-06
AXES = ("fsdp", "sub")
GRAD_WIRE = jnp.bfloat16
VEC_COLS = 256


def layer_norm(values, gain, shift):
    average = jnp.mean(values, axis=-1, keepdims=True)
    centered = values - average
    variance = jnp.mean(centered * centered, axis=-1, keepdims=True)
    return centered * lax.rsqrt(variance + EPSILON) * gain + shift


def gelu_exact(values):
    return values * (0.5 * (1.0 + lax.erf(values * (2.0 ** -0.5))))


def project(rows_low, weight):
    return jnp.dot(rows_low, weight, preferred_element_type=jnp.float32)


def reverse_projection(grad_low, weight):
    return lax.dot_general(
        grad_low, weight, (((1,), (1,)), ((), ())), preferred_element_type=jnp.float32
    )


def weight_grad(rows_low, grad_low):
    return lax.dot_general(
        rows_low, grad_low, (((0,), (0,)), ((), ())), preferred_element_type=jnp.float32
    )


def column_sum(grad_low):
    return jnp.sum(grad_low.astype(jnp.float32), axis=0)


def attention_scores(query_heads, key_heads, valid_keys, scale):
    scores = (
        jnp.einsum("sqhd,skhd->shqk", query_heads, key_heads, preferred_element_type=jnp.float32)
        * scale
    )
    return jnp.where(valid_keys[:, None, None, :], scores, -1e30)


def pack_vectors(rows, vectors, dtype):
    cols = [v.reshape(rows, -1).astype(dtype) for v in vectors]
    block = jnp.concatenate(cols, axis=1)
    return jnp.pad(block, ((0, 0), (0, VEC_COLS - block.shape[1])))


def unpack_vectors(block, widths):
    out, at = [], 0
    for width in widths:
        out.append(block[:, at : at + width].reshape(-1))
        at += width
    return out


def gather_rows(pack):
    return lax.all_gather(pack, AXES, axis=0, tiled=True)


def scatter_rows(pack):
    return lax.psum_scatter(pack.astype(GRAD_WIRE), AXES, scatter_dimension=0, tiled=True).astype(
        jnp.float32
    )


def _pick(bit, first, second):
    return jnp.where(bit == 0, first, second), jnp.where(bit == 0, second, first)


def tree_gather(block, last_bit):
    n_sub = lax.axis_size("sub")
    n_f = lax.axis_size("fsdp")
    bits = n_f.bit_length() - 1
    chip = lax.axis_index("fsdp")
    order = [b for b in range(bits - 1, -1, -1) if b != last_bit] + [last_bit]
    acc = block
    done = []
    for j in order:
        pairs = [(g, g ^ (1 << j)) for g in range(n_f)]
        recv = lax.ppermute(acc, "fsdp", pairs)
        bit = (chip >> j) & 1
        lo, hi = _pick(bit, acc, recv)
        axis = sum(1 for b in done if b > j)
        acc = jnp.stack([lo, hi], axis=axis)
        done.append(j)
    acc = acc.reshape((n_f,) + block.shape)
    core = lax.axis_index("sub")
    recv = lax.ppermute(acc, "sub", [(0, 1), (1, 0)])
    lo, hi = _pick(core, acc, recv)
    full = jnp.stack([lo, hi], axis=1)
    return full.reshape((n_f * n_sub * block.shape[0],) + block.shape[1:])


def tree_scatter(full, first_bit):
    n_sub = lax.axis_size("sub")
    n_f = lax.axis_size("fsdp")
    rows = full.shape[0] // (n_sub * n_f)
    acc = full.reshape(n_f, n_sub, rows, -1)
    core = lax.axis_index("sub")
    keep = lax.dynamic_index_in_dim(acc, core, 1, keepdims=False)
    send = lax.dynamic_index_in_dim(acc, 1 - core, 1, keepdims=False)
    acc = keep + lax.ppermute(send, "sub", [(0, 1), (1, 0)])
    chip = lax.axis_index("fsdp")
    bits = n_f.bit_length() - 1
    acc = acc.reshape((2,) * bits + (rows, -1))
    left = list(range(bits - 1, -1, -1))
    order = [first_bit] + [b for b in range(bits) if b != first_bit]
    for j in order:
        axis = left.index(j)
        left.remove(j)
        bit = (chip >> j) & 1
        keep = lax.dynamic_index_in_dim(acc, bit, axis, keepdims=False)
        send = lax.dynamic_index_in_dim(acc, 1 - bit, axis, keepdims=False)
        pairs = [(g, g ^ (1 << j)) for g in range(n_f)]
        recv = lax.ppermute(send.astype(GRAD_WIRE), "fsdp", pairs)
        acc = keep + recv.astype(jnp.float32)
    return acc.reshape(rows, -1)


def body(
    inputs,
    lengths,
    positions,
    masked_output_gradient,
    w_query,
    b_query,
    w_key,
    w_value,
    b_value,
    w_out,
    b_out,
    gain_attn,
    shift_attn,
    w_up,
    b_up,
    w_down,
    b_down,
    gain_ffn,
    shift_ffn,
):
    seq_count, seq_slots, width = inputs.shape
    head_count = width // HD
    scale = HD ** (-0.5)
    row_count = seq_count * seq_slots
    head_shape = (seq_count, seq_slots, head_count, HD)
    shard_rows = w_query.shape[0]
    ff_ratio = w_down.shape[0] // shard_rows
    ff_width = w_up.shape[1]
    token_ids = jnp.arange(seq_slots, dtype=jnp.int32)
    valid_keys = token_ids[None, :] < lengths[:, None]

    with jax.named_scope("gather_attn"):
        vec_pack = pack_vectors(
            shard_rows, (b_query, b_value, b_out, gain_attn, shift_attn), jnp.bfloat16
        )
        query_part = tree_gather(jnp.concatenate([w_query, vec_pack], axis=1), 0)
        kv_part = tree_gather(jnp.concatenate([w_key, w_value], axis=1), 1)
        out_weight = tree_gather(w_out, 2)
    query_weight = query_part[:, 0:width]
    key_weight = kv_part[:, 0:width]
    value_weight = kv_part[:, width : 2 * width]
    query_bias, value_bias, out_bias, norm1_gain, norm1_shift = unpack_vectors(
        query_part[:, width:], (1, 1, 1, 1, 1)
    )

    with jax.named_scope("gather_ffn"):
        ffn_pack = jnp.concatenate(
            [
                w_up,
                pack_vectors(
                    shard_rows, (b_up, b_down, gain_ffn, shift_ffn), jnp.bfloat16
                ),
            ],
            axis=1,
        )
        ffn_full = gather_rows(ffn_pack)
        down_weight = gather_rows(w_down)
    up_weight = ffn_full[:, 0:ff_width]
    up_bias, downward_bias, norm2_gain, norm2_shift = unpack_vectors(
        ffn_full[:, ff_width:], (ff_ratio, 1, 1, 1)
    )

    flat_in = inputs.reshape(row_count, width)
    input_rows = flat_in.astype(jnp.float32)
    query_low = (project(flat_in, query_weight) + query_bias.astype(jnp.float32)).astype(
        jnp.bfloat16
    )
    keys_low = project(flat_in, key_weight).astype(jnp.bfloat16)
    values_low = (project(flat_in, value_weight) + value_bias.astype(jnp.float32)).astype(
        jnp.bfloat16
    )
    query_heads = query_low.reshape(head_shape)
    key_heads = keys_low.reshape(head_shape)
    value_heads = values_low.reshape(head_shape)
    scores = attention_scores(query_heads, key_heads, valid_keys, scale)
    row_top = jnp.max(scores, axis=-1, keepdims=True)
    expon = jnp.exp(scores - row_top)
    row_total = jnp.sum(expon, axis=-1, keepdims=True)
    log_total = row_top + jnp.log(row_total)
    probs_low = (expon / row_total).astype(jnp.bfloat16)
    attention_mixed = jnp.einsum(
        "shqk,skhd->sqhd", probs_low, value_heads, preferred_element_type=jnp.float32
    )
    attended_low = attention_mixed.reshape(row_count, width).astype(jnp.bfloat16)
    branch = project(attended_low, out_weight) + out_bias.astype(jnp.float32)
    middle, norm1_pull = jax.vjp(
        layer_norm,
        input_rows + branch,
        norm1_gain.astype(jnp.float32),
        norm1_shift.astype(jnp.float32),
    )
    middle_low = middle.astype(jnp.bfloat16)
    hidden = project(middle_low, up_weight) + up_bias.astype(jnp.float32)
    active, gelu_pull = jax.vjp(gelu_exact, hidden)
    active_low = active.astype(jnp.bfloat16)
    second_branch = project(active_low, down_weight) + downward_bias.astype(jnp.float32)
    output, norm2_pull = jax.vjp(
        layer_norm,
        middle + second_branch,
        norm2_gain.astype(jnp.float32),
        norm2_shift.astype(jnp.float32),
    )
    position_matches = (positions[:, :, None] == token_ids[None, None, :]).astype(jnp.bfloat16)
    cotangent = jnp.einsum(
        "efw,efv->ewv", position_matches, masked_output_gradient, preferred_element_type=jnp.float32
    ).reshape(row_count, width)
    grad_sum2, grad_gain2, grad_shift2 = norm2_pull(cotangent)
    second_grad = grad_sum2.astype(jnp.bfloat16)
    grad_down = weight_grad(active_low, second_grad)
    grad_down_bias = column_sum(second_grad)
    (grad_hidden,) = gelu_pull(reverse_projection(second_grad, down_weight))
    hidden_grad = grad_hidden.astype(jnp.bfloat16)
    grad_up = weight_grad(middle_low, hidden_grad)
    grad_up_bias = column_sum(hidden_grad)
    grad_middle = grad_sum2 + reverse_projection(hidden_grad, up_weight)
    grad_residual, grad_gain1, grad_shift1 = norm1_pull(grad_middle)
    branch_grad = grad_residual.astype(jnp.bfloat16)
    grad_out = weight_grad(attended_low, branch_grad)
    grad_out_bias = column_sum(branch_grad)

    with jax.named_scope("scatter_down"):
        grad_down_own = scatter_rows(grad_down)
    with jax.named_scope("scatter_late"):
        late_pack = jnp.concatenate(
            [
                grad_up,
                grad_out,
                pack_vectors(
                    width,
                    (
                        grad_up_bias,
                        grad_down_bias,
                        grad_gain2,
                        grad_shift2,
                        grad_out_bias,
                        grad_gain1,
                        grad_shift1,
                    ),
                    jnp.float32,
                ),
            ],
            axis=1,
        )
        late_pack, branch_grad = lax.optimization_barrier((late_pack, branch_grad))
        late_own = scatter_rows(late_pack)
    grad_up_own = late_own[:, 0:ff_width]
    grad_out_own = late_own[:, ff_width : ff_width + width]
    (
        grad_up_bias_own,
        grad_down_bias_own,
        grad_gain2_own,
        grad_shift2_own,
        grad_out_bias_own,
        grad_gain1_own,
        grad_shift1_own,
    ) = unpack_vectors(late_own[:, ff_width + width :], (ff_ratio, 1, 1, 1, 1, 1, 1))

    attended_grad = (
        reverse_projection(branch_grad, out_weight).astype(jnp.bfloat16).reshape(head_shape)
    )
    scores_again = attention_scores(query_heads, key_heads, valid_keys, scale)
    probs = jnp.exp(scores_again - log_total)
    probs_again = probs.astype(jnp.bfloat16)
    probs_grad = jnp.einsum(
        "sqhd,skhd->shqk", attended_grad, value_heads, preferred_element_type=jnp.float32
    )
    values_grad = jnp.einsum(
        "shqk,sqhd->skhd", probs_again, attended_grad, preferred_element_type=jnp.float32
    )
    values_grad = values_grad.astype(jnp.bfloat16).reshape(row_count, width)
    inner_sum = jnp.sum(probs * probs_grad, axis=-1, keepdims=True)
    scores_grad = (probs * (probs_grad - inner_sum)).astype(jnp.bfloat16)
    query_grad = jnp.einsum(
        "shqk,skhd->sqhd", scores_grad, key_heads, preferred_element_type=jnp.float32
    )
    query_grad = (query_grad * scale).astype(jnp.bfloat16).reshape(row_count, width)
    keys_grad = jnp.einsum(
        "shqk,sqhd->skhd", scores_grad, query_heads, preferred_element_type=jnp.float32
    )
    keys_grad = (keys_grad * scale).astype(jnp.bfloat16).reshape(row_count, width)
    grad_query = weight_grad(flat_in, query_grad)
    grad_query_bias = column_sum(query_grad)
    grad_key = weight_grad(flat_in, keys_grad)
    grad_value = weight_grad(flat_in, values_grad)
    value_bias_gradient = column_sum(values_grad)
    grad_input = (
        grad_residual
        + reverse_projection(query_grad, query_weight)
        + reverse_projection(keys_grad, key_weight)
        + reverse_projection(values_grad, value_weight)
    )
    with jax.named_scope("scatter_qkv"):
        query_own_pack = tree_scatter(
            jnp.concatenate(
                [
                    grad_query,
                    pack_vectors(width, (grad_query_bias, value_bias_gradient), jnp.float32),
                ],
                axis=1,
            ),
            0,
        )
        grad_key_own = tree_scatter(grad_key, 1)
        grad_value_own = tree_scatter(grad_value, 2)
    grad_query_own = query_own_pack[:, 0:width]
    grad_query_bias_own, value_bias_gradient_own = unpack_vectors(
        query_own_pack[:, width:], (1, 1)
    )
    return (
        output.astype(jnp.bfloat16).reshape(inputs.shape),
        grad_input.astype(jnp.bfloat16).reshape(inputs.shape),
        grad_query_own,
        grad_query_bias_own,
        grad_key_own,
        grad_value_own,
        value_bias_gradient_own,
        grad_out_own,
        grad_out_bias_own,
        grad_gain1_own,
        grad_shift1_own,
        grad_up_own,
        grad_up_bias_own,
        grad_down_own,
        grad_down_bias_own,
        grad_gain2_own,
        grad_shift2_own,
    )


def solution(mesh):
    rows3 = P(AXES, None, None)
    rows2 = P(AXES, None)
    rows1 = P(AXES)
    return jax.shard_map(
        body,
        mesh=mesh,
        in_specs=(
            rows3,
            rows1,
            rows2,
            rows3,
            rows2,
            rows1,
            rows2,
            rows2,
            rows1,
            rows2,
            rows1,
            rows1,
            rows1,
            rows2,
            rows1,
            rows2,
            rows1,
            rows1,
            rows1,
        ),
        out_specs=(
            rows3,
            rows3,
            rows2,
            rows1,
            rows2,
            rows2,
            rows1,
            rows2,
            rows1,
            rows1,
            rows1,
            rows2,
            rows1,
            rows2,
            rows1,
            rows1,
            rows1,
        ),
        check_vma=False,
    )
```

```python
import jax
import jax.numpy as jnp
from jax import lax
from jax.sharding import PartitionSpec as P

HD = 64
EPSILON = 1e-06
AXES = ("fsdp", "sub")
GRAD_WIRE = jnp.bfloat16
VEC_COLS = 256


def layer_norm(values, gain, shift):
    average = jnp.mean(values, axis=-1, keepdims=True)
    centered = values - average
    variance = jnp.mean(centered * centered, axis=-1, keepdims=True)
    return centered * lax.rsqrt(variance + EPSILON) * gain + shift


def gelu_exact(values):
    return values * (0.5 * (1.0 + lax.erf(values * (2.0 ** -0.5))))


def project(rows_low, weight):
    return jnp.dot(rows_low, weight, preferred_element_type=jnp.float32)


def reverse_projection(grad_low, weight):
    return lax.dot_general(
        grad_low, weight, (((1,), (1,)), ((), ())), preferred_element_type=jnp.float32
    )


def weight_grad(rows_low, grad_low):
    return lax.dot_general(
        rows_low, grad_low, (((0,), (0,)), ((), ())), preferred_element_type=jnp.float32
    )


def column_sum(grad_low):
    return jnp.sum(grad_low.astype(jnp.float32), axis=0)


def attention_scores(query_heads, key_heads, valid_keys, scale):
    scores = (
        jnp.einsum("sqhd,skhd->shqk", query_heads, key_heads, preferred_element_type=jnp.float32)
        * scale
    )
    return jnp.where(valid_keys[:, None, None, :], scores, -1e30)


def pack_vectors(rows, vectors, dtype):
    cols = [v.reshape(rows, -1).astype(dtype) for v in vectors]
    block = jnp.concatenate(cols, axis=1)
    return jnp.pad(block, ((0, 0), (0, VEC_COLS - block.shape[1])))


def unpack_vectors(block, widths):
    out, at = [], 0
    for width in widths:
        out.append(block[:, at : at + width].reshape(-1))
        at += width
    return out


def gather_rows(pack):
    return lax.all_gather(pack, AXES, axis=0, tiled=True)


def scatter_rows(pack):
    return lax.psum_scatter(pack.astype(GRAD_WIRE), AXES, scatter_dimension=0, tiled=True).astype(
        jnp.float32
    )


def _pick(bit, first, second):
    return jnp.where(bit == 0, first, second), jnp.where(bit == 0, second, first)


def tree_gather(block, last_bit):
    n_sub = lax.axis_size("sub")
    n_f = lax.axis_size("fsdp")
    bits = n_f.bit_length() - 1
    chip = lax.axis_index("fsdp")
    order = [b for b in range(bits - 1, -1, -1) if b != last_bit] + [last_bit]
    acc = block
    done = []
    for j in order:
        pairs = [(g, g ^ (1 << j)) for g in range(n_f)]
        recv = lax.ppermute(acc, "fsdp", pairs)
        bit = (chip >> j) & 1
        lo, hi = _pick(bit, acc, recv)
        axis = sum(1 for b in done if b > j)
        acc = jnp.stack([lo, hi], axis=axis)
        done.append(j)
    acc = acc.reshape((n_f,) + block.shape)
    core = lax.axis_index("sub")
    recv = lax.ppermute(acc, "sub", [(0, 1), (1, 0)])
    lo, hi = _pick(core, acc, recv)
    full = jnp.stack([lo, hi], axis=1)
    return full.reshape((n_f * n_sub * block.shape[0],) + block.shape[1:])


def tree_scatter(full, first_bit):
    n_sub = lax.axis_size("sub")
    n_f = lax.axis_size("fsdp")
    rows = full.shape[0] // (n_sub * n_f)
    acc = full.reshape(n_f, n_sub, rows, -1)
    core = lax.axis_index("sub")
    keep = lax.dynamic_index_in_dim(acc, core, 1, keepdims=False)
    send = lax.dynamic_index_in_dim(acc, 1 - core, 1, keepdims=False)
    acc = keep + lax.ppermute(send, "sub", [(0, 1), (1, 0)])
    chip = lax.axis_index("fsdp")
    bits = n_f.bit_length() - 1
    acc = acc.reshape((2,) * bits + (rows, -1))
    left = list(range(bits - 1, -1, -1))
    order = [first_bit] + [b for b in range(bits) if b != first_bit]
    for j in order:
        axis = left.index(j)
        left.remove(j)
        bit = (chip >> j) & 1
        keep = lax.dynamic_index_in_dim(acc, bit, axis, keepdims=False)
        send = lax.dynamic_index_in_dim(acc, 1 - bit, axis, keepdims=False)
        pairs = [(g, g ^ (1 << j)) for g in range(n_f)]
        recv = lax.ppermute(send.astype(GRAD_WIRE), "fsdp", pairs)
        acc = keep + recv.astype(jnp.float32)
    return acc.reshape(rows, -1)


def body(
    inputs,
    lengths,
    positions,
    masked_output_gradient,
    w_query,
    b_query,
    w_key,
    w_value,
    b_value,
    w_out,
    b_out,
    gain_attn,
    shift_attn,
    w_up,
    b_up,
    w_down,
    b_down,
    gain_ffn,
    shift_ffn,
):
    seq_count, seq_slots, width = inputs.shape
    head_count = width // HD
    scale = HD ** (-0.5)
    row_count = seq_count * seq_slots
    head_shape = (seq_count, seq_slots, head_count, HD)
    shard_rows = w_query.shape[0]
    ff_ratio = w_down.shape[0] // shard_rows
    ff_width = w_up.shape[1]
    token_ids = jnp.arange(seq_slots, dtype=jnp.int32)
    valid_keys = token_ids[None, :] < lengths[:, None]

    with jax.named_scope("gather_attn"):
        vec_pack = pack_vectors(
            shard_rows, (b_query, b_value, b_out, gain_attn, shift_attn), jnp.bfloat16
        )
        cut = (width // 6, width * 2 // 3)
        query_part = tree_gather(
            jnp.concatenate([w_query, w_value[:, : cut[0]], vec_pack], axis=1), 0
        )
        key_part = tree_gather(jnp.concatenate([w_key, w_value[:, cut[0] : cut[1]]], axis=1), 1)
        out_part = tree_gather(jnp.concatenate([w_value[:, cut[1] :], w_out], axis=1), 2)
    query_weight = query_part[:, 0:width]
    key_weight = key_part[:, 0:width]
    value_weight = jnp.concatenate(
        [
            query_part[:, width : width + cut[0]],
            key_part[:, width:],
            out_part[:, : width - cut[1]],
        ],
        axis=1,
    )
    out_weight = out_part[:, width - cut[1] :]
    vec_start = width + cut[0]
    query_bias, value_bias, out_bias, norm1_gain, norm1_shift = unpack_vectors(
        query_part[:, vec_start:], (1, 1, 1, 1, 1)
    )

    with jax.named_scope("gather_ffn"):
        ffn_pack = jnp.concatenate(
            [
                w_up,
                pack_vectors(
                    shard_rows, (b_up, b_down, gain_ffn, shift_ffn), jnp.bfloat16
                ),
            ],
            axis=1,
        )
        ffn_full = gather_rows(ffn_pack)
        down_weight = gather_rows(w_down)
    up_weight = ffn_full[:, 0:ff_width]
    up_bias, downward_bias, norm2_gain, norm2_shift = unpack_vectors(
        ffn_full[:, ff_width:], (ff_ratio, 1, 1, 1)
    )

    flat_in = inputs.reshape(row_count, width)
    input_rows = flat_in.astype(jnp.float32)
    query_low = (project(flat_in, query_weight) + query_bias.astype(jnp.float32)).astype(
        jnp.bfloat16
    )
    keys_low = project(flat_in, key_weight).astype(jnp.bfloat16)
    values_low = (project(flat_in, value_weight) + value_bias.astype(jnp.float32)).astype(
        jnp.bfloat16
    )
    query_heads = query_low.reshape(head_shape)
    key_heads = keys_low.reshape(head_shape)
    value_heads = values_low.reshape(head_shape)
    scores = attention_scores(query_heads, key_heads, valid_keys, scale)
    row_top = jnp.max(scores, axis=-1, keepdims=True)
    expon = jnp.exp(scores - row_top)
    row_total = jnp.sum(expon, axis=-1, keepdims=True)
    log_total = row_top + jnp.log(row_total)
    probs_low = (expon / row_total).astype(jnp.bfloat16)
    attention_mixed = jnp.einsum(
        "shqk,skhd->sqhd", probs_low, value_heads, preferred_element_type=jnp.float32
    )
    attended_low = attention_mixed.reshape(row_count, width).astype(jnp.bfloat16)
    branch = project(attended_low, out_weight) + out_bias.astype(jnp.float32)
    middle, norm1_pull = jax.vjp(
        layer_norm,
        input_rows + branch,
        norm1_gain.astype(jnp.float32),
        norm1_shift.astype(jnp.float32),
    )
    middle_low = middle.astype(jnp.bfloat16)
    hidden = project(middle_low, up_weight) + up_bias.astype(jnp.float32)
    active, gelu_pull = jax.vjp(gelu_exact, hidden)
    active_low = active.astype(jnp.bfloat16)
    second_branch = project(active_low, down_weight) + downward_bias.astype(jnp.float32)
    output, norm2_pull = jax.vjp(
        layer_norm,
        middle + second_branch,
        norm2_gain.astype(jnp.float32),
        norm2_shift.astype(jnp.float32),
    )
    position_matches = (positions[:, :, None] == token_ids[None, None, :]).astype(jnp.bfloat16)
    cotangent = jnp.einsum(
        "efw,efv->ewv", position_matches, masked_output_gradient, preferred_element_type=jnp.float32
    ).reshape(row_count, width)
    grad_sum2, grad_gain2, grad_shift2 = norm2_pull(cotangent)
    second_grad = grad_sum2.astype(jnp.bfloat16)
    grad_down = weight_grad(active_low, second_grad)
    grad_down_bias = column_sum(second_grad)
    (grad_hidden,) = gelu_pull(reverse_projection(second_grad, down_weight))
    hidden_grad = grad_hidden.astype(jnp.bfloat16)
    grad_up = weight_grad(middle_low, hidden_grad)
    grad_up_bias = column_sum(hidden_grad)
    grad_middle = grad_sum2 + reverse_projection(hidden_grad, up_weight)
    grad_residual, grad_gain1, grad_shift1 = norm1_pull(grad_middle)
    branch_grad = grad_residual.astype(jnp.bfloat16)
    grad_out = weight_grad(attended_low, branch_grad)
    grad_out_bias = column_sum(branch_grad)

    with jax.named_scope("scatter_late"):
        late_pack = jnp.concatenate(
            [
                grad_up,
                grad_down.reshape(width, ff_ratio * width),
                grad_out,
                pack_vectors(
                    width,
                    (
                        grad_up_bias,
                        grad_down_bias,
                        grad_gain2,
                        grad_shift2,
                        grad_out_bias,
                        grad_gain1,
                        grad_shift1,
                    ),
                    jnp.float32,
                ),
            ],
            axis=1,
        )
        late_pack, branch_grad = lax.optimization_barrier((late_pack, branch_grad))
        late_own = scatter_rows(late_pack)
    grad_down_own = late_own[:, ff_width : 2 * ff_width].reshape(shard_rows * ff_ratio, width)
    late_own = jnp.concatenate([late_own[:, 0:ff_width], late_own[:, 2 * ff_width :]], axis=1)
    grad_up_own = late_own[:, 0:ff_width]
    grad_out_own = late_own[:, ff_width : ff_width + width]
    (
        grad_up_bias_own,
        grad_down_bias_own,
        grad_gain2_own,
        grad_shift2_own,
        grad_out_bias_own,
        grad_gain1_own,
        grad_shift1_own,
    ) = unpack_vectors(late_own[:, ff_width + width :], (ff_ratio, 1, 1, 1, 1, 1, 1))

    attended_grad = (
        reverse_projection(branch_grad, out_weight).astype(jnp.bfloat16).reshape(head_shape)
    )
    scores_again = attention_scores(query_heads, key_heads, valid_keys, scale)
    probs = jnp.exp(scores_again - log_total)
    probs_again = probs.astype(jnp.bfloat16)
    probs_grad = jnp.einsum(
        "sqhd,skhd->shqk", attended_grad, value_heads, preferred_element_type=jnp.float32
    )
    values_grad = jnp.einsum(
        "shqk,sqhd->skhd", probs_again, attended_grad, preferred_element_type=jnp.float32
    )
    values_grad = values_grad.astype(jnp.bfloat16).reshape(row_count, width)
    inner_sum = jnp.sum(probs * probs_grad, axis=-1, keepdims=True)
    scores_grad = (probs * (probs_grad - inner_sum)).astype(jnp.bfloat16)
    query_grad = jnp.einsum(
        "shqk,skhd->sqhd", scores_grad, key_heads, preferred_element_type=jnp.float32
    )
    query_grad = (query_grad * scale).astype(jnp.bfloat16).reshape(row_count, width)
    keys_grad = jnp.einsum(
        "shqk,sqhd->skhd", scores_grad, query_heads, preferred_element_type=jnp.float32
    )
    keys_grad = (keys_grad * scale).astype(jnp.bfloat16).reshape(row_count, width)
    grad_query = weight_grad(flat_in, query_grad)
    grad_query_bias = column_sum(query_grad)
    grad_key = weight_grad(flat_in, keys_grad)
    grad_value = weight_grad(flat_in, values_grad)
    value_bias_gradient = column_sum(values_grad)
    grad_input = (
        grad_residual
        + reverse_projection(query_grad, query_weight)
        + reverse_projection(keys_grad, key_weight)
        + reverse_projection(values_grad, value_weight)
    )
    with jax.named_scope("scatter_qkv"):
        query_own_pack = tree_scatter(
            jnp.concatenate(
                [
                    grad_query,
                    pack_vectors(width, (grad_query_bias, value_bias_gradient), jnp.float32),
                ],
                axis=1,
            ),
            0,
        )
        grad_key_own = tree_scatter(grad_key, 1)
        grad_value_own = tree_scatter(grad_value, 2)
    grad_query_own = query_own_pack[:, 0:width]
    grad_query_bias_own, value_bias_gradient_own = unpack_vectors(
        query_own_pack[:, width:], (1, 1)
    )
    return (
        output.astype(jnp.bfloat16).reshape(inputs.shape),
        grad_input.astype(jnp.bfloat16).reshape(inputs.shape),
        grad_query_own,
        grad_query_bias_own,
        grad_key_own,
        grad_value_own,
        value_bias_gradient_own,
        grad_out_own,
        grad_out_bias_own,
        grad_gain1_own,
        grad_shift1_own,
        grad_up_own,
        grad_up_bias_own,
        grad_down_own,
        grad_down_bias_own,
        grad_gain2_own,
        grad_shift2_own,
    )


def solution(mesh):
    rows3 = P(AXES, None, None)
    rows2 = P(AXES, None)
    rows1 = P(AXES)
    return jax.shard_map(
        body,
        mesh=mesh,
        in_specs=(
            rows3,
            rows1,
            rows2,
            rows3,
            rows2,
            rows1,
            rows2,
            rows2,
            rows1,
            rows2,
            rows1,
            rows1,
            rows1,
            rows2,
            rows1,
            rows2,
            rows1,
            rows1,
            rows1,
        ),
        out_specs=(
            rows3,
            rows3,
            rows2,
            rows1,
            rows2,
            rows2,
            rows1,
            rows2,
            rows1,
            rows1,
            rows1,
            rows2,
            rows1,
            rows2,
            rows1,
            rows1,
            rows1,
        ),
        check_vma=False,
    )
```

```python
import jax
import jax.numpy as jnp
from jax import lax
from jax.sharding import PartitionSpec as P

HD = 64
EPSILON = 1e-06
AXES = ("fsdp", "sub")
GRAD_WIRE = jnp.bfloat16
VEC_COLS = 256


def layer_norm(values, gain, shift):
    average = jnp.mean(values, axis=-1, keepdims=True)
    centered = values - average
    variance = jnp.mean(centered * centered, axis=-1, keepdims=True)
    return centered * lax.rsqrt(variance + EPSILON) * gain + shift


def gelu_exact(values):
    return values * (0.5 * (1.0 + lax.erf(values * (2.0 ** -0.5))))


def project(rows_low, weight):
    return jnp.dot(rows_low, weight, preferred_element_type=jnp.float32)


def reverse_projection(grad_low, weight):
    return lax.dot_general(
        grad_low, weight, (((1,), (1,)), ((), ())), preferred_element_type=jnp.float32
    )


def weight_grad(rows_low, grad_low):
    return lax.dot_general(
        rows_low, grad_low, (((0,), (0,)), ((), ())), preferred_element_type=jnp.float32
    )


def column_sum(grad_low):
    return jnp.sum(grad_low.astype(jnp.float32), axis=0)


def attention_scores(query_heads, key_heads, valid_keys, scale):
    scores = (
        jnp.einsum("shqd,shkd->shqk", query_heads, key_heads, preferred_element_type=jnp.float32)
        * scale
    )
    return jnp.where(valid_keys[:, None, None, :], scores, -1e30)


def pack_vectors(rows, vectors, dtype):
    cols = [v.reshape(rows, -1).astype(dtype) for v in vectors]
    block = jnp.concatenate(cols, axis=1)
    return jnp.pad(block, ((0, 0), (0, VEC_COLS - block.shape[1])))


def unpack_vectors(block, widths):
    out, at = [], 0
    for width in widths:
        out.append(block[:, at : at + width].reshape(-1))
        at += width
    return out


def gather_rows(pack):
    return lax.all_gather(pack, AXES, axis=0, tiled=True)


def scatter_rows(pack):
    return lax.psum_scatter(pack.astype(GRAD_WIRE), AXES, scatter_dimension=0, tiled=True).astype(
        jnp.float32
    )


def _pick(bit, first, second):
    return jnp.where(bit == 0, first, second), jnp.where(bit == 0, second, first)


def tree_gather(block, last_bit):
    n_sub = lax.axis_size("sub")
    n_f = lax.axis_size("fsdp")
    bits = n_f.bit_length() - 1
    chip = lax.axis_index("fsdp")
    order = [b for b in range(bits - 1, -1, -1) if b != last_bit] + [last_bit]
    acc = block
    done = []
    for j in order:
        pairs = [(g, g ^ (1 << j)) for g in range(n_f)]
        recv = lax.ppermute(acc, "fsdp", pairs)
        bit = (chip >> j) & 1
        lo, hi = _pick(bit, acc, recv)
        axis = sum(1 for b in done if b > j)
        acc = jnp.stack([lo, hi], axis=axis)
        done.append(j)
    acc = acc.reshape((n_f,) + block.shape)
    core = lax.axis_index("sub")
    recv = lax.ppermute(acc, "sub", [(0, 1), (1, 0)])
    lo, hi = _pick(core, acc, recv)
    full = jnp.stack([lo, hi], axis=1)
    return full.reshape((n_f * n_sub * block.shape[0],) + block.shape[1:])


def tree_scatter(full, first_bit):
    n_sub = lax.axis_size("sub")
    n_f = lax.axis_size("fsdp")
    rows = full.shape[0] // (n_sub * n_f)
    acc = full.reshape(n_f, n_sub, rows, -1)
    core = lax.axis_index("sub")
    keep = lax.dynamic_index_in_dim(acc, core, 1, keepdims=False)
    send = lax.dynamic_index_in_dim(acc, 1 - core, 1, keepdims=False)
    acc = keep + lax.ppermute(send, "sub", [(0, 1), (1, 0)])
    chip = lax.axis_index("fsdp")
    bits = n_f.bit_length() - 1
    acc = acc.reshape((2,) * bits + (rows, -1))
    left = list(range(bits - 1, -1, -1))
    order = [first_bit] + [b for b in range(bits) if b != first_bit]
    for j in order:
        axis = left.index(j)
        left.remove(j)
        bit = (chip >> j) & 1
        keep = lax.dynamic_index_in_dim(acc, bit, axis, keepdims=False)
        send = lax.dynamic_index_in_dim(acc, 1 - bit, axis, keepdims=False)
        pairs = [(g, g ^ (1 << j)) for g in range(n_f)]
        recv = lax.ppermute(send.astype(GRAD_WIRE), "fsdp", pairs)
        acc = keep + recv.astype(jnp.float32)
    return acc.reshape(rows, -1)


def body(
    inputs,
    lengths,
    positions,
    masked_output_gradient,
    w_query,
    b_query,
    w_key,
    w_value,
    b_value,
    w_out,
    b_out,
    gain_attn,
    shift_attn,
    w_up,
    b_up,
    w_down,
    b_down,
    gain_ffn,
    shift_ffn,
):
    seq_count, seq_slots, width = inputs.shape
    head_count = width // HD
    scale = HD ** (-0.5)
    row_count = seq_count * seq_slots
    head_shape = (seq_count, seq_slots, head_count, HD)
    shard_rows = w_query.shape[0]
    ff_ratio = w_down.shape[0] // shard_rows
    ff_width = w_up.shape[1]
    token_ids = jnp.arange(seq_slots, dtype=jnp.int32)
    valid_keys = token_ids[None, :] < lengths[:, None]

    with jax.named_scope("gather_attn"):
        vec_pack = pack_vectors(
            shard_rows, (b_query, b_value, b_out, gain_attn, shift_attn), jnp.bfloat16
        )
        cut = (width // 6, width * 2 // 3)
        query_part = tree_gather(
            jnp.concatenate([w_query, w_value[:, : cut[0]], vec_pack], axis=1), 0
        )
        key_part = tree_gather(jnp.concatenate([w_key, w_value[:, cut[0] : cut[1]]], axis=1), 1)
        out_part = tree_gather(jnp.concatenate([w_value[:, cut[1] :], w_out], axis=1), 2)
    query_weight = query_part[:, 0:width]
    key_weight = key_part[:, 0:width]
    value_weight = jnp.concatenate(
        [
            query_part[:, width : width + cut[0]],
            key_part[:, width:],
            out_part[:, : width - cut[1]],
        ],
        axis=1,
    )
    out_weight = out_part[:, width - cut[1] :]
    vec_start = width + cut[0]
    query_bias, value_bias, out_bias, norm1_gain, norm1_shift = unpack_vectors(
        query_part[:, vec_start:], (1, 1, 1, 1, 1)
    )

    with jax.named_scope("gather_ffn"):
        ffn_pack = jnp.concatenate(
            [
                w_up,
                pack_vectors(
                    shard_rows, (b_up, b_down, gain_ffn, shift_ffn), jnp.bfloat16
                ),
            ],
            axis=1,
        )
        ffn_full = gather_rows(ffn_pack)
        down_weight = gather_rows(w_down)
    up_weight = ffn_full[:, 0:ff_width]
    up_bias, downward_bias, norm2_gain, norm2_shift = unpack_vectors(
        ffn_full[:, ff_width:], (ff_ratio, 1, 1, 1)
    )

    flat_in = inputs.reshape(row_count, width)
    input_rows = flat_in.astype(jnp.float32)
    head_weights = (head_count, HD)
    query_w3 = query_weight.reshape((width,) + head_weights)
    key_w3 = key_weight.reshape((width,) + head_weights)
    value_w3 = value_weight.reshape((width,) + head_weights)
    out_w3 = out_weight.reshape(head_weights + (width,))
    query_heads = (
        jnp.einsum("snc,chd->shnd", inputs, query_w3, preferred_element_type=jnp.float32)
        + query_bias.astype(jnp.float32).reshape(head_weights)[None, :, None, :]
    ).astype(jnp.bfloat16)
    key_heads = jnp.einsum(
        "snc,chd->shnd", inputs, key_w3, preferred_element_type=jnp.float32
    ).astype(jnp.bfloat16)
    value_heads = (
        jnp.einsum("snc,chd->shnd", inputs, value_w3, preferred_element_type=jnp.float32)
        + value_bias.astype(jnp.float32).reshape(head_weights)[None, :, None, :]
    ).astype(jnp.bfloat16)
    scores = attention_scores(query_heads, key_heads, valid_keys, scale)
    row_top = jnp.max(scores, axis=-1, keepdims=True)
    expon = jnp.exp(scores - row_top)
    row_total = jnp.sum(expon, axis=-1, keepdims=True)
    log_total = row_top + jnp.log(row_total)
    probs_low = (expon / row_total).astype(jnp.bfloat16)
    attention_mixed = jnp.einsum(
        "shqk,shkd->shqd", probs_low, value_heads, preferred_element_type=jnp.float32
    )
    attended_low = attention_mixed.astype(jnp.bfloat16)
    branch = (
        jnp.einsum("shqd,hdc->sqc", attended_low, out_w3, preferred_element_type=jnp.float32)
        .reshape(row_count, width)
    ) + out_bias.astype(jnp.float32)
    middle, norm1_pull = jax.vjp(
        layer_norm,
        input_rows + branch,
        norm1_gain.astype(jnp.float32),
        norm1_shift.astype(jnp.float32),
    )
    middle_low = middle.astype(jnp.bfloat16)
    hidden = project(middle_low, up_weight) + up_bias.astype(jnp.float32)
    active, gelu_pull = jax.vjp(gelu_exact, hidden)
    active_low = active.astype(jnp.bfloat16)
    second_branch = project(active_low, down_weight) + downward_bias.astype(jnp.float32)
    output, norm2_pull = jax.vjp(
        layer_norm,
        middle + second_branch,
        norm2_gain.astype(jnp.float32),
        norm2_shift.astype(jnp.float32),
    )
    position_matches = (positions[:, :, None] == token_ids[None, None, :]).astype(jnp.bfloat16)
    cotangent = jnp.einsum(
        "efw,efv->ewv", position_matches, masked_output_gradient, preferred_element_type=jnp.float32
    ).reshape(row_count, width)
    grad_sum2, grad_gain2, grad_shift2 = norm2_pull(cotangent)
    second_grad = grad_sum2.astype(jnp.bfloat16)
    grad_down = weight_grad(active_low, second_grad)
    grad_down_bias = column_sum(second_grad)
    (grad_hidden,) = gelu_pull(reverse_projection(second_grad, down_weight))
    hidden_grad = grad_hidden.astype(jnp.bfloat16)
    grad_up = weight_grad(middle_low, hidden_grad)
    grad_up_bias = column_sum(hidden_grad)
    grad_middle = grad_sum2 + reverse_projection(hidden_grad, up_weight)
    grad_residual, grad_gain1, grad_shift1 = norm1_pull(grad_middle)
    branch_grad = grad_residual.astype(jnp.bfloat16)
    branch_grad3 = branch_grad.reshape(inputs.shape)
    grad_out = jnp.einsum(
        "shqd,sqc->hdc", attended_low, branch_grad3, preferred_element_type=jnp.float32
    ).reshape(width, width)
    grad_out_bias = column_sum(branch_grad)

    with jax.named_scope("scatter_late"):
        late_pack = jnp.concatenate(
            [
                grad_up,
                grad_down.reshape(width, ff_ratio * width),
                grad_out,
                pack_vectors(
                    width,
                    (
                        grad_up_bias,
                        grad_down_bias,
                        grad_gain2,
                        grad_shift2,
                        grad_out_bias,
                        grad_gain1,
                        grad_shift1,
                    ),
                    jnp.float32,
                ),
            ],
            axis=1,
        )
        late_pack, branch_grad = lax.optimization_barrier((late_pack, branch_grad))
        late_own = scatter_rows(late_pack)
    grad_down_own = late_own[:, ff_width : 2 * ff_width].reshape(shard_rows * ff_ratio, width)
    late_own = jnp.concatenate([late_own[:, 0:ff_width], late_own[:, 2 * ff_width :]], axis=1)
    grad_up_own = late_own[:, 0:ff_width]
    grad_out_own = late_own[:, ff_width : ff_width + width]
    (
        grad_up_bias_own,
        grad_down_bias_own,
        grad_gain2_own,
        grad_shift2_own,
        grad_out_bias_own,
        grad_gain1_own,
        grad_shift1_own,
    ) = unpack_vectors(late_own[:, ff_width + width :], (ff_ratio, 1, 1, 1, 1, 1, 1))

    attended_grad = jnp.einsum(
        "sqc,hdc->shqd", branch_grad3, out_w3, preferred_element_type=jnp.float32
    ).astype(jnp.bfloat16)
    scores_again = attention_scores(query_heads, key_heads, valid_keys, scale)
    probs = jnp.exp(scores_again - log_total)
    probs_again = probs.astype(jnp.bfloat16)
    probs_grad = jnp.einsum(
        "shqd,shkd->shqk", attended_grad, value_heads, preferred_element_type=jnp.float32
    )
    values_grad = jnp.einsum(
        "shqk,shqd->shkd", probs_again, attended_grad, preferred_element_type=jnp.float32
    ).astype(jnp.bfloat16)
    inner_sum = jnp.sum(probs * probs_grad, axis=-1, keepdims=True)
    scores_grad = (probs * (probs_grad - inner_sum)).astype(jnp.bfloat16)
    query_grad = jnp.einsum(
        "shqk,shkd->shqd", scores_grad, key_heads, preferred_element_type=jnp.float32
    )
    query_grad = (query_grad * scale).astype(jnp.bfloat16)
    keys_grad = jnp.einsum(
        "shqk,shqd->shkd", scores_grad, query_heads, preferred_element_type=jnp.float32
    )
    keys_grad = (keys_grad * scale).astype(jnp.bfloat16)

    def head_weight_grad(head_grad):
        return jnp.einsum(
            "snc,shnd->chd", inputs, head_grad, preferred_element_type=jnp.float32
        ).reshape(width, width)

    def head_column_sum(head_grad):
        return jnp.sum(head_grad.astype(jnp.float32), axis=(0, 2)).reshape(width)

    def head_reverse(head_grad, w3):
        return jnp.einsum(
            "shnd,chd->snc", head_grad, w3, preferred_element_type=jnp.float32
        ).reshape(row_count, width)

    grad_query = head_weight_grad(query_grad)
    grad_query_bias = head_column_sum(query_grad)
    grad_key = head_weight_grad(keys_grad)
    grad_value = head_weight_grad(values_grad)
    value_bias_gradient = head_column_sum(values_grad)
    grad_input = (
        grad_residual
        + head_reverse(query_grad, query_w3)
        + head_reverse(keys_grad, key_w3)
        + head_reverse(values_grad, value_w3)
    )
    with jax.named_scope("scatter_qkv"):
        query_own_pack = tree_scatter(
            jnp.concatenate(
                [
                    grad_query,
                    pack_vectors(width, (grad_query_bias, value_bias_gradient), jnp.float32),
                ],
                axis=1,
            ),
            0,
        )
        grad_key_own = tree_scatter(grad_key, 1)
        grad_value_own = tree_scatter(grad_value, 2)
    grad_query_own = query_own_pack[:, 0:width]
    grad_query_bias_own, value_bias_gradient_own = unpack_vectors(
        query_own_pack[:, width:], (1, 1)
    )
    return (
        output.astype(jnp.bfloat16).reshape(inputs.shape),
        grad_input.astype(jnp.bfloat16).reshape(inputs.shape),
        grad_query_own,
        grad_query_bias_own,
        grad_key_own,
        grad_value_own,
        value_bias_gradient_own,
        grad_out_own,
        grad_out_bias_own,
        grad_gain1_own,
        grad_shift1_own,
        grad_up_own,
        grad_up_bias_own,
        grad_down_own,
        grad_down_bias_own,
        grad_gain2_own,
        grad_shift2_own,
    )


def solution(mesh):
    rows3 = P(AXES, None, None)
    rows2 = P(AXES, None)
    rows1 = P(AXES)
    return jax.shard_map(
        body,
        mesh=mesh,
        in_specs=(
            rows3,
            rows1,
            rows2,
            rows3,
            rows2,
            rows1,
            rows2,
            rows2,
            rows1,
            rows2,
            rows1,
            rows1,
            rows1,
            rows2,
            rows1,
            rows2,
            rows1,
            rows1,
            rows1,
        ),
        out_specs=(
            rows3,
            rows3,
            rows2,
            rows1,
            rows2,
            rows2,
            rows1,
            rows2,
            rows1,
            rows1,
            rows1,
            rows2,
            rows1,
            rows2,
            rows1,
            rows1,
            rows1,
        ),
        check_vma=False,
    )
```

```python
import jax
import jax.numpy as jnp
from jax import lax
from jax.sharding import PartitionSpec as P

HD = 64
EPSILON = 1e-06
AXES = ("fsdp", "sub")
GRAD_WIRE = jnp.bfloat16
VEC_COLS = 256


def layer_norm(values, gain, shift):
    average = jnp.mean(values, axis=-1, keepdims=True)
    centered = values - average
    variance = jnp.mean(centered * centered, axis=-1, keepdims=True)
    return centered * lax.rsqrt(variance + EPSILON) * gain + shift


def gelu_exact(values):
    return values * (0.5 * (1.0 + lax.erf(values * (2.0 ** -0.5))))


def project(rows_low, weight):
    return jnp.dot(rows_low, weight, preferred_element_type=jnp.float32)


def reverse_projection(grad_low, weight):
    return lax.dot_general(
        grad_low, weight, (((1,), (1,)), ((), ())), preferred_element_type=jnp.float32
    )


def weight_grad(rows_low, grad_low):
    return lax.dot_general(
        rows_low, grad_low, (((0,), (0,)), ((), ())), preferred_element_type=jnp.float32
    )


def column_sum(grad_low):
    return jnp.sum(grad_low.astype(jnp.float32), axis=0)


def attention_scores(query_heads, key_heads, valid_keys, scale):
    scores = (
        jnp.einsum("sqhd,skhd->shqk", query_heads, key_heads, preferred_element_type=jnp.float32)
        * scale
    )
    return jnp.where(valid_keys[:, None, None, :], scores, -1e30)


def pack_vectors(rows, vectors, dtype):
    cols = [v.reshape(rows, -1).astype(dtype) for v in vectors]
    block = jnp.concatenate(cols, axis=1)
    return jnp.pad(block, ((0, 0), (0, VEC_COLS - block.shape[1])))


def unpack_vectors(block, widths):
    out, at = [], 0
    for width in widths:
        out.append(block[:, at : at + width].reshape(-1))
        at += width
    return out


def gather_rows(pack):
    return lax.all_gather(pack, AXES, axis=0, tiled=True)


def scatter_rows(pack):
    return lax.psum_scatter(pack.astype(GRAD_WIRE), AXES, scatter_dimension=0, tiled=True).astype(
        jnp.float32
    )


def _pick(bit, first, second):
    return jnp.where(bit == 0, first, second), jnp.where(bit == 0, second, first)


def tree_gather(block, last_bit):
    n_sub = lax.axis_size("sub")
    n_f = lax.axis_size("fsdp")
    bits = n_f.bit_length() - 1
    chip = lax.axis_index("fsdp")
    order = [b for b in range(bits - 1, -1, -1) if b != last_bit] + [last_bit]
    acc = block
    done = []
    for j in order:
        pairs = [(g, g ^ (1 << j)) for g in range(n_f)]
        recv = lax.ppermute(acc, "fsdp", pairs)
        bit = (chip >> j) & 1
        lo, hi = _pick(bit, acc, recv)
        axis = sum(1 for b in done if b > j)
        acc = jnp.stack([lo, hi], axis=axis)
        done.append(j)
    acc = acc.reshape((n_f,) + block.shape)
    core = lax.axis_index("sub")
    recv = lax.ppermute(acc, "sub", [(0, 1), (1, 0)])
    lo, hi = _pick(core, acc, recv)
    full = jnp.stack([lo, hi], axis=1)
    return full.reshape((n_f * n_sub * block.shape[0],) + block.shape[1:])


def tree_scatter(full, first_bit):
    n_sub = lax.axis_size("sub")
    n_f = lax.axis_size("fsdp")
    rows = full.shape[0] // (n_sub * n_f)
    acc = full.reshape(n_f, n_sub, rows, -1)
    core = lax.axis_index("sub")
    keep = lax.dynamic_index_in_dim(acc, core, 1, keepdims=False)
    send = lax.dynamic_index_in_dim(acc, 1 - core, 1, keepdims=False)
    acc = keep + lax.ppermute(send, "sub", [(0, 1), (1, 0)])
    chip = lax.axis_index("fsdp")
    bits = n_f.bit_length() - 1
    acc = acc.reshape((2,) * bits + (rows, -1))
    left = list(range(bits - 1, -1, -1))
    order = [first_bit] + [b for b in range(bits) if b != first_bit]
    for j in order:
        axis = left.index(j)
        left.remove(j)
        bit = (chip >> j) & 1
        keep = lax.dynamic_index_in_dim(acc, bit, axis, keepdims=False)
        send = lax.dynamic_index_in_dim(acc, 1 - bit, axis, keepdims=False)
        pairs = [(g, g ^ (1 << j)) for g in range(n_f)]
        recv = lax.ppermute(send.astype(GRAD_WIRE), "fsdp", pairs)
        acc = keep + recv.astype(jnp.float32)
    return acc.reshape(rows, -1)


def body(
    inputs,
    lengths,
    positions,
    masked_output_gradient,
    w_query,
    b_query,
    w_key,
    w_value,
    b_value,
    w_out,
    b_out,
    gain_attn,
    shift_attn,
    w_up,
    b_up,
    w_down,
    b_down,
    gain_ffn,
    shift_ffn,
):
    seq_count, seq_slots, width = inputs.shape
    head_count = width // HD
    scale = HD ** (-0.5)
    row_count = seq_count * seq_slots
    head_shape = (seq_count, seq_slots, head_count, HD)
    shard_rows = w_query.shape[0]
    ff_ratio = w_down.shape[0] // shard_rows
    ff_width = w_up.shape[1]
    token_ids = jnp.arange(seq_slots, dtype=jnp.int32)
    valid_keys = token_ids[None, :] < lengths[:, None]

    with jax.named_scope("gather_attn"):
        vec_pack = pack_vectors(
            shard_rows, (b_query, b_value, b_out, gain_attn, shift_attn), jnp.bfloat16
        )
        cut = (width // 6, width * 2 // 3)
        query_part = tree_gather(
            jnp.concatenate([w_query, w_value[:, : cut[0]], vec_pack], axis=1), 0
        )
        key_part = tree_gather(jnp.concatenate([w_key, w_value[:, cut[0] : cut[1]]], axis=1), 1)
        out_part = tree_gather(jnp.concatenate([w_value[:, cut[1] :], w_out], axis=1), 2)
    query_weight = query_part[:, 0:width]
    key_weight = key_part[:, 0:width]
    value_weight = jnp.concatenate(
        [
            query_part[:, width : width + cut[0]],
            key_part[:, width:],
            out_part[:, : width - cut[1]],
        ],
        axis=1,
    )
    out_weight = out_part[:, width - cut[1] :]
    vec_start = width + cut[0]
    query_bias, value_bias, out_bias, norm1_gain, norm1_shift = unpack_vectors(
        query_part[:, vec_start:], (1, 1, 1, 1, 1)
    )

    with jax.named_scope("gather_ffn"):
        ffn_pack = jnp.concatenate(
            [
                w_up,
                pack_vectors(
                    shard_rows, (b_up, b_down, gain_ffn, shift_ffn), jnp.bfloat16
                ),
            ],
            axis=1,
        )
        ffn_full = gather_rows(ffn_pack)
        down_weight = gather_rows(w_down)
    up_weight = ffn_full[:, 0:ff_width]
    up_bias, downward_bias, norm2_gain, norm2_shift = unpack_vectors(
        ffn_full[:, ff_width:], (ff_ratio, 1, 1, 1)
    )

    flat_in = inputs.reshape(row_count, width)
    input_rows = flat_in.astype(jnp.float32)
    query_low = (project(flat_in, query_weight) + query_bias.astype(jnp.float32)).astype(
        jnp.bfloat16
    )
    keys_low = project(flat_in, key_weight).astype(jnp.bfloat16)
    values_low = (project(flat_in, value_weight) + value_bias.astype(jnp.float32)).astype(
        jnp.bfloat16
    )
    query_heads = query_low.reshape(head_shape)
    key_heads = keys_low.reshape(head_shape)
    value_heads = values_low.reshape(head_shape)
    scores = attention_scores(query_heads, key_heads, valid_keys, scale)
    row_top = jnp.max(scores, axis=-1, keepdims=True)
    expon = jnp.exp(scores - row_top)
    row_total = jnp.sum(expon, axis=-1, keepdims=True)
    log_total = row_top + jnp.log(row_total)
    probs_low = (expon / row_total).astype(jnp.bfloat16)
    attention_mixed = jnp.einsum(
        "shqk,skhd->sqhd", probs_low, value_heads, preferred_element_type=jnp.float32
    )
    attended_low = attention_mixed.reshape(row_count, width).astype(jnp.bfloat16)
    branch = project(attended_low, out_weight) + out_bias.astype(jnp.float32)
    middle, norm1_pull = jax.vjp(
        layer_norm,
        input_rows + branch,
        norm1_gain.astype(jnp.float32),
        norm1_shift.astype(jnp.float32),
    )
    middle_low = middle.astype(jnp.bfloat16)
    hidden = project(middle_low, up_weight) + up_bias.astype(jnp.float32)
    active, gelu_pull = jax.vjp(gelu_exact, hidden)
    active_low = active.astype(jnp.bfloat16)
    second_branch = project(active_low, down_weight) + downward_bias.astype(jnp.float32)
    output, norm2_pull = jax.vjp(
        layer_norm,
        middle + second_branch,
        norm2_gain.astype(jnp.float32),
        norm2_shift.astype(jnp.float32),
    )
    position_matches = (positions[:, :, None] == token_ids[None, None, :]).astype(jnp.bfloat16)
    cotangent = jnp.einsum(
        "efw,efv->ewv", position_matches, masked_output_gradient, preferred_element_type=jnp.float32
    ).reshape(row_count, width)
    grad_sum2, grad_gain2, grad_shift2 = norm2_pull(cotangent)
    second_grad = grad_sum2.astype(jnp.bfloat16)
    grad_down = weight_grad(active_low, second_grad)
    grad_down_bias = column_sum(second_grad)
    (grad_hidden,) = gelu_pull(reverse_projection(second_grad, down_weight))
    hidden_grad = grad_hidden.astype(jnp.bfloat16)
    grad_up = weight_grad(middle_low, hidden_grad)
    grad_up_bias = column_sum(hidden_grad)
    grad_middle = grad_sum2 + reverse_projection(hidden_grad, up_weight)
    grad_residual, grad_gain1, grad_shift1 = norm1_pull(grad_middle)
    branch_grad = grad_residual.astype(jnp.bfloat16)
    grad_out = weight_grad(attended_low, branch_grad)
    grad_out_bias = column_sum(branch_grad)

    with jax.named_scope("scatter_late"):
        late_pack = jnp.concatenate(
            [
                grad_up.astype(GRAD_WIRE),
                grad_down.astype(GRAD_WIRE).reshape(width, ff_ratio * width),
                grad_out.astype(GRAD_WIRE),
                pack_vectors(
                    width,
                    (
                        grad_up_bias,
                        grad_down_bias,
                        grad_gain2,
                        grad_shift2,
                        grad_out_bias,
                        grad_gain1,
                        grad_shift1,
                    ),
                    GRAD_WIRE,
                ),
            ],
            axis=1,
        )
        late_pack, branch_grad = lax.optimization_barrier((late_pack, branch_grad))
        late_own = scatter_rows(late_pack)
    grad_down_own = late_own[:, ff_width : 2 * ff_width].reshape(shard_rows * ff_ratio, width)
    late_own = jnp.concatenate([late_own[:, 0:ff_width], late_own[:, 2 * ff_width :]], axis=1)
    grad_up_own = late_own[:, 0:ff_width]
    grad_out_own = late_own[:, ff_width : ff_width + width]
    (
        grad_up_bias_own,
        grad_down_bias_own,
        grad_gain2_own,
        grad_shift2_own,
        grad_out_bias_own,
        grad_gain1_own,
        grad_shift1_own,
    ) = unpack_vectors(late_own[:, ff_width + width :], (ff_ratio, 1, 1, 1, 1, 1, 1))

    attended_grad = (
        reverse_projection(branch_grad, out_weight).astype(jnp.bfloat16).reshape(head_shape)
    )
    scores_again = attention_scores(query_heads, key_heads, valid_keys, scale)
    probs = jnp.exp(scores_again - log_total)
    probs_again = probs.astype(jnp.bfloat16)
    probs_grad = jnp.einsum(
        "sqhd,skhd->shqk", attended_grad, value_heads, preferred_element_type=jnp.float32
    )
    values_grad = jnp.einsum(
        "shqk,sqhd->skhd", probs_again, attended_grad, preferred_element_type=jnp.float32
    )
    values_grad = values_grad.astype(jnp.bfloat16).reshape(row_count, width)
    inner_sum = jnp.sum(probs * probs_grad, axis=-1, keepdims=True)
    scores_grad = (probs * (probs_grad - inner_sum)).astype(jnp.bfloat16)
    query_grad = jnp.einsum(
        "shqk,skhd->sqhd", scores_grad, key_heads, preferred_element_type=jnp.float32
    )
    query_grad = (query_grad * scale).astype(jnp.bfloat16).reshape(row_count, width)
    keys_grad = jnp.einsum(
        "shqk,sqhd->skhd", scores_grad, query_heads, preferred_element_type=jnp.float32
    )
    keys_grad = (keys_grad * scale).astype(jnp.bfloat16).reshape(row_count, width)
    grad_query = weight_grad(flat_in, query_grad)
    grad_query_bias = column_sum(query_grad)
    grad_key = weight_grad(flat_in, keys_grad)
    grad_value = weight_grad(flat_in, values_grad)
    value_bias_gradient = column_sum(values_grad)
    grad_input = (
        grad_residual
        + reverse_projection(query_grad, query_weight)
        + reverse_projection(keys_grad, key_weight)
        + reverse_projection(values_grad, value_weight)
    )
    with jax.named_scope("scatter_qkv"):
        query_own_pack = tree_scatter(
            jnp.concatenate(
                [
                    grad_query,
                    pack_vectors(width, (grad_query_bias, value_bias_gradient), jnp.float32),
                ],
                axis=1,
            ),
            0,
        )
        grad_key_own = tree_scatter(grad_key, 1)
        grad_value_own = tree_scatter(grad_value, 2)
    grad_query_own = query_own_pack[:, 0:width]
    grad_query_bias_own, value_bias_gradient_own = unpack_vectors(
        query_own_pack[:, width:], (1, 1)
    )
    return (
        output.astype(jnp.bfloat16).reshape(inputs.shape),
        grad_input.astype(jnp.bfloat16).reshape(inputs.shape),
        grad_query_own,
        grad_query_bias_own,
        grad_key_own,
        grad_value_own,
        value_bias_gradient_own,
        grad_out_own,
        grad_out_bias_own,
        grad_gain1_own,
        grad_shift1_own,
        grad_up_own,
        grad_up_bias_own,
        grad_down_own,
        grad_down_bias_own,
        grad_gain2_own,
        grad_shift2_own,
    )


def solution(mesh):
    rows3 = P(AXES, None, None)
    rows2 = P(AXES, None)
    rows1 = P(AXES)
    return jax.shard_map(
        body,
        mesh=mesh,
        in_specs=(
            rows3,
            rows1,
            rows2,
            rows3,
            rows2,
            rows1,
            rows2,
            rows2,
            rows1,
            rows2,
            rows1,
            rows1,
            rows1,
            rows2,
            rows1,
            rows2,
            rows1,
            rows1,
            rows1,
        ),
        out_specs=(
            rows3,
            rows3,
            rows2,
            rows1,
            rows2,
            rows2,
            rows1,
            rows2,
            rows1,
            rows1,
            rows1,
            rows2,
            rows1,
            rows2,
            rows1,
            rows1,
            rows1,
        ),
        check_vma=False,
    )
```

```python
import jax
import jax.numpy as jnp
from jax import lax
from jax.sharding import PartitionSpec as P

HD = 64
EPSILON = 1e-06
AXES = ("fsdp", "sub")
GRAD_WIRE = jnp.bfloat16
VEC_COLS = 256


def layer_norm(values, gain, shift):
    average = jnp.mean(values, axis=-1, keepdims=True)
    centered = values - average
    variance = jnp.mean(centered * centered, axis=-1, keepdims=True)
    return centered * lax.rsqrt(variance + EPSILON) * gain + shift


def gelu_exact(values):
    return values * (0.5 * (1.0 + lax.erf(values * (2.0 ** -0.5))))


def project(rows_low, weight):
    return jnp.dot(rows_low, weight, preferred_element_type=jnp.float32)


def reverse_projection(grad_low, weight):
    return lax.dot_general(
        grad_low, weight, (((1,), (1,)), ((), ())), preferred_element_type=jnp.float32
    )


def weight_grad(rows_low, grad_low):
    return lax.dot_general(
        rows_low, grad_low, (((0,), (0,)), ((), ())), preferred_element_type=jnp.float32
    )


def column_sum(grad_low):
    return jnp.sum(grad_low.astype(jnp.float32), axis=0)


def attention_scores(query_heads, key_heads, valid_keys, scale):
    scores = (
        jnp.einsum("shqd,shkd->shqk", query_heads, key_heads, preferred_element_type=jnp.float32)
        * scale
    )
    return jnp.where(valid_keys[:, None, None, :], scores, -1e30)


def pack_vectors(rows, vectors, dtype):
    cols = [v.reshape(rows, -1).astype(dtype) for v in vectors]
    block = jnp.concatenate(cols, axis=1)
    return jnp.pad(block, ((0, 0), (0, VEC_COLS - block.shape[1])))


def unpack_vectors(block, widths):
    out, at = [], 0
    for width in widths:
        out.append(block[:, at : at + width].reshape(-1))
        at += width
    return out


def gather_rows(pack):
    return lax.all_gather(pack, AXES, axis=0, tiled=True)


def scatter_rows(pack):
    return lax.psum_scatter(pack.astype(GRAD_WIRE), AXES, scatter_dimension=0, tiled=True).astype(
        jnp.float32
    )


def _pick(bit, first, second):
    return jnp.where(bit == 0, first, second), jnp.where(bit == 0, second, first)


def tree_gather(block, last_bit):
    n_sub = lax.axis_size("sub")
    n_f = lax.axis_size("fsdp")
    bits = n_f.bit_length() - 1
    chip = lax.axis_index("fsdp")
    order = [b for b in range(bits - 1, -1, -1) if b != last_bit] + [last_bit]
    acc = block
    done = []
    for j in order:
        pairs = [(g, g ^ (1 << j)) for g in range(n_f)]
        recv = lax.ppermute(acc, "fsdp", pairs)
        bit = (chip >> j) & 1
        lo, hi = _pick(bit, acc, recv)
        axis = sum(1 for b in done if b > j)
        acc = jnp.stack([lo, hi], axis=axis)
        done.append(j)
    acc = acc.reshape((n_f,) + block.shape)
    core = lax.axis_index("sub")
    recv = lax.ppermute(acc, "sub", [(0, 1), (1, 0)])
    lo, hi = _pick(core, acc, recv)
    full = jnp.stack([lo, hi], axis=1)
    return full.reshape((n_f * n_sub * block.shape[0],) + block.shape[1:])


def tree_scatter(full, first_bit):
    n_sub = lax.axis_size("sub")
    n_f = lax.axis_size("fsdp")
    rows = full.shape[0] // (n_sub * n_f)
    acc = full.reshape(n_f, n_sub, rows, -1)
    core = lax.axis_index("sub")
    keep = lax.dynamic_index_in_dim(acc, core, 1, keepdims=False)
    send = lax.dynamic_index_in_dim(acc, 1 - core, 1, keepdims=False)
    acc = keep + lax.ppermute(send, "sub", [(0, 1), (1, 0)])
    chip = lax.axis_index("fsdp")
    bits = n_f.bit_length() - 1
    acc = acc.reshape((2,) * bits + (rows, -1))
    left = list(range(bits - 1, -1, -1))
    order = [first_bit] + [b for b in range(bits) if b != first_bit]
    for j in order:
        axis = left.index(j)
        left.remove(j)
        bit = (chip >> j) & 1
        keep = lax.dynamic_index_in_dim(acc, bit, axis, keepdims=False)
        send = lax.dynamic_index_in_dim(acc, 1 - bit, axis, keepdims=False)
        pairs = [(g, g ^ (1 << j)) for g in range(n_f)]
        recv = lax.ppermute(send.astype(GRAD_WIRE), "fsdp", pairs)
        acc = keep + recv.astype(jnp.float32)
    return acc.reshape(rows, -1)


def body(
    inputs,
    lengths,
    positions,
    masked_output_gradient,
    w_query,
    b_query,
    w_key,
    w_value,
    b_value,
    w_out,
    b_out,
    gain_attn,
    shift_attn,
    w_up,
    b_up,
    w_down,
    b_down,
    gain_ffn,
    shift_ffn,
):
    seq_count, seq_slots, width = inputs.shape
    head_count = width // HD
    scale = HD ** (-0.5)
    row_count = seq_count * seq_slots
    head_shape = (seq_count, seq_slots, head_count, HD)
    shard_rows = w_query.shape[0]
    ff_ratio = w_down.shape[0] // shard_rows
    ff_width = w_up.shape[1]
    token_ids = jnp.arange(seq_slots, dtype=jnp.int32)
    valid_keys = token_ids[None, :] < lengths[:, None]

    with jax.named_scope("gather_attn"):
        vec_pack = pack_vectors(
            shard_rows, (b_query, b_value, b_out, gain_attn, shift_attn), jnp.bfloat16
        )
        cut = (width // 6, width * 2 // 3)
        query_part = tree_gather(
            jnp.concatenate([w_query, w_value[:, : cut[0]], vec_pack], axis=1), 0
        )
        key_part = tree_gather(jnp.concatenate([w_key, w_value[:, cut[0] : cut[1]]], axis=1), 1)
        out_part = tree_gather(jnp.concatenate([w_value[:, cut[1] :], w_out], axis=1), 2)
    query_weight = query_part[:, 0:width]
    key_weight = key_part[:, 0:width]
    value_weight = jnp.concatenate(
        [
            query_part[:, width : width + cut[0]],
            key_part[:, width:],
            out_part[:, : width - cut[1]],
        ],
        axis=1,
    )
    out_weight = out_part[:, width - cut[1] :]
    vec_start = width + cut[0]
    query_bias, value_bias, out_bias, norm1_gain, norm1_shift = unpack_vectors(
        query_part[:, vec_start:], (1, 1, 1, 1, 1)
    )

    with jax.named_scope("gather_ffn"):
        ffn_pack = jnp.concatenate(
            [
                w_up,
                pack_vectors(
                    shard_rows, (b_up, b_down, gain_ffn, shift_ffn), jnp.bfloat16
                ),
            ],
            axis=1,
        )
        ffn_full = gather_rows(ffn_pack)
        down_weight = gather_rows(w_down)
    up_weight = ffn_full[:, 0:ff_width]
    up_bias, downward_bias, norm2_gain, norm2_shift = unpack_vectors(
        ffn_full[:, ff_width:], (ff_ratio, 1, 1, 1)
    )

    flat_in = inputs.reshape(row_count, width)
    input_rows = flat_in.astype(jnp.float32)
    head_weights = (head_count, HD)
    query_w3 = query_weight.reshape((width,) + head_weights)
    key_w3 = key_weight.reshape((width,) + head_weights)
    value_w3 = value_weight.reshape((width,) + head_weights)
    out_w3 = out_weight.reshape(head_weights + (width,))
    query_heads = (
        jnp.einsum("snc,chd->shnd", inputs, query_w3, preferred_element_type=jnp.float32)
        + query_bias.astype(jnp.float32).reshape(head_weights)[None, :, None, :]
    ).astype(jnp.bfloat16)
    key_heads = jnp.einsum(
        "snc,chd->shnd", inputs, key_w3, preferred_element_type=jnp.float32
    ).astype(jnp.bfloat16)
    value_heads = (
        jnp.einsum("snc,chd->shnd", inputs, value_w3, preferred_element_type=jnp.float32)
        + value_bias.astype(jnp.float32).reshape(head_weights)[None, :, None, :]
    ).astype(jnp.bfloat16)
    scores = attention_scores(query_heads, key_heads, valid_keys, scale)
    row_top = jnp.max(scores, axis=-1, keepdims=True)
    expon = jnp.exp(scores - row_top)
    row_total = jnp.sum(expon, axis=-1, keepdims=True)
    log_total = row_top + jnp.log(row_total)
    probs_low = (expon / row_total).astype(jnp.bfloat16)
    attention_mixed = jnp.einsum(
        "shqk,shkd->shqd", probs_low, value_heads, preferred_element_type=jnp.float32
    )
    attended_low = attention_mixed.astype(jnp.bfloat16)
    branch = (
        jnp.einsum("shqd,hdc->sqc", attended_low, out_w3, preferred_element_type=jnp.float32)
        .reshape(row_count, width)
    ) + out_bias.astype(jnp.float32)
    middle, norm1_pull = jax.vjp(
        layer_norm,
        input_rows + branch,
        norm1_gain.astype(jnp.float32),
        norm1_shift.astype(jnp.float32),
    )
    middle_low = middle.astype(jnp.bfloat16)
    hidden = project(middle_low, up_weight) + up_bias.astype(jnp.float32)
    active, gelu_pull = jax.vjp(gelu_exact, hidden)
    active_low = active.astype(jnp.bfloat16)
    second_branch = project(active_low, down_weight) + downward_bias.astype(jnp.float32)
    output, norm2_pull = jax.vjp(
        layer_norm,
        middle + second_branch,
        norm2_gain.astype(jnp.float32),
        norm2_shift.astype(jnp.float32),
    )
    position_matches = (positions[:, :, None] == token_ids[None, None, :]).astype(jnp.bfloat16)
    cotangent = jnp.einsum(
        "efw,efv->ewv", position_matches, masked_output_gradient, preferred_element_type=jnp.float32
    ).reshape(row_count, width)
    grad_sum2, grad_gain2, grad_shift2 = norm2_pull(cotangent)
    second_grad = grad_sum2.astype(jnp.bfloat16)
    grad_down = weight_grad(active_low, second_grad)
    grad_down_bias = column_sum(second_grad)
    (grad_hidden,) = gelu_pull(reverse_projection(second_grad, down_weight))
    hidden_grad = grad_hidden.astype(jnp.bfloat16)
    grad_up = weight_grad(middle_low, hidden_grad)
    grad_up_bias = column_sum(hidden_grad)
    grad_middle = grad_sum2 + reverse_projection(hidden_grad, up_weight)
    grad_residual, grad_gain1, grad_shift1 = norm1_pull(grad_middle)
    branch_grad = grad_residual.astype(jnp.bfloat16)
    grad_out = jnp.einsum(
        "shqd,sqc->hdc", attended_low, branch_grad.reshape(inputs.shape),
        preferred_element_type=jnp.float32,
    ).reshape(width, width)
    grad_out_bias = column_sum(branch_grad)

    with jax.named_scope("scatter_late"):
        late_pack = jnp.concatenate(
            [
                grad_up.astype(GRAD_WIRE),
                grad_down.astype(GRAD_WIRE).reshape(width, ff_ratio * width),
                grad_out.astype(GRAD_WIRE),
                pack_vectors(
                    width,
                    (
                        grad_up_bias,
                        grad_down_bias,
                        grad_gain2,
                        grad_shift2,
                        grad_out_bias,
                        grad_gain1,
                        grad_shift1,
                    ),
                    GRAD_WIRE,
                ),
            ],
            axis=1,
        )
        late_pack, branch_grad = lax.optimization_barrier((late_pack, branch_grad))
        late_own = scatter_rows(late_pack)
    grad_down_own = late_own[:, ff_width : 2 * ff_width].reshape(shard_rows * ff_ratio, width)
    late_own = jnp.concatenate([late_own[:, 0:ff_width], late_own[:, 2 * ff_width :]], axis=1)
    grad_up_own = late_own[:, 0:ff_width]
    grad_out_own = late_own[:, ff_width : ff_width + width]
    (
        grad_up_bias_own,
        grad_down_bias_own,
        grad_gain2_own,
        grad_shift2_own,
        grad_out_bias_own,
        grad_gain1_own,
        grad_shift1_own,
    ) = unpack_vectors(late_own[:, ff_width + width :], (ff_ratio, 1, 1, 1, 1, 1, 1))

    attended_grad = (
        reverse_projection(branch_grad, out_weight).astype(jnp.bfloat16).reshape(head_shape)
    )
    scores_again = attention_scores(query_heads, key_heads, valid_keys, scale)
    probs = jnp.exp(scores_again - log_total)
    probs_again = probs.astype(jnp.bfloat16)
    probs_grad = jnp.einsum(
        "sqhd,shkd->shqk", attended_grad, value_heads, preferred_element_type=jnp.float32
    )
    values_grad = jnp.einsum(
        "shqk,sqhd->skhd", probs_again, attended_grad, preferred_element_type=jnp.float32
    )
    values_grad = values_grad.astype(jnp.bfloat16).reshape(row_count, width)
    inner_sum = jnp.sum(probs * probs_grad, axis=-1, keepdims=True)
    scores_grad = (probs * (probs_grad - inner_sum)).astype(jnp.bfloat16)
    query_grad = jnp.einsum(
        "shqk,shkd->sqhd", scores_grad, key_heads, preferred_element_type=jnp.float32
    )
    query_grad = (query_grad * scale).astype(jnp.bfloat16).reshape(row_count, width)
    keys_grad = jnp.einsum(
        "shqk,shqd->skhd", scores_grad, query_heads, preferred_element_type=jnp.float32
    )
    keys_grad = (keys_grad * scale).astype(jnp.bfloat16).reshape(row_count, width)
    grad_query = weight_grad(flat_in, query_grad)
    grad_query_bias = column_sum(query_grad)
    grad_key = weight_grad(flat_in, keys_grad)
    grad_value = weight_grad(flat_in, values_grad)
    value_bias_gradient = column_sum(values_grad)
    grad_input = (
        grad_residual
        + reverse_projection(query_grad, query_weight)
        + reverse_projection(keys_grad, key_weight)
        + reverse_projection(values_grad, value_weight)
    )
    with jax.named_scope("scatter_qkv"):
        query_own_pack = tree_scatter(
            jnp.concatenate(
                [
                    grad_query,
                    pack_vectors(width, (grad_query_bias, value_bias_gradient), jnp.float32),
                ],
                axis=1,
            ),
            0,
        )
        grad_key_own = tree_scatter(grad_key, 1)
        grad_value_own = tree_scatter(grad_value, 2)
    grad_query_own = query_own_pack[:, 0:width]
    grad_query_bias_own, value_bias_gradient_own = unpack_vectors(
        query_own_pack[:, width:], (1, 1)
    )
    return (
        output.astype(jnp.bfloat16).reshape(inputs.shape),
        grad_input.astype(jnp.bfloat16).reshape(inputs.shape),
        grad_query_own,
        grad_query_bias_own,
        grad_key_own,
        grad_value_own,
        value_bias_gradient_own,
        grad_out_own,
        grad_out_bias_own,
        grad_gain1_own,
        grad_shift1_own,
        grad_up_own,
        grad_up_bias_own,
        grad_down_own,
        grad_down_bias_own,
        grad_gain2_own,
        grad_shift2_own,
    )


def solution(mesh):
    rows3 = P(AXES, None, None)
    rows2 = P(AXES, None)
    rows1 = P(AXES)
    return jax.shard_map(
        body,
        mesh=mesh,
        in_specs=(
            rows3,
            rows1,
            rows2,
            rows3,
            rows2,
            rows1,
            rows2,
            rows2,
            rows1,
            rows2,
            rows1,
            rows1,
            rows1,
            rows2,
            rows1,
            rows2,
            rows1,
            rows1,
            rows1,
        ),
        out_specs=(
            rows3,
            rows3,
            rows2,
            rows1,
            rows2,
            rows2,
            rows1,
            rows2,
            rows1,
            rows1,
            rows1,
            rows2,
            rows1,
            rows2,
            rows1,
            rows1,
            rows1,
        ),
        check_vma=False,
    )
```

```python
import jax
import jax.numpy as jnp
from jax import lax
from jax.sharding import PartitionSpec as P

HD = 64
EPSILON = 1e-06
AXES = ("fsdp", "sub")
GRAD_WIRE = jnp.bfloat16
VEC_COLS = 256


def layer_norm(values, gain, shift):
    average = jnp.mean(values, axis=-1, keepdims=True)
    centered = values - average
    variance = jnp.mean(centered * centered, axis=-1, keepdims=True)
    return centered * lax.rsqrt(variance + EPSILON) * gain + shift


def gelu_exact(values):
    return values * (0.5 * (1.0 + lax.erf(values * (2.0 ** -0.5))))


def project(rows_low, weight):
    return jnp.dot(rows_low, weight, preferred_element_type=jnp.float32)


def reverse_projection(grad_low, weight):
    return lax.dot_general(
        grad_low, weight, (((1,), (1,)), ((), ())), preferred_element_type=jnp.float32
    )


def weight_grad(rows_low, grad_low):
    return lax.dot_general(
        rows_low, grad_low, (((0,), (0,)), ((), ())), preferred_element_type=jnp.float32
    )


def column_sum(grad_low):
    return jnp.sum(grad_low.astype(jnp.float32), axis=0)


def attention_scores(query_heads, key_heads, valid_keys, scale):
    scores = (
        jnp.einsum("shqd,shkd->shqk", query_heads, key_heads, preferred_element_type=jnp.float32)
        * scale
    )
    return jnp.where(valid_keys[:, None, None, :], scores, -1e30)


def pack_vectors(rows, vectors, dtype):
    cols = [v.reshape(rows, -1).astype(dtype) for v in vectors]
    block = jnp.concatenate(cols, axis=1)
    return jnp.pad(block, ((0, 0), (0, VEC_COLS - block.shape[1])))


def unpack_vectors(block, widths):
    out, at = [], 0
    for width in widths:
        out.append(block[:, at : at + width].reshape(-1))
        at += width
    return out


def gather_rows(pack):
    return lax.all_gather(pack, AXES, axis=0, tiled=True)


def scatter_rows(pack):
    return lax.psum_scatter(pack.astype(GRAD_WIRE), AXES, scatter_dimension=0, tiled=True).astype(
        jnp.float32
    )


def _pick(bit, first, second):
    return jnp.where(bit == 0, first, second), jnp.where(bit == 0, second, first)


def tree_gather(block, last_bit):
    n_sub = lax.axis_size("sub")
    n_f = lax.axis_size("fsdp")
    bits = n_f.bit_length() - 1
    chip = lax.axis_index("fsdp")
    order = [b for b in range(bits - 1, -1, -1) if b != last_bit] + [last_bit]
    acc = block
    done = []
    for j in order:
        pairs = [(g, g ^ (1 << j)) for g in range(n_f)]
        recv = lax.ppermute(acc, "fsdp", pairs)
        bit = (chip >> j) & 1
        lo, hi = _pick(bit, acc, recv)
        axis = sum(1 for b in done if b > j)
        acc = jnp.stack([lo, hi], axis=axis)
        done.append(j)
    acc = acc.reshape((n_f,) + block.shape)
    core = lax.axis_index("sub")
    recv = lax.ppermute(acc, "sub", [(0, 1), (1, 0)])
    lo, hi = _pick(core, acc, recv)
    full = jnp.stack([lo, hi], axis=1)
    return full.reshape((n_f * n_sub * block.shape[0],) + block.shape[1:])


def tree_scatter(full, first_bit):
    n_sub = lax.axis_size("sub")
    n_f = lax.axis_size("fsdp")
    rows = full.shape[0] // (n_sub * n_f)
    acc = full.reshape(n_f, n_sub, rows, -1)
    core = lax.axis_index("sub")
    keep = lax.dynamic_index_in_dim(acc, core, 1, keepdims=False)
    send = lax.dynamic_index_in_dim(acc, 1 - core, 1, keepdims=False)
    acc = keep + lax.ppermute(send, "sub", [(0, 1), (1, 0)])
    chip = lax.axis_index("fsdp")
    bits = n_f.bit_length() - 1
    acc = acc.reshape((2,) * bits + (rows, -1))
    left = list(range(bits - 1, -1, -1))
    order = [first_bit] + [b for b in range(bits) if b != first_bit]
    for j in order:
        axis = left.index(j)
        left.remove(j)
        bit = (chip >> j) & 1
        keep = lax.dynamic_index_in_dim(acc, bit, axis, keepdims=False)
        send = lax.dynamic_index_in_dim(acc, 1 - bit, axis, keepdims=False)
        pairs = [(g, g ^ (1 << j)) for g in range(n_f)]
        recv = lax.ppermute(send.astype(GRAD_WIRE), "fsdp", pairs)
        acc = keep + recv.astype(jnp.float32)
    return acc.reshape(rows, -1)


def body(
    inputs,
    lengths,
    positions,
    masked_output_gradient,
    w_query,
    b_query,
    w_key,
    w_value,
    b_value,
    w_out,
    b_out,
    gain_attn,
    shift_attn,
    w_up,
    b_up,
    w_down,
    b_down,
    gain_ffn,
    shift_ffn,
):
    seq_count, seq_slots, width = inputs.shape
    head_count = width // HD
    scale = HD ** (-0.5)
    row_count = seq_count * seq_slots
    head_shape = (seq_count, seq_slots, head_count, HD)
    shard_rows = w_query.shape[0]
    ff_ratio = w_down.shape[0] // shard_rows
    ff_width = w_up.shape[1]
    token_ids = jnp.arange(seq_slots, dtype=jnp.int32)
    valid_keys = token_ids[None, :] < lengths[:, None]

    with jax.named_scope("gather_attn"):
        vec_pack = pack_vectors(
            shard_rows, (b_query, b_value, b_out, gain_attn, shift_attn), jnp.bfloat16
        )
        cut = (width // 6, width * 2 // 3)
        query_part = tree_gather(
            jnp.concatenate([w_query, w_value[:, : cut[0]], vec_pack], axis=1), 0
        )
        key_part = tree_gather(jnp.concatenate([w_key, w_value[:, cut[0] : cut[1]]], axis=1), 1)
        out_part = tree_gather(jnp.concatenate([w_value[:, cut[1] :], w_out], axis=1), 2)
    query_weight = query_part[:, 0:width]
    key_weight = key_part[:, 0:width]
    value_weight = jnp.concatenate(
        [
            query_part[:, width : width + cut[0]],
            key_part[:, width:],
            out_part[:, : width - cut[1]],
        ],
        axis=1,
    )
    out_weight = out_part[:, width - cut[1] :]
    vec_start = width + cut[0]
    query_bias, value_bias, out_bias, norm1_gain, norm1_shift = unpack_vectors(
        query_part[:, vec_start:], (1, 1, 1, 1, 1)
    )

    with jax.named_scope("gather_ffn"):
        ffn_pack = jnp.concatenate(
            [
                w_up,
                pack_vectors(
                    shard_rows, (b_up, b_down, gain_ffn, shift_ffn), jnp.bfloat16
                ),
            ],
            axis=1,
        )
        ffn_full = gather_rows(ffn_pack)
        late_w_down, _ = lax.optimization_barrier((w_down, (query_part, key_part, out_part)))
        third = width // 3
        down_weight = jnp.concatenate(
            [
                tree_gather(late_w_down[:, part * third : (part + 1) * third], part)
                for part in range(3)
            ],
            axis=1,
        )
    up_weight = ffn_full[:, 0:ff_width]
    up_bias, downward_bias, norm2_gain, norm2_shift = unpack_vectors(
        ffn_full[:, ff_width:], (ff_ratio, 1, 1, 1)
    )

    flat_in = inputs.reshape(row_count, width)
    input_rows = flat_in.astype(jnp.float32)
    head_weights = (head_count, HD)
    query_w3 = query_weight.reshape((width,) + head_weights)
    key_w3 = key_weight.reshape((width,) + head_weights)
    value_w3 = value_weight.reshape((width,) + head_weights)
    out_w3 = out_weight.reshape(head_weights + (width,))
    query_heads = (
        jnp.einsum("snc,chd->shnd", inputs, query_w3, preferred_element_type=jnp.float32)
        + query_bias.astype(jnp.float32).reshape(head_weights)[None, :, None, :]
    ).astype(jnp.bfloat16)
    key_heads = jnp.einsum(
        "snc,chd->shnd", inputs, key_w3, preferred_element_type=jnp.float32
    ).astype(jnp.bfloat16)
    value_heads = (
        jnp.einsum("snc,chd->shnd", inputs, value_w3, preferred_element_type=jnp.float32)
        + value_bias.astype(jnp.float32).reshape(head_weights)[None, :, None, :]
    ).astype(jnp.bfloat16)
    scores = attention_scores(query_heads, key_heads, valid_keys, scale)
    row_top = jnp.max(scores, axis=-1, keepdims=True)
    expon = jnp.exp(scores - row_top)
    row_total = jnp.sum(expon, axis=-1, keepdims=True)
    log_total = row_top + jnp.log(row_total)
    probs_low = (expon / row_total).astype(jnp.bfloat16)
    attention_mixed = jnp.einsum(
        "shqk,shkd->shqd", probs_low, value_heads, preferred_element_type=jnp.float32
    )
    attended_low = attention_mixed.astype(jnp.bfloat16)
    branch = (
        jnp.einsum("shqd,hdc->sqc", attended_low, out_w3, preferred_element_type=jnp.float32)
        .reshape(row_count, width)
    ) + out_bias.astype(jnp.float32)
    middle, norm1_pull = jax.vjp(
        layer_norm,
        input_rows + branch,
        norm1_gain.astype(jnp.float32),
        norm1_shift.astype(jnp.float32),
    )
    middle_low = middle.astype(jnp.bfloat16)
    hidden = project(middle_low, up_weight) + up_bias.astype(jnp.float32)
    active, gelu_pull = jax.vjp(gelu_exact, hidden)
    active_low = active.astype(jnp.bfloat16)
    second_branch = project(active_low, down_weight) + downward_bias.astype(jnp.float32)
    output, norm2_pull = jax.vjp(
        layer_norm,
        middle + second_branch,
        norm2_gain.astype(jnp.float32),
        norm2_shift.astype(jnp.float32),
    )
    position_matches = (positions[:, :, None] == token_ids[None, None, :]).astype(jnp.bfloat16)
    cotangent = jnp.einsum(
        "efw,efv->ewv", position_matches, masked_output_gradient, preferred_element_type=jnp.float32
    ).reshape(row_count, width)
    grad_sum2, grad_gain2, grad_shift2 = norm2_pull(cotangent)
    second_grad = grad_sum2.astype(jnp.bfloat16)
    grad_down = weight_grad(active_low, second_grad)
    grad_down_bias = column_sum(second_grad)
    (grad_hidden,) = gelu_pull(reverse_projection(second_grad, down_weight))
    hidden_grad = grad_hidden.astype(jnp.bfloat16)
    grad_up = weight_grad(middle_low, hidden_grad)
    grad_up_bias = column_sum(hidden_grad)
    grad_middle = grad_sum2 + reverse_projection(hidden_grad, up_weight)
    grad_residual, grad_gain1, grad_shift1 = norm1_pull(grad_middle)
    branch_grad = grad_residual.astype(jnp.bfloat16)
    grad_out = jnp.einsum(
        "shqd,sqc->hdc", attended_low, branch_grad.reshape(inputs.shape),
        preferred_element_type=jnp.float32,
    ).reshape(width, width)
    grad_out_bias = column_sum(branch_grad)

    with jax.named_scope("scatter_late"):
        late_pack = jnp.concatenate(
            [
                grad_up.astype(GRAD_WIRE),
                grad_down.astype(GRAD_WIRE).reshape(width, ff_ratio * width),
                grad_out.astype(GRAD_WIRE),
                pack_vectors(
                    width,
                    (
                        grad_up_bias,
                        grad_down_bias,
                        grad_gain2,
                        grad_shift2,
                        grad_out_bias,
                        grad_gain1,
                        grad_shift1,
                    ),
                    GRAD_WIRE,
                ),
            ],
            axis=1,
        )
        late_pack, branch_grad = lax.optimization_barrier((late_pack, branch_grad))
        late_own = scatter_rows(late_pack)
    grad_down_own = late_own[:, ff_width : 2 * ff_width].reshape(shard_rows * ff_ratio, width)
    late_own = jnp.concatenate([late_own[:, 0:ff_width], late_own[:, 2 * ff_width :]], axis=1)
    grad_up_own = late_own[:, 0:ff_width]
    grad_out_own = late_own[:, ff_width : ff_width + width]
    (
        grad_up_bias_own,
        grad_down_bias_own,
        grad_gain2_own,
        grad_shift2_own,
        grad_out_bias_own,
        grad_gain1_own,
        grad_shift1_own,
    ) = unpack_vectors(late_own[:, ff_width + width :], (ff_ratio, 1, 1, 1, 1, 1, 1))

    attended_grad = (
        reverse_projection(branch_grad, out_weight).astype(jnp.bfloat16).reshape(head_shape)
    )
    scores_again = attention_scores(query_heads, key_heads, valid_keys, scale)
    probs = jnp.exp(scores_again - log_total)
    probs_again = probs.astype(jnp.bfloat16)
    probs_grad = jnp.einsum(
        "sqhd,shkd->shqk", attended_grad, value_heads, preferred_element_type=jnp.float32
    )
    values_grad = jnp.einsum(
        "shqk,sqhd->skhd", probs_again, attended_grad, preferred_element_type=jnp.float32
    )
    values_grad = values_grad.astype(jnp.bfloat16).reshape(row_count, width)
    inner_sum = jnp.sum(probs * probs_grad, axis=-1, keepdims=True)
    scores_grad = (probs * (probs_grad - inner_sum)).astype(jnp.bfloat16)
    query_grad = jnp.einsum(
        "shqk,shkd->sqhd", scores_grad, key_heads, preferred_element_type=jnp.float32
    )
    query_grad = (query_grad * scale).astype(jnp.bfloat16).reshape(row_count, width)
    keys_grad = jnp.einsum(
        "shqk,shqd->skhd", scores_grad, query_heads, preferred_element_type=jnp.float32
    )
    keys_grad = (keys_grad * scale).astype(jnp.bfloat16).reshape(row_count, width)
    grad_query = weight_grad(flat_in, query_grad)
    grad_query_bias = column_sum(query_grad)
    grad_key = weight_grad(flat_in, keys_grad)
    grad_value = weight_grad(flat_in, values_grad)
    value_bias_gradient = column_sum(values_grad)
    grad_input = (
        grad_residual
        + reverse_projection(query_grad, query_weight)
        + reverse_projection(keys_grad, key_weight)
        + reverse_projection(values_grad, value_weight)
    )
    with jax.named_scope("scatter_qkv"):
        query_own_pack = tree_scatter(
            jnp.concatenate(
                [
                    grad_query,
                    pack_vectors(width, (grad_query_bias, value_bias_gradient), jnp.float32),
                ],
                axis=1,
            ),
            0,
        )
        grad_key_own = tree_scatter(grad_key, 1)
        grad_value_own = tree_scatter(grad_value, 2)
    grad_query_own = query_own_pack[:, 0:width]
    grad_query_bias_own, value_bias_gradient_own = unpack_vectors(
        query_own_pack[:, width:], (1, 1)
    )
    return (
        output.astype(jnp.bfloat16).reshape(inputs.shape),
        grad_input.astype(jnp.bfloat16).reshape(inputs.shape),
        grad_query_own,
        grad_query_bias_own,
        grad_key_own,
        grad_value_own,
        value_bias_gradient_own,
        grad_out_own,
        grad_out_bias_own,
        grad_gain1_own,
        grad_shift1_own,
        grad_up_own,
        grad_up_bias_own,
        grad_down_own,
        grad_down_bias_own,
        grad_gain2_own,
        grad_shift2_own,
    )


def solution(mesh):
    rows3 = P(AXES, None, None)
    rows2 = P(AXES, None)
    rows1 = P(AXES)
    return jax.shard_map(
        body,
        mesh=mesh,
        in_specs=(
            rows3,
            rows1,
            rows2,
            rows3,
            rows2,
            rows1,
            rows2,
            rows2,
            rows1,
            rows2,
            rows1,
            rows1,
            rows1,
            rows2,
            rows1,
            rows2,
            rows1,
            rows1,
            rows1,
        ),
        out_specs=(
            rows3,
            rows3,
            rows2,
            rows1,
            rows2,
            rows2,
            rows1,
            rows2,
            rows1,
            rows1,
            rows1,
            rows2,
            rows1,
            rows2,
            rows1,
            rows1,
            rows1,
        ),
        check_vma=False,
    )
```

```python
import jax
import jax.numpy as jnp
from jax import lax
from jax.sharding import PartitionSpec as P

HD = 64
EPSILON = 1e-06
AXES = ("fsdp", "sub")
GRAD_WIRE = jnp.bfloat16
VEC_COLS = 256


def layer_norm(values, gain, shift):
    average = jnp.mean(values, axis=-1, keepdims=True)
    centered = values - average
    variance = jnp.mean(centered * centered, axis=-1, keepdims=True)
    return centered * lax.rsqrt(variance + EPSILON) * gain + shift


def gelu_exact(values):
    return values * (0.5 * (1.0 + lax.erf(values * (2.0 ** -0.5))))


def project(rows_low, weight):
    return jnp.dot(rows_low, weight, preferred_element_type=jnp.float32)


def reverse_projection(grad_low, weight):
    return lax.dot_general(
        grad_low, weight, (((1,), (1,)), ((), ())), preferred_element_type=jnp.float32
    )


def weight_grad(rows_low, grad_low):
    return lax.dot_general(
        rows_low, grad_low, (((0,), (0,)), ((), ())), preferred_element_type=jnp.float32
    )


def column_sum(grad_low):
    return jnp.sum(grad_low.astype(jnp.float32), axis=0)


def attention_scores(query_heads, key_heads, valid_keys, scale):
    scores = (
        jnp.einsum("shqd,shkd->shqk", query_heads, key_heads, preferred_element_type=jnp.float32)
        * scale
    )
    return jnp.where(valid_keys[:, None, None, :], scores, -1e30)


def pack_vectors(rows, vectors, dtype):
    cols = [v.reshape(rows, -1).astype(dtype) for v in vectors]
    block = jnp.concatenate(cols, axis=1)
    return jnp.pad(block, ((0, 0), (0, VEC_COLS - block.shape[1])))


def unpack_vectors(block, widths):
    out, at = [], 0
    for width in widths:
        out.append(block[:, at : at + width].reshape(-1))
        at += width
    return out


def gather_rows(pack):
    return lax.all_gather(pack, AXES, axis=0, tiled=True)


def scatter_rows(pack):
    return lax.psum_scatter(pack.astype(GRAD_WIRE), AXES, scatter_dimension=0, tiled=True).astype(
        jnp.float32
    )


def _pick(bit, first, second):
    return jnp.where(bit == 0, first, second), jnp.where(bit == 0, second, first)


def tree_gather(block, last_bit):
    n_sub = lax.axis_size("sub")
    n_f = lax.axis_size("fsdp")
    bits = n_f.bit_length() - 1
    chip = lax.axis_index("fsdp")
    order = [b for b in range(bits - 1, -1, -1) if b != last_bit] + [last_bit]
    acc = block
    done = []
    for j in order:
        pairs = [(g, g ^ (1 << j)) for g in range(n_f)]
        recv = lax.ppermute(acc, "fsdp", pairs)
        bit = (chip >> j) & 1
        lo, hi = _pick(bit, acc, recv)
        axis = sum(1 for b in done if b > j)
        acc = jnp.stack([lo, hi], axis=axis)
        done.append(j)
    acc = acc.reshape((n_f,) + block.shape)
    core = lax.axis_index("sub")
    recv = lax.ppermute(acc, "sub", [(0, 1), (1, 0)])
    lo, hi = _pick(core, acc, recv)
    full = jnp.stack([lo, hi], axis=1)
    return full.reshape((n_f * n_sub * block.shape[0],) + block.shape[1:])


def tree_scatter(full, first_bit):
    n_sub = lax.axis_size("sub")
    n_f = lax.axis_size("fsdp")
    rows = full.shape[0] // (n_sub * n_f)
    acc = full.reshape(n_f, n_sub, rows, -1)
    core = lax.axis_index("sub")
    keep = lax.dynamic_index_in_dim(acc, core, 1, keepdims=False)
    send = lax.dynamic_index_in_dim(acc, 1 - core, 1, keepdims=False)
    acc = keep + lax.ppermute(send, "sub", [(0, 1), (1, 0)])
    chip = lax.axis_index("fsdp")
    bits = n_f.bit_length() - 1
    acc = acc.reshape((2,) * bits + (rows, -1))
    left = list(range(bits - 1, -1, -1))
    order = [first_bit] + [b for b in range(bits) if b != first_bit]
    for j in order:
        axis = left.index(j)
        left.remove(j)
        bit = (chip >> j) & 1
        keep = lax.dynamic_index_in_dim(acc, bit, axis, keepdims=False)
        send = lax.dynamic_index_in_dim(acc, 1 - bit, axis, keepdims=False)
        pairs = [(g, g ^ (1 << j)) for g in range(n_f)]
        recv = lax.ppermute(send.astype(GRAD_WIRE), "fsdp", pairs)
        acc = keep + recv.astype(jnp.float32)
    return acc.reshape(rows, -1)


def body(
    inputs,
    lengths,
    positions,
    masked_output_gradient,
    w_query,
    b_query,
    w_key,
    w_value,
    b_value,
    w_out,
    b_out,
    gain_attn,
    shift_attn,
    w_up,
    b_up,
    w_down,
    b_down,
    gain_ffn,
    shift_ffn,
):
    seq_count, seq_slots, width = inputs.shape
    head_count = width // HD
    scale = HD ** (-0.5)
    row_count = seq_count * seq_slots
    head_shape = (seq_count, seq_slots, head_count, HD)
    shard_rows = w_query.shape[0]
    ff_ratio = w_down.shape[0] // shard_rows
    ff_width = w_up.shape[1]
    token_ids = jnp.arange(seq_slots, dtype=jnp.int32)
    valid_keys = token_ids[None, :] < lengths[:, None]

    with jax.named_scope("gather_attn"):
        vec_pack = pack_vectors(
            shard_rows,
            (
                b_query,
                b_value,
                b_out,
                gain_attn,
                shift_attn,
                b_up,
                b_down,
                gain_ffn,
                shift_ffn,
            ),
            jnp.bfloat16,
        )
        cut = (width // 6, width * 2 // 3)
        query_part = tree_gather(
            jnp.concatenate([w_query, w_value[:, : cut[0]], vec_pack], axis=1), 0
        )
        key_part = tree_gather(jnp.concatenate([w_key, w_value[:, cut[0] : cut[1]]], axis=1), 1)
        out_part = tree_gather(jnp.concatenate([w_value[:, cut[1] :], w_out], axis=1), 2)
    query_weight = query_part[:, 0:width]
    key_weight = key_part[:, 0:width]
    value_weight = jnp.concatenate(
        [
            query_part[:, width : width + cut[0]],
            key_part[:, width:],
            out_part[:, : width - cut[1]],
        ],
        axis=1,
    )
    out_weight = out_part[:, width - cut[1] :]
    vec_start = width + cut[0]
    (
        query_bias,
        value_bias,
        out_bias,
        norm1_gain,
        norm1_shift,
        up_bias,
        downward_bias,
        norm2_gain,
        norm2_shift,
    ) = unpack_vectors(query_part[:, vec_start:], (1, 1, 1, 1, 1, ff_ratio, 1, 1, 1))

    with jax.named_scope("gather_ffn"):
        up_weight = gather_rows(w_up)
        down_weight = gather_rows(w_down)

    flat_in = inputs.reshape(row_count, width)
    input_rows = flat_in.astype(jnp.float32)
    head_weights = (head_count, HD)
    query_w3 = query_weight.reshape((width,) + head_weights)
    key_w3 = key_weight.reshape((width,) + head_weights)
    value_w3 = value_weight.reshape((width,) + head_weights)
    out_w3 = out_weight.reshape(head_weights + (width,))
    query_heads = (
        jnp.einsum("snc,chd->shnd", inputs, query_w3, preferred_element_type=jnp.float32)
        + query_bias.astype(jnp.float32).reshape(head_weights)[None, :, None, :]
    ).astype(jnp.bfloat16)
    key_heads = jnp.einsum(
        "snc,chd->shnd", inputs, key_w3, preferred_element_type=jnp.float32
    ).astype(jnp.bfloat16)
    value_heads = (
        jnp.einsum("snc,chd->shnd", inputs, value_w3, preferred_element_type=jnp.float32)
        + value_bias.astype(jnp.float32).reshape(head_weights)[None, :, None, :]
    ).astype(jnp.bfloat16)
    scores = attention_scores(query_heads, key_heads, valid_keys, scale)
    row_top = jnp.max(scores, axis=-1, keepdims=True)
    expon = jnp.exp(scores - row_top)
    row_total = jnp.sum(expon, axis=-1, keepdims=True)
    log_total = row_top + jnp.log(row_total)
    probs_low = (expon / row_total).astype(jnp.bfloat16)
    attention_mixed = jnp.einsum(
        "shqk,shkd->shqd", probs_low, value_heads, preferred_element_type=jnp.float32
    )
    attended_low = attention_mixed.astype(jnp.bfloat16)
    branch = (
        jnp.einsum("shqd,hdc->sqc", attended_low, out_w3, preferred_element_type=jnp.float32)
        .reshape(row_count, width)
    ) + out_bias.astype(jnp.float32)
    middle, norm1_pull = jax.vjp(
        layer_norm,
        input_rows + branch,
        norm1_gain.astype(jnp.float32),
        norm1_shift.astype(jnp.float32),
    )
    middle_low = middle.astype(jnp.bfloat16)
    hidden = project(middle_low, up_weight) + up_bias.astype(jnp.float32)
    active, gelu_pull = jax.vjp(gelu_exact, hidden)
    active_low = active.astype(jnp.bfloat16)
    second_branch = project(active_low, down_weight) + downward_bias.astype(jnp.float32)
    output, norm2_pull = jax.vjp(
        layer_norm,
        middle + second_branch,
        norm2_gain.astype(jnp.float32),
        norm2_shift.astype(jnp.float32),
    )
    position_matches = (positions[:, :, None] == token_ids[None, None, :]).astype(jnp.bfloat16)
    cotangent = jnp.einsum(
        "efw,efv->ewv", position_matches, masked_output_gradient, preferred_element_type=jnp.float32
    ).reshape(row_count, width)
    grad_sum2, grad_gain2, grad_shift2 = norm2_pull(cotangent)
    second_grad = grad_sum2.astype(jnp.bfloat16)
    grad_down = weight_grad(active_low, second_grad)
    grad_down_bias = column_sum(second_grad)
    (grad_hidden,) = gelu_pull(reverse_projection(second_grad, down_weight))
    hidden_grad = grad_hidden.astype(jnp.bfloat16)
    grad_up = weight_grad(middle_low, hidden_grad)
    grad_up_bias = column_sum(hidden_grad)
    grad_middle = grad_sum2 + reverse_projection(hidden_grad, up_weight)
    grad_residual, grad_gain1, grad_shift1 = norm1_pull(grad_middle)
    branch_grad = grad_residual.astype(jnp.bfloat16)
    grad_out = jnp.einsum(
        "shqd,sqc->hdc", attended_low, branch_grad.reshape(inputs.shape),
        preferred_element_type=jnp.float32,
    ).reshape(width, width)
    grad_out_bias = column_sum(branch_grad)

    with jax.named_scope("scatter_late"):
        late_pack = jnp.concatenate(
            [
                grad_up.astype(GRAD_WIRE),
                grad_down.astype(GRAD_WIRE).reshape(width, ff_ratio * width),
                grad_out.astype(GRAD_WIRE),
                pack_vectors(
                    width,
                    (
                        grad_up_bias,
                        grad_down_bias,
                        grad_gain2,
                        grad_shift2,
                        grad_out_bias,
                        grad_gain1,
                        grad_shift1,
                    ),
                    GRAD_WIRE,
                ),
            ],
            axis=1,
        )
        late_pack, branch_grad = lax.optimization_barrier((late_pack, branch_grad))
        late_own = scatter_rows(late_pack)
    grad_down_own = late_own[:, ff_width : 2 * ff_width].reshape(shard_rows * ff_ratio, width)
    late_own = jnp.concatenate([late_own[:, 0:ff_width], late_own[:, 2 * ff_width :]], axis=1)
    grad_up_own = late_own[:, 0:ff_width]
    grad_out_own = late_own[:, ff_width : ff_width + width]
    (
        grad_up_bias_own,
        grad_down_bias_own,
        grad_gain2_own,
        grad_shift2_own,
        grad_out_bias_own,
        grad_gain1_own,
        grad_shift1_own,
    ) = unpack_vectors(late_own[:, ff_width + width :], (ff_ratio, 1, 1, 1, 1, 1, 1))

    attended_grad = (
        reverse_projection(branch_grad, out_weight).astype(jnp.bfloat16).reshape(head_shape)
    )
    scores_again = attention_scores(query_heads, key_heads, valid_keys, scale)
    probs = jnp.exp(scores_again - log_total)
    probs_again = probs.astype(jnp.bfloat16)
    probs_grad = jnp.einsum(
        "sqhd,shkd->shqk", attended_grad, value_heads, preferred_element_type=jnp.float32
    )
    values_grad = jnp.einsum(
        "shqk,sqhd->skhd", probs_again, attended_grad, preferred_element_type=jnp.float32
    )
    values_grad = values_grad.astype(jnp.bfloat16).reshape(row_count, width)
    inner_sum = jnp.sum(probs * probs_grad, axis=-1, keepdims=True)
    scores_grad = (probs * (probs_grad - inner_sum)).astype(jnp.bfloat16)
    query_grad = jnp.einsum(
        "shqk,shkd->sqhd", scores_grad, key_heads, preferred_element_type=jnp.float32
    )
    query_grad = (query_grad * scale).astype(jnp.bfloat16).reshape(row_count, width)
    keys_grad = jnp.einsum(
        "shqk,shqd->skhd", scores_grad, query_heads, preferred_element_type=jnp.float32
    )
    keys_grad = (keys_grad * scale).astype(jnp.bfloat16).reshape(row_count, width)
    grad_query = weight_grad(flat_in, query_grad)
    grad_query_bias = column_sum(query_grad)
    grad_key = weight_grad(flat_in, keys_grad)
    grad_value = weight_grad(flat_in, values_grad)
    value_bias_gradient = column_sum(values_grad)
    grad_input = (
        grad_residual
        + reverse_projection(query_grad, query_weight)
        + reverse_projection(keys_grad, key_weight)
        + reverse_projection(values_grad, value_weight)
    )
    with jax.named_scope("scatter_qkv"):
        query_own_pack = tree_scatter(
            jnp.concatenate(
                [
                    grad_query,
                    pack_vectors(width, (grad_query_bias, value_bias_gradient), jnp.float32),
                ],
                axis=1,
            ),
            0,
        )
        grad_key_own = tree_scatter(grad_key, 1)
        grad_value_own = tree_scatter(grad_value, 2)
    grad_query_own = query_own_pack[:, 0:width]
    grad_query_bias_own, value_bias_gradient_own = unpack_vectors(
        query_own_pack[:, width:], (1, 1)
    )
    return (
        output.astype(jnp.bfloat16).reshape(inputs.shape),
        grad_input.astype(jnp.bfloat16).reshape(inputs.shape),
        grad_query_own,
        grad_query_bias_own,
        grad_key_own,
        grad_value_own,
        value_bias_gradient_own,
        grad_out_own,
        grad_out_bias_own,
        grad_gain1_own,
        grad_shift1_own,
        grad_up_own,
        grad_up_bias_own,
        grad_down_own,
        grad_down_bias_own,
        grad_gain2_own,
        grad_shift2_own,
    )


def solution(mesh):
    rows3 = P(AXES, None, None)
    rows2 = P(AXES, None)
    rows1 = P(AXES)
    return jax.shard_map(
        body,
        mesh=mesh,
        in_specs=(
            rows3,
            rows1,
            rows2,
            rows3,
            rows2,
            rows1,
            rows2,
            rows2,
            rows1,
            rows2,
            rows1,
            rows1,
            rows1,
            rows2,
            rows1,
            rows2,
            rows1,
            rows1,
            rows1,
        ),
        out_specs=(
            rows3,
            rows3,
            rows2,
            rows1,
            rows2,
            rows2,
            rows1,
            rows2,
            rows1,
            rows1,
            rows1,
            rows2,
            rows1,
            rows2,
            rows1,
            rows1,
            rows1,
        ),
        check_vma=False,
    )
```

```python
import jax
import jax.numpy as jnp
from jax import lax
from jax.sharding import PartitionSpec as P

HD = 64
EPSILON = 1e-06
AXES = ("fsdp", "sub")
GRAD_WIRE = jnp.bfloat16
VEC_COLS = 256


def layer_norm(values, gain, shift):
    average = jnp.mean(values, axis=-1, keepdims=True)
    centered = values - average
    variance = jnp.mean(centered * centered, axis=-1, keepdims=True)
    return centered * lax.rsqrt(variance + EPSILON) * gain + shift


def gelu_exact(values):
    return values * (0.5 * (1.0 + lax.erf(values * (2.0 ** -0.5))))


def project(rows_low, weight):
    return jnp.dot(rows_low, weight, preferred_element_type=jnp.float32)


def reverse_projection(grad_low, weight):
    return lax.dot_general(
        grad_low, weight, (((1,), (1,)), ((), ())), preferred_element_type=jnp.float32
    )


def weight_grad(rows_low, grad_low):
    return lax.dot_general(
        rows_low, grad_low, (((0,), (0,)), ((), ())), preferred_element_type=jnp.float32
    )


def column_sum(grad_low):
    return jnp.sum(grad_low.astype(jnp.float32), axis=0)


def attention_scores(query_heads, key_heads, valid_keys, scale):
    scores = (
        jnp.einsum("shqd,shkd->shqk", query_heads, key_heads, preferred_element_type=jnp.float32)
        * scale
    )
    return jnp.where(valid_keys[:, None, None, :], scores, -1e30)


def pack_vectors(rows, vectors, dtype):
    cols = [v.reshape(rows, -1).astype(dtype) for v in vectors]
    block = jnp.concatenate(cols, axis=1)
    return jnp.pad(block, ((0, 0), (0, VEC_COLS - block.shape[1])))


def unpack_vectors(block, widths):
    out, at = [], 0
    for width in widths:
        out.append(block[:, at : at + width].reshape(-1))
        at += width
    return out


def gather_rows(pack):
    return lax.all_gather(pack, AXES, axis=0, tiled=True)


def scatter_rows(pack):
    return lax.psum_scatter(pack.astype(GRAD_WIRE), AXES, scatter_dimension=0, tiled=True).astype(
        jnp.float32
    )


def _pick(bit, first, second):
    return jnp.where(bit == 0, first, second), jnp.where(bit == 0, second, first)


def tree_gather(block, last_bit):
    n_sub = lax.axis_size("sub")
    n_f = lax.axis_size("fsdp")
    bits = n_f.bit_length() - 1
    chip = lax.axis_index("fsdp")
    order = [b for b in range(bits - 1, -1, -1) if b != last_bit] + [last_bit]
    acc = block
    done = []
    for j in order:
        pairs = [(g, g ^ (1 << j)) for g in range(n_f)]
        recv = lax.ppermute(acc, "fsdp", pairs)
        bit = (chip >> j) & 1
        lo, hi = _pick(bit, acc, recv)
        axis = sum(1 for b in done if b > j)
        acc = jnp.stack([lo, hi], axis=axis)
        done.append(j)
    acc = acc.reshape((n_f,) + block.shape)
    core = lax.axis_index("sub")
    recv = lax.ppermute(acc, "sub", [(0, 1), (1, 0)])
    lo, hi = _pick(core, acc, recv)
    full = jnp.stack([lo, hi], axis=1)
    return full.reshape((n_f * n_sub * block.shape[0],) + block.shape[1:])


def tree_scatter(full, first_bit):
    n_sub = lax.axis_size("sub")
    n_f = lax.axis_size("fsdp")
    rows = full.shape[0] // (n_sub * n_f)
    acc = full.reshape(n_f, n_sub, rows, -1)
    core = lax.axis_index("sub")
    keep = lax.dynamic_index_in_dim(acc, core, 1, keepdims=False)
    send = lax.dynamic_index_in_dim(acc, 1 - core, 1, keepdims=False)
    acc = keep + lax.ppermute(send, "sub", [(0, 1), (1, 0)])
    chip = lax.axis_index("fsdp")
    bits = n_f.bit_length() - 1
    acc = acc.reshape((2,) * bits + (rows, -1))
    left = list(range(bits - 1, -1, -1))
    order = [first_bit] + [b for b in range(bits) if b != first_bit]
    for j in order:
        axis = left.index(j)
        left.remove(j)
        bit = (chip >> j) & 1
        keep = lax.dynamic_index_in_dim(acc, bit, axis, keepdims=False)
        send = lax.dynamic_index_in_dim(acc, 1 - bit, axis, keepdims=False)
        pairs = [(g, g ^ (1 << j)) for g in range(n_f)]
        recv = lax.ppermute(send.astype(GRAD_WIRE), "fsdp", pairs)
        acc = keep + recv.astype(jnp.float32)
    return acc.reshape(rows, -1)


def body(
    inputs,
    lengths,
    positions,
    masked_output_gradient,
    w_query,
    b_query,
    w_key,
    w_value,
    b_value,
    w_out,
    b_out,
    gain_attn,
    shift_attn,
    w_up,
    b_up,
    w_down,
    b_down,
    gain_ffn,
    shift_ffn,
):
    seq_count, seq_slots, width = inputs.shape
    head_count = width // HD
    scale = HD ** (-0.5)
    row_count = seq_count * seq_slots
    head_shape = (seq_count, seq_slots, head_count, HD)
    shard_rows = w_query.shape[0]
    ff_ratio = w_down.shape[0] // shard_rows
    ff_width = w_up.shape[1]
    token_ids = jnp.arange(seq_slots, dtype=jnp.int32)
    valid_keys = token_ids[None, :] < lengths[:, None]

    with jax.named_scope("gather_attn"):
        vec_pack = pack_vectors(
            shard_rows, (b_query, b_value, b_out, gain_attn, shift_attn), jnp.bfloat16
        )
        cut = (width // 6, width * 2 // 3)
        query_part = tree_gather(
            jnp.concatenate([w_query, w_value[:, : cut[0]], vec_pack], axis=1), 0
        )
        key_part = tree_gather(jnp.concatenate([w_key, w_value[:, cut[0] : cut[1]]], axis=1), 1)
        out_part = tree_gather(jnp.concatenate([w_value[:, cut[1] :], w_out], axis=1), 2)
    query_weight = query_part[:, 0:width]
    key_weight = key_part[:, 0:width]
    value_weight = jnp.concatenate(
        [
            query_part[:, width : width + cut[0]],
            key_part[:, width:],
            out_part[:, : width - cut[1]],
        ],
        axis=1,
    )
    out_weight = out_part[:, width - cut[1] :]
    vec_start = width + cut[0]
    query_bias, value_bias, out_bias, norm1_gain, norm1_shift = unpack_vectors(
        query_part[:, vec_start:], (1, 1, 1, 1, 1)
    )

    with jax.named_scope("gather_ffn"):
        ffn_pack = jnp.concatenate(
            [
                w_up,
                pack_vectors(
                    shard_rows, (b_up, b_down, gain_ffn, shift_ffn), jnp.bfloat16
                ),
            ],
            axis=1,
        )
        ffn_full = gather_rows(ffn_pack)
        down_weight = gather_rows(w_down)
    up_weight = ffn_full[:, 0:ff_width]
    up_bias, downward_bias, norm2_gain, norm2_shift = unpack_vectors(
        ffn_full[:, ff_width:], (ff_ratio, 1, 1, 1)
    )

    flat_in = inputs.reshape(row_count, width)
    input_rows = flat_in.astype(jnp.float32)
    head_weights = (head_count, HD)
    query_w3 = query_weight.reshape((width,) + head_weights)
    key_w3 = key_weight.reshape((width,) + head_weights)
    value_w3 = value_weight.reshape((width,) + head_weights)
    out_w3 = out_weight.reshape(head_weights + (width,))
    query_heads = (
        jnp.einsum("snc,chd->shnd", inputs, query_w3, preferred_element_type=jnp.float32)
        + query_bias.astype(jnp.float32).reshape(head_weights)[None, :, None, :]
    ).astype(jnp.bfloat16)
    key_heads = jnp.einsum(
        "snc,chd->shnd", inputs, key_w3, preferred_element_type=jnp.float32
    ).astype(jnp.bfloat16)
    value_heads = (
        jnp.einsum("snc,chd->shnd", inputs, value_w3, preferred_element_type=jnp.float32)
        + value_bias.astype(jnp.float32).reshape(head_weights)[None, :, None, :]
    ).astype(jnp.bfloat16)
    scores = attention_scores(query_heads, key_heads, valid_keys, scale)
    row_top = jnp.max(scores, axis=-1, keepdims=True)
    expon = jnp.exp(scores - row_top)
    row_total = jnp.sum(expon, axis=-1, keepdims=True)
    log_total = row_top + jnp.log(row_total)
    probs_low = (expon * (1.0 / row_total)).astype(jnp.bfloat16)
    attention_mixed = jnp.einsum(
        "shqk,shkd->shqd", probs_low, value_heads, preferred_element_type=jnp.float32
    )
    attended_low = attention_mixed.astype(jnp.bfloat16)
    branch = (
        jnp.einsum("shqd,hdc->sqc", attended_low, out_w3, preferred_element_type=jnp.float32)
        .reshape(row_count, width)
    ) + out_bias.astype(jnp.float32)
    middle, norm1_pull = jax.vjp(
        layer_norm,
        input_rows + branch,
        norm1_gain.astype(jnp.float32),
        norm1_shift.astype(jnp.float32),
    )
    middle_low = middle.astype(jnp.bfloat16)
    hidden = project(middle_low, up_weight) + up_bias.astype(jnp.float32)
    active, gelu_pull = jax.vjp(gelu_exact, hidden)
    active_low = active.astype(jnp.bfloat16)
    second_branch = project(active_low, down_weight) + downward_bias.astype(jnp.float32)
    output, norm2_pull = jax.vjp(
        layer_norm,
        middle + second_branch,
        norm2_gain.astype(jnp.float32),
        norm2_shift.astype(jnp.float32),
    )
    position_matches = (positions[:, :, None] == token_ids[None, None, :]).astype(jnp.bfloat16)
    cotangent = jnp.einsum(
        "efw,efv->ewv", position_matches, masked_output_gradient, preferred_element_type=jnp.float32
    ).reshape(row_count, width)
    grad_sum2, grad_gain2, grad_shift2 = norm2_pull(cotangent)
    second_grad = grad_sum2.astype(jnp.bfloat16)
    grad_down = weight_grad(active_low, second_grad)
    grad_down_bias = column_sum(second_grad)
    (grad_hidden,) = gelu_pull(reverse_projection(second_grad, down_weight))
    hidden_grad = grad_hidden.astype(jnp.bfloat16)
    grad_up = weight_grad(middle_low, hidden_grad)
    grad_up_bias = column_sum(hidden_grad)
    grad_middle = grad_sum2 + reverse_projection(hidden_grad, up_weight)
    grad_residual, grad_gain1, grad_shift1 = norm1_pull(grad_middle)
    branch_grad = grad_residual.astype(jnp.bfloat16)
    grad_out = jnp.einsum(
        "shqd,sqc->hdc", attended_low, branch_grad.reshape(inputs.shape),
        preferred_element_type=jnp.float32,
    ).reshape(width, width)
    grad_out_bias = column_sum(branch_grad)

    with jax.named_scope("scatter_late"):
        late_pack = jnp.concatenate(
            [
                grad_up.astype(GRAD_WIRE),
                grad_down.astype(GRAD_WIRE).reshape(width, ff_ratio * width),
                grad_out.astype(GRAD_WIRE),
                pack_vectors(
                    width,
                    (
                        grad_up_bias,
                        grad_down_bias,
                        grad_gain2,
                        grad_shift2,
                        grad_out_bias,
                        grad_gain1,
                        grad_shift1,
                    ),
                    GRAD_WIRE,
                ),
            ],
            axis=1,
        )
        late_pack, branch_grad = lax.optimization_barrier((late_pack, branch_grad))
        late_own = scatter_rows(late_pack)
    grad_down_own = late_own[:, ff_width : 2 * ff_width].reshape(shard_rows * ff_ratio, width)
    late_own = jnp.concatenate([late_own[:, 0:ff_width], late_own[:, 2 * ff_width :]], axis=1)
    grad_up_own = late_own[:, 0:ff_width]
    grad_out_own = late_own[:, ff_width : ff_width + width]
    (
        grad_up_bias_own,
        grad_down_bias_own,
        grad_gain2_own,
        grad_shift2_own,
        grad_out_bias_own,
        grad_gain1_own,
        grad_shift1_own,
    ) = unpack_vectors(late_own[:, ff_width + width :], (ff_ratio, 1, 1, 1, 1, 1, 1))

    attended_grad = (
        reverse_projection(branch_grad, out_weight).astype(jnp.bfloat16).reshape(head_shape)
    )
    scores_again = attention_scores(query_heads, key_heads, valid_keys, scale)
    probs = jnp.exp(scores_again - log_total)
    probs_again = probs.astype(jnp.bfloat16)
    probs_grad = jnp.einsum(
        "sqhd,shkd->shqk", attended_grad, value_heads, preferred_element_type=jnp.float32
    )
    values_grad = jnp.einsum(
        "shqk,sqhd->skhd", probs_again, attended_grad, preferred_element_type=jnp.float32
    )
    values_grad = values_grad.astype(jnp.bfloat16).reshape(row_count, width)
    inner_sum = jnp.sum(probs * probs_grad, axis=-1, keepdims=True)
    scores_grad = (probs * (probs_grad - inner_sum)).astype(jnp.bfloat16)
    query_grad = jnp.einsum(
        "shqk,shkd->sqhd", scores_grad, key_heads, preferred_element_type=jnp.float32
    )
    query_grad = (query_grad * scale).astype(jnp.bfloat16).reshape(row_count, width)
    keys_grad = jnp.einsum(
        "shqk,shqd->skhd", scores_grad, query_heads, preferred_element_type=jnp.float32
    )
    keys_grad = (keys_grad * scale).astype(jnp.bfloat16).reshape(row_count, width)
    grad_query = weight_grad(flat_in, query_grad)
    grad_query_bias = column_sum(query_grad)
    grad_key = weight_grad(flat_in, keys_grad)
    grad_value = weight_grad(flat_in, values_grad)
    value_bias_gradient = column_sum(values_grad)
    grad_input = (
        grad_residual
        + reverse_projection(query_grad, query_weight)
        + reverse_projection(keys_grad, key_weight)
        + reverse_projection(values_grad, value_weight)
    )
    with jax.named_scope("scatter_qkv"):
        query_own_pack = tree_scatter(
            jnp.concatenate(
                [
                    grad_query,
                    pack_vectors(width, (grad_query_bias, value_bias_gradient), jnp.float32),
                ],
                axis=1,
            ),
            0,
        )
        grad_key_own = tree_scatter(grad_key, 1)
        grad_value_own = tree_scatter(grad_value, 2)
    grad_query_own = query_own_pack[:, 0:width]
    grad_query_bias_own, value_bias_gradient_own = unpack_vectors(
        query_own_pack[:, width:], (1, 1)
    )
    return (
        output.astype(jnp.bfloat16).reshape(inputs.shape),
        grad_input.astype(jnp.bfloat16).reshape(inputs.shape),
        grad_query_own,
        grad_query_bias_own,
        grad_key_own,
        grad_value_own,
        value_bias_gradient_own,
        grad_out_own,
        grad_out_bias_own,
        grad_gain1_own,
        grad_shift1_own,
        grad_up_own,
        grad_up_bias_own,
        grad_down_own,
        grad_down_bias_own,
        grad_gain2_own,
        grad_shift2_own,
    )


def solution(mesh):
    rows3 = P(AXES, None, None)
    rows2 = P(AXES, None)
    rows1 = P(AXES)
    return jax.shard_map(
        body,
        mesh=mesh,
        in_specs=(
            rows3,
            rows1,
            rows2,
            rows3,
            rows2,
            rows1,
            rows2,
            rows2,
            rows1,
            rows2,
            rows1,
            rows1,
            rows1,
            rows2,
            rows1,
            rows2,
            rows1,
            rows1,
            rows1,
        ),
        out_specs=(
            rows3,
            rows3,
            rows2,
            rows1,
            rows2,
            rows2,
            rows1,
            rows2,
            rows1,
            rows1,
            rows1,
            rows2,
            rows1,
            rows2,
            rows1,
            rows1,
            rows1,
        ),
        check_vma=False,
    )
```
